32 devices in a mesh: blk: 8 (over y, x, core), grp: 4 (over z).
Axes of the slice: x: 2, y: 2, z: 4, core: 2. Of those that a mesh axis runs over, the one named last changes fastest.
Arguments:
- image_embeds: bfloat16 [4096, 1152], P(('blk', 'grp')), may hold values from -6 to 6
- text_embeds: bfloat16 [4096, 1152], P(('blk', 'grp')), may hold values from -6 to 6
Outputs:
- image_embed_gradient: bfloat16 [4096, 1152], P(('blk', 'grp'))
- text_embed_gradient: bfloat16 [4096, 1152], P(('blk', 'grp'))
The draws below stay inside these ranges and needn't reach their ends.
All inputs are finite; a program needn't handle non-finite values.
Results may differ from the reference program's by a relative error of at most 0.0059.
Values may be sent and summed in bfloat16 or wider, within the bound.
A program may use at most 64 MiB of HBM per device.

```python
import jax
import jax.numpy as jnp
from jax import lax

EMBED_WIDTH = 1152
BLOCK_ROWS = 128
STEPS = 16
BATCH = 4096


def block_scale(rng, dims, cuts, smallest, largest):
    def one(position, blocks):
        heights = jax.random.uniform(jax.random.fold_in(jax.random.fold_in(rng, 6), position), (blocks,), jnp.float32, smallest / len(cuts), largest / len(cuts))
        return jnp.repeat(jnp.exp(heights), dims[position] // blocks).reshape((-1,) + (1,) * (len(dims) - position - 1))

    loudness = one(*cuts[0])
    for cut in cuts[1:]:
        loudness = loudness * one(*cut)
    return loudness


def gaussian(key, extent, scale, reach, split=(), held_as=jnp.bfloat16):
    drawn = scale * jax.random.normal(key, extent, jnp.float32)
    if split:
        drawn = drawn * block_scale(key, extent, split, -0.22, 0.18)
    return jnp.clip(drawn, -reach, reach).astype(held_as)


def setup_inputs(seed: int = 0) -> dict:
    seeds = jax.random.split(jax.random.key(seed), 3)
    return {
        "image_embeds": gaussian(seeds[0], (BATCH, EMBED_WIDTH), 1.0, 6.0, ((0, 32),)),
        "text_embeds": gaussian(seeds[1], (BATCH, EMBED_WIDTH), 1.0, 6.0, ((0, 32),)),
    }


LOGIT_SCALE = 10.0
BIAS_LOGIT = -2.0
EPSILON = 1e-06

def normalize(values):
    wide = values.astype(jnp.float32)
    length = jnp.sqrt(lax.optimization_barrier(jnp.sum(wide * wide, axis=-1, keepdims=True)) + EPSILON)
    return (wide / length, length)

def undo_normalization(grad, unit, length):
    inner = lax.optimization_barrier(jnp.sum(unit * grad, axis=-1, keepdims=True))
    return (grad - unit * inner) / length

def pair_weights(pair_logits, is_first):
    count = pair_logits.shape[-1]
    diagonal_mask = jnp.eye(count, dtype=bool) & is_first
    return jnp.where(diagonal_mask, -jax.nn.sigmoid(-pair_logits), jax.nn.sigmoid(pair_logits))

def reference(image_embeds, text_embeds):
    block_list = image_embeds.shape[0] // BLOCK_ROWS
    image_normalized, image_norm = normalize(image_embeds)
    text_normalized, text_norm = normalize(text_embeds)
    image_reduced = image_normalized.astype(jnp.bfloat16).astype(jnp.float32).reshape(block_list, BLOCK_ROWS, EMBED_WIDTH)
    text_low = text_normalized.astype(jnp.bfloat16).astype(jnp.float32).reshape(block_list, BLOCK_ROWS, EMBED_WIDTH)

    def advance(running, offset):
        image_total, text_total = running
        shifted_block = jnp.roll(text_low, offset, axis=0)
        pair_logits = LOGIT_SCALE * jnp.einsum('gty,gky->gtk', image_reduced, shifted_block) + BIAS_LOGIT
        weights = pair_weights(pair_logits, offset == 0).astype(jnp.bfloat16).astype(jnp.float32)
        image_total = image_total + jnp.einsum('prc,pcd->prd', weights, shifted_block)
        text_terms = jnp.einsum('prc,prd->pcd', weights, image_reduced)
        text_total = text_total + jnp.roll(text_terms, -offset, axis=0)
        return ((image_total, text_total), None)
    zeros = jnp.zeros((block_list, BLOCK_ROWS, EMBED_WIDTH), jnp.float32)
    (image_total, text_total), _ = lax.scan(advance, (zeros, zeros), jnp.arange(STEPS, dtype=jnp.int32))
    image_gradient = LOGIT_SCALE * image_total.reshape(block_list * BLOCK_ROWS, EMBED_WIDTH)
    text_gradient = LOGIT_SCALE * text_total.reshape(block_list * BLOCK_ROWS, EMBED_WIDTH)
    image_embed_gradient = undo_normalization(image_gradient, image_normalized, image_norm).astype(jnp.bfloat16)
    text_embed_gradient = undo_normalization(text_gradient, text_normalized, text_norm).astype(jnp.bfloat16)
    return (image_embed_gradient, text_embed_gradient)
```

```python
import functools

import jax
import jax.numpy as jnp
from jax import lax
from jax.experimental import pallas as pl
from jax.experimental.pallas import tpu as pltpu
from jax.sharding import PartitionSpec as P

LOGIT_SCALE = 10.0
BIAS_LOGIT = -2.0
EPSILON = 1e-06
PIECE_ROWS = 16
MESH = pl.DeviceIdType.MESH


def kernel(chips, depth, reach, window, image_ref, text_ref, image_out, text_out,
           held, total, own_scale, local_sem, send_sem, recv_sem):
    blk = lax.axis_index("blk")
    grp = lax.axis_index("grp")
    chip, core = blk // 2, blk % 2
    relayed = chips == 4 and reach == 2 and 4 * depth - 1 < window

    def view(kind):
        return (
            chip + kind * (chips - 1 - 2 * chip),
            core + kind * (1 - 2 * core),
            grp + kind * (depth - 1 - 2 * grp),
        )

    def device(kind, c, k, z):
        c = (c + chips) % chips
        linear = 2 * c + k
        return (
            linear + kind * (2 * chips - 1 - 2 * linear),
            z + kind * (depth - 1 - 2 * z),
        )

    first_kind = 1 - chip % 2 if relayed else 0
    kinds = (first_kind, 1 - first_kind)

    def need(k, z, d, source_k, source_z):
        offset = (2 * d + k - source_k) * depth + z - source_z
        return (offset >= 0) & (offset < window)

    def chip_need(z, d, source_k, source_z):
        return need(0, z, d, source_k, source_z) | need(1, z, d, source_k, source_z)

    def arrives(kind, d, source_z):
        c, k, z = view(kind)
        wanted = chip_need(z, d, k, source_z)
        if relayed:
            wanted = wanted | ((d == 2) & (c % 2 == 1))
        return wanted

    def copy(kind, path, source_slot, target_slot, z, target):
        return pltpu.make_async_remote_copy(
            src_ref=held.at[kind, source_slot, z],
            dst_ref=held.at[kind, target_slot, z],
            send_sem=send_sem.at[kind, path, z],
            recv_sem=recv_sem.at[kind, target_slot, z],
            device_id=target,
            device_id_type=MESH,
        )

    def own_sends(kind, z2):
        c, k, z = view(kind)
        sends = [
            ((z2 <= z) & (z + 1 < depth), 0, k, k, (c, k, z + 1)),
            ((z2 >= z) & (z >= 1), 1, k, k, (c, k, z - 1)),
        ]
        for d in range(1, reach + 1):
            wanted = chip_need(z, d, k, z2)
            if relayed and d == 1:
                inside = (z2 > 0) & (z2 < depth - 1)
                wanted = (c % 2 == 0) & (inside | (z2 == z))
            if relayed and d == 2:
                wanted = wanted | (c % 2 == 1)
            sends.append((wanted, 1 + d, k, 2 * d + k, (c + d, k, z)))
        sends.append((need(1 - k, z, 0, k, z2), 2 + reach, k, k, (c, 1 - k, z)))
        return sends

    def arrival_sends(kind, d, z2):
        c, k, z = view(kind)
        sends = []
        slot = 2 * d + k
        if relayed:
            sends.append(((c % 2 == 1) & (d == 2), 3 + reach, slot, 2 + k, (c - 1, k, z)))
            outer = (c % 2 == 1) & (d == 1) & ((z2 == 0) | (z2 == depth - 1))
            sends.append((outer & (z2 <= z) & (z + 1 < depth),
                          4 + 2 * reach, slot, slot, (c, k, z + 1)))
            sends.append((outer & (z2 >= z) & (z >= 1),
                          5 + 2 * reach, slot, slot, (c, k, z - 1)))
        sends.append((need(1 - k, z, d, k, z2), 3 + reach + d, slot, slot, (c, 1 - k, z)))
        return sends

    def each(kind, sends, z2, finish=False):
        for wanted, path, source_slot, target_slot, target in sends:
            @pl.when(wanted)
            def _():
                moved = copy(kind, path, source_slot, target_slot, z2, device(kind, *target))
                if finish:
                    moved.wait_send()
                else:
                    moved.start()

    def await_block(kind, slot, z2):
        c, k, z = view(kind)
        copy(kind, 0, slot, slot, z2, device(kind, c, 1 - k, z)).wait_recv()

    own = []
    for kind, ref in ((0, text_ref), (1, image_ref)):
        _, k, z = view(kind)
        loaded = pltpu.make_async_copy(ref, held.at[kind, k, z], local_sem.at[kind])
        loaded.start()
        own.append(loaded)

    barrier = pltpu.get_barrier_semaphore()

    def greet(target):
        pl.semaphore_signal(barrier, inc=1, device_id=target, device_id_type=MESH)

    greet((2 * chip + 1 - core, grp))
    if relayed:
        partners = [chip + 1 - 2 * (chip % 2), (chip + 2) % 4]
    else:
        partners = [(chip + d + chips) % chips for d in range(-reach, reach + 1) if d]
    for partner in partners:
        greet((2 * partner + core, grp))

    @pl.when(grp > 0)
    def _():
        greet((blk, grp - 1))

    @pl.when(grp < depth - 1)
    def _():
        greet((blk, grp + 1))

    for loaded in own:
        loaded.wait()
    pl.semaphore_wait(
        barrier,
        1 + len(partners) + (grp > 0).astype(jnp.int32) + (grp < depth - 1).astype(jnp.int32),
    )

    def own_block(kind):
        _, k, z = view(kind)
        return held[kind, k, z]

    def inverse_length(block):
        wide = block.astype(jnp.float32)
        return lax.rsqrt(jnp.sum(wide * wide, axis=-1, keepdims=True) + EPSILON)

    rows = held.shape[3]

    def tile(kind, slot, z2):
        _, k, z = view(kind)
        other = held[kind, slot, z2]
        mine = own_block(1 - kind)
        columns = jnp.broadcast_to(inverse_length(other), (rows, rows)).T
        product = lax.dot_general(
            mine, other, (((1,), (1,)), ((), ())), preferred_element_type=jnp.float32
        )
        logits = LOGIT_SCALE * product * own_scale[kind] * columns + BIAS_LOGIT
        inverse = jnp.exp(-logits)
        weights = 1.0 / (1.0 + inverse)
        diagonal = lax.broadcasted_iota(jnp.int32, (rows, rows), 0) == lax.broadcasted_iota(
            jnp.int32, (rows, rows), 1
        )
        first = ((slot == k) & (z2 == z)).astype(jnp.float32)
        positive = jnp.where(diagonal, first, 0.0)
        weights = jnp.where(positive > 0.5, -inverse * weights, weights)
        scaled = (weights * columns).astype(jnp.bfloat16)
        total[kind] += jnp.dot(scaled, other, preferred_element_type=jnp.float32)

    def position(kind, sign, distance):
        _, _, z = view(kind)
        z2 = z + sign * distance
        valid = (z2 >= 0) & (z2 < depth) & (distance >= 0)
        return z2, valid & ((sign > 0) | (distance > 0))

    def prepare(kind, carry):
        total[kind] = jnp.zeros(total.shape[1:], jnp.float32)
        own_scale[kind] = jnp.broadcast_to(inverse_length(own_block(1 - kind)), (rows, rows))
        return carry

    def start_own(kind):
        _, _, z = view(kind)
        each(kind, own_sends(kind, z), z)

    for kind in kinds:
        start_own(kind)
    lax.fori_loop(0, 2, prepare, 0)

    def half_turn(index, carry):
        turn = index // 2
        kind = first_kind + (index % 2) * (1 - 2 * first_kind)
        _, k, z = view(kind)

        for sign in (1, -1):
            z2, valid = position(kind, sign, turn)

            @pl.when(valid & (turn > 0))
            def _():
                await_block(kind, k, z2)
                each(kind, own_sends(kind, z2), z2)

        def stage(step, carry):
            d = jnp.where(step == 0, reach, jnp.where(step == 1, 0, reach - step + 1))
            distance = turn - (d > 0).astype(jnp.int32)
            for sign in (1, -1):
                z2, valid = position(kind, sign, distance)

                @pl.when((d > 0) & valid & arrives(kind, d, z2))
                def _():
                    await_block(kind, 2 * d + k, z2)
                    each(kind, arrival_sends(kind, d, z2), z2)

            def work(item, carry):
                source_k = (k + item // 2) % 2
                z2, valid = position(kind, 1 - 2 * (item % 2), distance)
                slot = 2 * d + source_k

                @pl.when(valid & need(k, z, d, source_k, z2))
                def _():
                    @pl.when(source_k != k)
                    def _():
                        await_block(kind, slot, z2)

                    tile(kind, slot, z2)

                return carry

            return lax.fori_loop(0, 4, work, carry)

        return lax.fori_loop(0, reach + 1, stage, carry)

    lax.fori_loop(0, 2 * (depth + 1), half_turn, 0)

    for kind, out in ((0, image_out), (1, text_out)):
        scale = own_scale[kind][:, :1]
        unit = own_block(1 - kind).astype(jnp.float32) * scale
        grad = LOGIT_SCALE * total[kind]
        inner = jnp.sum(unit * grad, axis=-1, keepdims=True)
        out[...] = ((grad - unit * inner) * scale).astype(out.dtype)

    def settle(z2, carry):
        for kind in (0, 1):
            each(kind, own_sends(kind, z2), z2, finish=True)
            for d in range(1, reach + 1):
                @pl.when(arrives(kind, d, z2))
                def _():
                    each(kind, arrival_sends(kind, d, z2), z2, finish=True)
        return carry

    lax.fori_loop(0, depth, settle, 0)


def ring_kernel(depth, window, pieces, early, image_ref, text_ref, image_out, text_out,
                raw, img, txt, own_sum, text_sum, sum_out, sum_in, part_out, part_core, part_x, part_y,
                load_sem, img_send, img_recv, txt_send, txt_recv, sum_send, sum_recv,
                part_send, part_recv):
    blk = lax.axis_index("blk")
    z = lax.axis_index("grp")
    chip, core = blk // 2, blk % 2
    odd = chip % 2
    rows = raw.shape[1]
    span = rows // pieces
    tiles = window // depth
    is_end = (z == 0) | (z == depth - 1)
    is_mid = (z > 0) & (z < depth - 1)
    inner = 1 - 2 * (z // 2)
    partner = (2 * chip + 1 - core, z)
    across = (2 * (chip + 1 - 2 * odd) + core, z)
    over = (2 * ((chip + 2) % 4) + core, z)

    def piece(j):
        return pl.ds(pl.multiple_of(j * span, span), span)

    def text_rows(slot, j):
        return pl.ds(pl.multiple_of(slot * rows + j * span, span), span)

    def remote(source, target, send, recv, device):
        return pltpu.make_async_remote_copy(
            src_ref=source, dst_ref=target, send_sem=send, recv_sem=recv,
            device_id=device, device_id_type=MESH,
        )

    def along(sign):
        return blk, jnp.minimum(jnp.maximum(z + sign, 0), depth - 1)

    def image_copy(source_z, sign, j):
        return remote(
            img.at[source_z, piece(j)], img.at[source_z, piece(j)],
            img_send.at[(sign + 1) // 2, source_z, j], img_recv.at[source_z, j],
            along(sign),
        )

    def sum_copy(target_z, sign, j):
        return remote(
            sum_out.at[target_z, piece(j)], sum_in.at[(1 - sign) // 2, target_z, piece(j)],
            sum_send.at[target_z, j], sum_recv.at[(1 - sign) // 2, target_z, j],
            along(sign),
        )

    def text_copy(path, source_slot, target_slot, j, device):
        return remote(
            txt.at[text_rows(source_slot, j)], txt.at[text_rows(target_slot, j)],
            txt_send.at[path, j], txt_recv.at[target_slot, j], device,
        )

    def text_over(j):
        return text_copy(0, 0, 4, j, over)

    def text_across(j):
        return text_copy(1, 4 * odd, 2, j, across)

    def text_core(slot, j):
        return text_copy(2 + slot // 2, slot, slot + 1 - 2 * core, j, partner)

    def part_copy(path, source_slot, target, j, device):
        return remote(
            part_out.at[source_slot, piece(j)], target.at[piece(j)],
            part_send.at[path, j], part_recv.at[path, j], device,
        )

    def part_to_core(index, j):
        return part_copy(index, 2 * index + 1, part_core.at[index], j, partner)

    def part_across(j):
        return part_copy(2, 2, part_x, j, across)

    def part_over(j):
        return part_copy(3, 4, part_y, j, over)

    def loop(count, body):
        def step(j, carry):
            body(j)
            return carry

        lax.fori_loop(0, count, step, 0)

    loads = []
    for kind, ref in ((0, image_ref), (1, text_ref)):
        load = pltpu.make_async_copy(ref, raw.at[kind], load_sem.at[kind])
        load.start()
        loads.append(load)

    barrier = pltpu.get_barrier_semaphore()

    def greet(target):
        pl.semaphore_signal(barrier, inc=1, device_id=target, device_id_type=MESH)

    for target in (partner, across, over):
        greet(target)

    @pl.when(z > 0)
    def _():
        greet((blk, z - 1))

    @pl.when(z < depth - 1)
    def _():
        greet((blk, z + 1))

    def inverse_length(wide):
        return lax.rsqrt(jnp.sum(wide * wide, axis=-1, keepdims=True) + EPSILON)

    def unit_low(kind):
        wide = raw[kind].astype(jnp.float32)
        return (wide * inverse_length(wide)).astype(jnp.bfloat16)

    loads[0].wait()
    img[z] = unit_low(0)
    loads[1].wait()
    txt[pl.ds(0, rows)] = unit_low(1)
    pl.semaphore_wait(
        barrier, 3 + (z > 0).astype(jnp.int32) + (z < depth - 1).astype(jnp.int32)
    )

    @pl.when(is_end)
    def _():
        loop(pieces, lambda j: image_copy(z, inner, j).start())

    @pl.when(is_mid)
    def _():
        def body(j):
            image_copy(z, inner, j).start()

            @pl.when(j < early)
            def _():
                image_copy(z, -inner, j).start()

        loop(pieces, body)

    def text_start(j):
        text_over(j).start()

        @pl.when(odd == 0)
        def _():
            text_across(j).start()

        @pl.when(core == 0)
        def _():
            text_core(0, j).start()

    loop(pieces, text_start)
    text_sum[...] = jnp.zeros(text_sum.shape, jnp.float32)

    lag = 4 if pieces > 4 else pieces

    def first(j):
        @pl.when(is_mid & (j < pieces))
        def _():
            image_copy(z + inner, -inner, j).wait_recv()
            image_copy(z + inner, -inner, j).start()
            image_copy(z - inner, inner, j).wait_recv()
            image_copy(z - inner, inner, j).start()

        @pl.when(j < pieces)
        def _():
            text_copy(0, 0, 4, j, over).wait_recv()

            @pl.when(odd == 1)
            def _():
                text_across(j).start()

            @pl.when(core == 1)
            def _():
                text_core(4, j).start()

        def second(i):
            text_copy(1, 0, 2, i, across).wait_recv()
            text_core(2, i).start()

        @pl.when((odd == 1) & (j < pieces))
        def _():
            second(j)

        @pl.when((odd == 0) & (j >= lag))
        def _():
            second(j - lag)

    loop(pieces + lag, first)

    def text_ready(j):
        text_copy(2, 0, 1, j, partner).wait_recv()
        text_copy(3, 0, 3, j, partner).wait_recv()

    loop(pieces, text_ready)

    def pass_far(low, high):
        far = z + 2 * inner

        def body(j):
            image_copy(far, -inner, low + j).wait_recv()
            image_copy(far, -inner, low + j).start()

        loop(high - low, body)

    def await_image(source_z, low, high):
        loop(high - low, lambda j: image_copy(source_z, -inner, low + j).wait_recv())

    def weigh(index, carry):
        @pl.when(is_mid & (index > 0))
        def _():
            low = (index - 1) * pieces // 4
            high = jnp.where(index == 3, pieces, index * pieces // 4)
            pass_far(low, high)

            @pl.when(index == 3)
            def _():
                loop(pieces - early, lambda j: image_copy(z, -inner, early + j).start())

        @pl.when(is_end & (index == 1))
        def _():
            await_image(z + 2 * inner, 0, pieces)

        @pl.when(is_end & (index == 2))
        def _():
            await_image(z + 3 * inner, 0, pieces)

        @pl.when(is_end & (index == 3))
        def _():
            await_image(z + inner, 0, pieces)

        end_step = (index == 1) * 2 + (index == 2) * 3 + (index == 3) * 1
        mid_step = (index == 1) * 1 - (index == 2) * 1 + (index == 3) * 2
        source = z + inner * jnp.where(is_end, end_step, mid_step)
        start = pl.multiple_of(jnp.where(source < z, rows, 0), rows)
        window_rows = pl.ds(start, tiles * rows)
        texts = txt[window_rows]
        image = img[source]
        product = lax.dot_general(
            image, texts, (((1,), (1,)), ((), ())), preferred_element_type=jnp.float32
        )
        inverse = jnp.exp(-BIAS_LOGIT - LOGIT_SCALE * product)
        weights = 1.0 / (1.0 + inverse)
        shape = (rows, tiles * rows)
        diagonal = lax.broadcasted_iota(jnp.int32, shape, 0) == lax.broadcasted_iota(
            jnp.int32, shape, 1
        )
        positive = jnp.where(diagonal, (index == 0).astype(jnp.float32), 0.0)
        weights = jnp.where(positive > 0.5, -inverse * weights, weights).astype(jnp.bfloat16)
        summed = jnp.dot(weights, texts, preferred_element_type=jnp.float32)
        own_sum[source] = summed

        @pl.when(is_end & (index > 0))
        def _():
            sum_out[source] = own_sum[source].astype(jnp.bfloat16)
            loop(pieces, lambda j: sum_copy(source, inner, j).start())

        text_sum[window_rows] += lax.dot_general(
            weights, image, (((0,), (0,)), ((), ())), preferred_element_type=jnp.float32
        )
        return carry

    lax.fori_loop(0, 4, weigh, 0)

    def relay(target_z, sign, j):
        arrived = sum_in[(1 - sign) // 2, target_z, piece(j)].astype(jnp.float32)
        sum_out[target_z, piece(j)] = (own_sum[target_z, piece(j)] + arrived).astype(jnp.bfloat16)
        sum_copy(target_z, sign, j).start()

    def await_sum(target_z, sign, j):
        sum_copy(target_z, sign, j).wait_recv()

    def part_rows(slot, j):
        return text_sum[text_rows(slot, j)]

    def part_first(j):
        for index in (0, 1):
            part_out[2 * index + 1, piece(j)] = part_rows(2 * index + 1, j).astype(jnp.bfloat16)
            part_to_core(index, j).start()

    def part_second(j):
        for index in (0, 1):
            part_to_core(index, j).wait_recv()
        near = part_core[1 - core, piece(j)].astype(jnp.float32)
        part_out[2, piece(j)] = (part_rows(2, j) + near).astype(jnp.bfloat16)
        part_across(j).start()

        @pl.when(odd == 0)
        def _():
            part_third(j, 0.0)

    def part_third(j, relayed):
        far = part_core[1, piece(j)].astype(jnp.float32)
        far = jnp.where(core == 1, far, 0.0) + relayed
        part_out[4, piece(j)] = (part_rows(4, j) + far).astype(jnp.bfloat16)
        part_over(j).start()

    def part_fourth(j):
        part_across(j).wait_recv()

        @pl.when(odd == 1)
        def _():
            part_third(j, part_x[piece(j)].astype(jnp.float32))

    loop(pieces, part_first)

    @pl.when(is_mid)
    def _():
        def near(j):
            await_sum(z + inner, inner, j)
            relay(z + inner, inner, j)

        loop(pieces, near)

    loop(pieces, part_second)

    def middle(j):
        part_fourth(j)

        @pl.when(is_mid)
        def _():
            await_sum(z + 2 * inner, inner, j)
            relay(z + 2 * inner, inner, j)

    loop(pieces, middle)

    @pl.when(is_mid)
    def _():
        def outer(j):
            await_sum(z - inner, -inner, j)
            relay(z - inner, -inner, j)

        loop(pieces, outer)

    def finish(kind, out, total, j):
        wide = raw[kind, piece(j)].astype(jnp.float32)
        scale = inverse_length(wide)
        unit = wide * scale
        grad = LOGIT_SCALE * total
        radial = jnp.sum(unit * grad, axis=-1, keepdims=True)
        out[piece(j)] = ((grad - unit * radial) * scale).astype(out.dtype)

    def finish_image(j):
        await_sum(z, -inner, j)
        total = own_sum[z, piece(j)] + sum_in[(1 + inner) // 2, z, piece(j)].astype(jnp.float32)

        @pl.when(is_mid)
        def _():
            await_sum(z, inner, j)

        other = sum_in[(1 - inner) // 2, z, piece(j)].astype(jnp.float32)
        finish(0, image_out, total + jnp.where(is_mid, other, 0.0), j)

    def finish_text(j):
        part_over(j).wait_recv()
        total = part_rows(0, j) + part_y[piece(j)].astype(jnp.float32)
        total += jnp.where(core == 0, part_core[0, piece(j)].astype(jnp.float32), 0.0)
        total += jnp.where(odd == 0, part_x[piece(j)].astype(jnp.float32), 0.0)
        finish(1, text_out, total, j)

    loop(pieces, finish_text)
    loop(pieces, finish_image)

    def settle(j):
        text_over(j).wait_send()
        text_across(j).wait_send()
        text_core(2, j).wait_send()
        part_across(j).wait_send()
        part_over(j).wait_send()
        for index in (0, 1):
            part_to_core(index, j).wait_send()

        @pl.when(core == 0)
        def _():
            text_core(0, j).wait_send()

        @pl.when(core == 1)
        def _():
            text_core(4, j).wait_send()

        image_copy(z, inner, j).wait_send()

        @pl.when(is_mid)
        def _():
            image_copy(z, -inner, j).wait_send()
            image_copy(z + inner, -inner, j).wait_send()
            image_copy(z - inner, inner, j).wait_send()
            image_copy(z + 2 * inner, -inner, j).wait_send()
            for step, sign in ((1, 1), (2, 1), (-1, -1)):
                sum_copy(z + step * inner, sign * inner, j).wait_send()

        @pl.when(is_end)
        def _():
            for step in (1, 2, 3):
                sum_copy(z + step * inner, inner, j).wait_send()

    loop(pieces, settle)


def square_call(depth, window, image_embeds, text_embeds, shape):
    rows, width = image_embeds.shape
    slots = window // depth + 1
    pieces = rows // PIECE_ROWS
    early = pieces // 2
    low, wide = jnp.bfloat16, jnp.float32
    return pl.pallas_call(
        functools.partial(ring_kernel, depth, window, pieces, early),
        out_shape=(shape, shape),
        in_specs=[pl.BlockSpec(memory_space=pl.ANY)] * 2,
        out_specs=(pl.BlockSpec(memory_space=pltpu.VMEM),) * 2,
        scratch_shapes=[
            pltpu.VMEM((2, rows, width), low),
            pltpu.VMEM((depth, rows, width), low),
            pltpu.VMEM((slots * rows, width), low),
            pltpu.VMEM((depth, rows, width), wide),
            pltpu.VMEM((slots * rows, width), wide),
            pltpu.VMEM((depth, rows, width), low),
            pltpu.VMEM((2, depth, rows, width), low),
            pltpu.VMEM((slots, rows, width), low),
            pltpu.VMEM((2, rows, width), low),
            pltpu.VMEM((rows, width), low),
            pltpu.VMEM((rows, width), low),
            pltpu.SemaphoreType.DMA((2,)),
            pltpu.SemaphoreType.DMA((2, depth, pieces)),
            pltpu.SemaphoreType.DMA((depth, pieces)),
            pltpu.SemaphoreType.DMA((5, pieces)),
            pltpu.SemaphoreType.DMA((slots, pieces)),
            pltpu.SemaphoreType.DMA((depth, pieces)),
            pltpu.SemaphoreType.DMA((2, depth, pieces)),
            pltpu.SemaphoreType.DMA((4, pieces)),
            pltpu.SemaphoreType.DMA((4, pieces)),
        ],
        compiler_params=pltpu.CompilerParams(collective_id=0, has_side_effects=True),
    )(image_embeds, text_embeds)


def solution(mesh):
    cycle, depth = mesh.shape["blk"], mesh.shape["grp"]
    window = min(20, cycle * depth // 2)
    chips = cycle // 2
    reach = 1
    while (2 * reach + 1) * depth - (depth - 1) < window:
        reach += 1
    slots = 2 * (reach + 1)

    def per_device(image_embeds, text_embeds):
        rows, width = image_embeds.shape
        shape = jax.ShapeDtypeStruct((rows, width), jnp.bfloat16)
        if chips == 4 and depth == 4 and window == 4 * depth:
            return square_call(depth, window, image_embeds, text_embeds, shape)
        return pl.pallas_call(
            functools.partial(kernel, chips, depth, reach, window),
            out_shape=(shape, shape),
            in_specs=[pl.BlockSpec(memory_space=pl.ANY)] * 2,
            out_specs=(pl.BlockSpec(memory_space=pltpu.VMEM),) * 2,
            scratch_shapes=[
                pltpu.VMEM((2, slots, depth, rows, width), jnp.bfloat16),
                pltpu.VMEM((2, rows, width), jnp.float32),
                pltpu.VMEM((2, rows, rows), jnp.float32),
                pltpu.SemaphoreType.DMA((2,)),
                pltpu.SemaphoreType.DMA((2, 6 + 2 * reach, depth)),
                pltpu.SemaphoreType.DMA((2, slots, depth)),
            ],
            compiler_params=pltpu.CompilerParams(collective_id=0, has_side_effects=True),
        )(image_embeds, text_embeds)

    placed = P(("blk", "grp"), None)
    return jax.shard_map(
        per_device, mesh=mesh, in_specs=(placed, placed), out_specs=(placed, placed), check_vma=False
    )
```

```python
import functools

import jax
import jax.numpy as jnp
from jax import lax
from jax.experimental import pallas as pl
from jax.experimental.pallas import tpu as pltpu
from jax.sharding import PartitionSpec as P

LOGIT_SCALE = 10.0
BIAS_LOGIT = -2.0
EPSILON = 1e-06
PIECE_ROWS = 32
MESH = pl.DeviceIdType.MESH


def kernel(chips, depth, reach, window, image_ref, text_ref, image_out, text_out,
           held, total, own_scale, local_sem, send_sem, recv_sem):
    blk = lax.axis_index("blk")
    grp = lax.axis_index("grp")
    chip, core = blk // 2, blk % 2
    relayed = chips == 4 and reach == 2 and 4 * depth - 1 < window

    def view(kind):
        return (
            chip + kind * (chips - 1 - 2 * chip),
            core + kind * (1 - 2 * core),
            grp + kind * (depth - 1 - 2 * grp),
        )

    def device(kind, c, k, z):
        c = (c + chips) % chips
        linear = 2 * c + k
        return (
            linear + kind * (2 * chips - 1 - 2 * linear),
            z + kind * (depth - 1 - 2 * z),
        )

    first_kind = 1 - chip % 2 if relayed else 0
    kinds = (first_kind, 1 - first_kind)

    def need(k, z, d, source_k, source_z):
        offset = (2 * d + k - source_k) * depth + z - source_z
        return (offset >= 0) & (offset < window)

    def chip_need(z, d, source_k, source_z):
        return need(0, z, d, source_k, source_z) | need(1, z, d, source_k, source_z)

    def arrives(kind, d, source_z):
        c, k, z = view(kind)
        wanted = chip_need(z, d, k, source_z)
        if relayed:
            wanted = wanted | ((d == 2) & (c % 2 == 1))
        return wanted

    def copy(kind, path, source_slot, target_slot, z, target):
        return pltpu.make_async_remote_copy(
            src_ref=held.at[kind, source_slot, z],
            dst_ref=held.at[kind, target_slot, z],
            send_sem=send_sem.at[kind, path, z],
            recv_sem=recv_sem.at[kind, target_slot, z],
            device_id=target,
            device_id_type=MESH,
        )

    def own_sends(kind, z2):
        c, k, z = view(kind)
        sends = [
            ((z2 <= z) & (z + 1 < depth), 0, k, k, (c, k, z + 1)),
            ((z2 >= z) & (z >= 1), 1, k, k, (c, k, z - 1)),
        ]
        for d in range(1, reach + 1):
            wanted = chip_need(z, d, k, z2)
            if relayed and d == 1:
                inside = (z2 > 0) & (z2 < depth - 1)
                wanted = (c % 2 == 0) & (inside | (z2 == z))
            if relayed and d == 2:
                wanted = wanted | (c % 2 == 1)
            sends.append((wanted, 1 + d, k, 2 * d + k, (c + d, k, z)))
        sends.append((need(1 - k, z, 0, k, z2), 2 + reach, k, k, (c, 1 - k, z)))
        return sends

    def arrival_sends(kind, d, z2):
        c, k, z = view(kind)
        sends = []
        slot = 2 * d + k
        if relayed:
            sends.append(((c % 2 == 1) & (d == 2), 3 + reach, slot, 2 + k, (c - 1, k, z)))
            outer = (c % 2 == 1) & (d == 1) & ((z2 == 0) | (z2 == depth - 1))
            sends.append((outer & (z2 <= z) & (z + 1 < depth),
                          4 + 2 * reach, slot, slot, (c, k, z + 1)))
            sends.append((outer & (z2 >= z) & (z >= 1),
                          5 + 2 * reach, slot, slot, (c, k, z - 1)))
        sends.append((need(1 - k, z, d, k, z2), 3 + reach + d, slot, slot, (c, 1 - k, z)))
        return sends

    def each(kind, sends, z2, finish=False):
        for wanted, path, source_slot, target_slot, target in sends:
            @pl.when(wanted)
            def _():
                moved = copy(kind, path, source_slot, target_slot, z2, device(kind, *target))
                if finish:
                    moved.wait_send()
                else:
                    moved.start()

    def await_block(kind, slot, z2):
        c, k, z = view(kind)
        copy(kind, 0, slot, slot, z2, device(kind, c, 1 - k, z)).wait_recv()

    own = []
    for kind, ref in ((0, text_ref), (1, image_ref)):
        _, k, z = view(kind)
        loaded = pltpu.make_async_copy(ref, held.at[kind, k, z], local_sem.at[kind])
        loaded.start()
        own.append(loaded)

    barrier = pltpu.get_barrier_semaphore()

    def greet(target):
        pl.semaphore_signal(barrier, inc=1, device_id=target, device_id_type=MESH)

    greet((2 * chip + 1 - core, grp))
    if relayed:
        partners = [chip + 1 - 2 * (chip % 2), (chip + 2) % 4]
    else:
        partners = [(chip + d + chips) % chips for d in range(-reach, reach + 1) if d]
    for partner in partners:
        greet((2 * partner + core, grp))

    @pl.when(grp > 0)
    def _():
        greet((blk, grp - 1))

    @pl.when(grp < depth - 1)
    def _():
        greet((blk, grp + 1))

    for loaded in own:
        loaded.wait()
    pl.semaphore_wait(
        barrier,
        1 + len(partners) + (grp > 0).astype(jnp.int32) + (grp < depth - 1).astype(jnp.int32),
    )

    def own_block(kind):
        _, k, z = view(kind)
        return held[kind, k, z]

    def inverse_length(block):
        wide = block.astype(jnp.float32)
        return lax.rsqrt(jnp.sum(wide * wide, axis=-1, keepdims=True) + EPSILON)

    rows = held.shape[3]

    def tile(kind, slot, z2):
        _, k, z = view(kind)
        other = held[kind, slot, z2]
        mine = own_block(1 - kind)
        columns = jnp.broadcast_to(inverse_length(other), (rows, rows)).T
        product = lax.dot_general(
            mine, other, (((1,), (1,)), ((), ())), preferred_element_type=jnp.float32
        )
        logits = LOGIT_SCALE * product * own_scale[kind] * columns + BIAS_LOGIT
        inverse = jnp.exp(-logits)
        weights = 1.0 / (1.0 + inverse)
        diagonal = lax.broadcasted_iota(jnp.int32, (rows, rows), 0) == lax.broadcasted_iota(
            jnp.int32, (rows, rows), 1
        )
        first = ((slot == k) & (z2 == z)).astype(jnp.float32)
        positive = jnp.where(diagonal, first, 0.0)
        weights = jnp.where(positive > 0.5, -inverse * weights, weights)
        scaled = (weights * columns).astype(jnp.bfloat16)
        total[kind] += jnp.dot(scaled, other, preferred_element_type=jnp.float32)

    def position(kind, sign, distance):
        _, _, z = view(kind)
        z2 = z + sign * distance
        valid = (z2 >= 0) & (z2 < depth) & (distance >= 0)
        return z2, valid & ((sign > 0) | (distance > 0))

    def prepare(kind, carry):
        total[kind] = jnp.zeros(total.shape[1:], jnp.float32)
        own_scale[kind] = jnp.broadcast_to(inverse_length(own_block(1 - kind)), (rows, rows))
        return carry

    def start_own(kind):
        _, _, z = view(kind)
        each(kind, own_sends(kind, z), z)

    for kind in kinds:
        start_own(kind)
    lax.fori_loop(0, 2, prepare, 0)

    def half_turn(index, carry):
        turn = index // 2
        kind = first_kind + (index % 2) * (1 - 2 * first_kind)
        _, k, z = view(kind)

        for sign in (1, -1):
            z2, valid = position(kind, sign, turn)

            @pl.when(valid & (turn > 0))
            def _():
                await_block(kind, k, z2)
                each(kind, own_sends(kind, z2), z2)

        def stage(step, carry):
            d = jnp.where(step == 0, reach, jnp.where(step == 1, 0, reach - step + 1))
            distance = turn - (d > 0).astype(jnp.int32)
            for sign in (1, -1):
                z2, valid = position(kind, sign, distance)

                @pl.when((d > 0) & valid & arrives(kind, d, z2))
                def _():
                    await_block(kind, 2 * d + k, z2)
                    each(kind, arrival_sends(kind, d, z2), z2)

            def work(item, carry):
                source_k = (k + item // 2) % 2
                z2, valid = position(kind, 1 - 2 * (item % 2), distance)
                slot = 2 * d + source_k

                @pl.when(valid & need(k, z, d, source_k, z2))
                def _():
                    @pl.when(source_k != k)
                    def _():
                        await_block(kind, slot, z2)

                    tile(kind, slot, z2)

                return carry

            return lax.fori_loop(0, 4, work, carry)

        return lax.fori_loop(0, reach + 1, stage, carry)

    lax.fori_loop(0, 2 * (depth + 1), half_turn, 0)

    for kind, out in ((0, image_out), (1, text_out)):
        scale = own_scale[kind][:, :1]
        unit = own_block(1 - kind).astype(jnp.float32) * scale
        grad = LOGIT_SCALE * total[kind]
        inner = jnp.sum(unit * grad, axis=-1, keepdims=True)
        out[...] = ((grad - unit * inner) * scale).astype(out.dtype)

    def settle(z2, carry):
        for kind in (0, 1):
            each(kind, own_sends(kind, z2), z2, finish=True)
            for d in range(1, reach + 1):
                @pl.when(arrives(kind, d, z2))
                def _():
                    each(kind, arrival_sends(kind, d, z2), z2, finish=True)
        return carry

    lax.fori_loop(0, depth, settle, 0)


def ring_kernel(depth, window, pieces, early, image_ref, text_ref, image_out, text_out,
                raw, img, txt, own_sum, text_sum, sum_out, sum_in, part_out, part_core, part_x, part_y,
                load_sem, img_send, img_recv, txt_send, txt_recv, sum_send, sum_recv,
                part_send, part_recv):
    blk = lax.axis_index("blk")
    z = lax.axis_index("grp")
    chip, core = blk // 2, blk % 2
    odd = chip % 2
    rows = raw.shape[1]
    span = rows // pieces
    tiles = window // depth
    is_end = (z == 0) | (z == depth - 1)
    is_mid = (z > 0) & (z < depth - 1)
    inner = 1 - 2 * (z // 2)
    partner = (2 * chip + 1 - core, z)
    across = (2 * (chip + 1 - 2 * odd) + core, z)
    over = (2 * ((chip + 2) % 4) + core, z)

    def piece(j):
        return pl.ds(pl.multiple_of(j * span, span), span)

    def text_rows(slot, j):
        return pl.ds(pl.multiple_of(slot * rows + j * span, span), span)

    def remote(source, target, send, recv, device):
        return pltpu.make_async_remote_copy(
            src_ref=source, dst_ref=target, send_sem=send, recv_sem=recv,
            device_id=device, device_id_type=MESH,
        )

    def along(sign):
        return blk, jnp.minimum(jnp.maximum(z + sign, 0), depth - 1)

    def image_copy(source_z, sign, j):
        return remote(
            img.at[source_z, piece(j)], img.at[source_z, piece(j)],
            img_send.at[(sign + 1) // 2, source_z, j], img_recv.at[source_z, j],
            along(sign),
        )

    def sum_copy(target_z, sign, j):
        return remote(
            sum_out.at[target_z, piece(j)], sum_in.at[(1 - sign) // 2, target_z, piece(j)],
            sum_send.at[target_z, j], sum_recv.at[(1 - sign) // 2, target_z, j],
            along(sign),
        )

    def text_copy(path, source_slot, target_slot, j, device):
        return remote(
            txt.at[text_rows(source_slot, j)], txt.at[text_rows(target_slot, j)],
            txt_send.at[path, j], txt_recv.at[target_slot, j], device,
        )

    def text_over(j):
        return text_copy(0, 0, 4, j, over)

    def text_across(j):
        return text_copy(1, 4 * odd, 2, j, across)

    def text_core(slot, j):
        return text_copy(2 + slot // 2, slot, slot + 1 - 2 * core, j, partner)

    def part_copy(path, source_slot, target, j, device):
        return remote(
            part_out.at[source_slot, piece(j)], target.at[piece(j)],
            part_send.at[path, j], part_recv.at[path, j], device,
        )

    def part_to_core(index, j):
        return part_copy(index, 2 * index + 1, part_core.at[index], j, partner)

    def part_across(j):
        return part_copy(2, 2, part_x, j, across)

    def part_over(j):
        return part_copy(3, 4, part_y, j, over)

    def loop(count, body):
        def step(j, carry):
            body(j)
            return carry

        lax.fori_loop(0, count, step, 0)

    loads = []
    for kind, ref in ((0, image_ref), (1, text_ref)):
        load = pltpu.make_async_copy(ref, raw.at[kind], load_sem.at[kind])
        load.start()
        loads.append(load)

    barrier = pltpu.get_barrier_semaphore()

    def greet(target):
        pl.semaphore_signal(barrier, inc=1, device_id=target, device_id_type=MESH)

    for target in (partner, across, over):
        greet(target)

    @pl.when(z > 0)
    def _():
        greet((blk, z - 1))

    @pl.when(z < depth - 1)
    def _():
        greet((blk, z + 1))

    def inverse_length(wide):
        return lax.rsqrt(jnp.sum(wide * wide, axis=-1, keepdims=True) + EPSILON)

    def unit_low(kind):
        wide = raw[kind].astype(jnp.float32)
        return (wide * inverse_length(wide)).astype(jnp.bfloat16)

    loads[0].wait()
    img[z] = unit_low(0)
    loads[1].wait()
    txt[pl.ds(0, rows)] = unit_low(1)
    pl.semaphore_wait(
        barrier, 3 + (z > 0).astype(jnp.int32) + (z < depth - 1).astype(jnp.int32)
    )

    @pl.when(is_end)
    def _():
        loop(pieces, lambda j: image_copy(z, inner, j).start())

    @pl.when(is_mid)
    def _():
        def body(j):
            image_copy(z, inner, j).start()

            @pl.when(j < early)
            def _():
                image_copy(z, -inner, j).start()

        loop(pieces, body)

    def text_start(j):
        text_over(j).start()

        @pl.when(odd == 0)
        def _():
            text_across(j).start()

        @pl.when(core == 0)
        def _():
            text_core(0, j).start()

    loop(pieces, text_start)
    text_sum[...] = jnp.zeros(text_sum.shape, jnp.float32)

    lag = pieces

    def pass_image(source_z, sign, j):
        image_copy(source_z, sign, j).wait_recv()
        image_copy(source_z, sign, j).start()

    def first(j):
        @pl.when(j < pieces)
        def _():
            text_copy(0, 0, 4, j, over).wait_recv()

            @pl.when(odd == 1)
            def _():
                text_across(j).start()

            @pl.when(core == 1)
            def _():
                text_core(4, j).start()

        def second(i):
            text_copy(1, 0, 2, i, across).wait_recv()
            text_core(2, i).start()

        @pl.when((odd == 1) & (j < pieces))
        def _():
            second(j)

        @pl.when(is_mid & (j < pieces))
        def _():
            pass_image(z + inner, -inner, j)
            pass_image(z - inner, inner, j)

        @pl.when((odd == 0) & (j >= lag))
        def _():
            second(j - lag)

        @pl.when(is_mid & (j >= pieces))
        def _():
            pass_image(z + 2 * inner, -inner, j - pieces)

    loop(pieces + lag, first)

    def text_ready(j):
        text_copy(2, 0, 1, j, partner).wait_recv()
        text_copy(3, 0, 3, j, partner).wait_recv()

    loop(pieces, text_ready)

    def await_image(source_z, low, high):
        loop(high - low, lambda j: image_copy(source_z, -inner, low + j).wait_recv())

    def weigh(index, carry):
        @pl.when(is_mid)
        def _():
            low = lag + (pieces - lag) * index // 4
            high = lag + (pieces - lag) * (index + 1) // 4
            loop(high - low, lambda j: pass_image(z + 2 * inner, -inner, low + j))

            @pl.when(index == 3)
            def _():
                loop(pieces - early, lambda j: image_copy(z, -inner, early + j).start())

        @pl.when(is_end & (index == 1))
        def _():
            await_image(z + 2 * inner, 0, pieces)

        @pl.when(is_end & (index == 2))
        def _():
            await_image(z + 3 * inner, 0, pieces)

        @pl.when(is_end & (index == 3))
        def _():
            await_image(z + inner, 0, pieces)

        end_step = (index == 1) * 2 + (index == 2) * 3 + (index == 3) * 1
        mid_step = (index == 1) * 1 - (index == 2) * 1 + (index == 3) * 2
        source = z + inner * jnp.where(is_end, end_step, mid_step)
        start = pl.multiple_of(jnp.where(source < z, rows, 0), rows)
        window_rows = pl.ds(start, tiles * rows)
        texts = txt[window_rows]
        image = img[source]
        product = lax.dot_general(
            image, texts, (((1,), (1,)), ((), ())), preferred_element_type=jnp.float32
        )
        inverse = jnp.exp(-BIAS_LOGIT - LOGIT_SCALE * product)
        weights = 1.0 / (1.0 + inverse)
        shape = (rows, tiles * rows)
        diagonal = lax.broadcasted_iota(jnp.int32, shape, 0) == lax.broadcasted_iota(
            jnp.int32, shape, 1
        )
        positive = jnp.where(diagonal, (index == 0).astype(jnp.float32), 0.0)
        weights = jnp.where(positive > 0.5, -inverse * weights, weights).astype(jnp.bfloat16)
        summed = jnp.dot(weights, texts, preferred_element_type=jnp.float32)
        own_sum[source] = summed

        @pl.when(is_end & (index > 0))
        def _():
            sum_out[source] = own_sum[source].astype(jnp.bfloat16)
            loop(pieces, lambda j: sum_copy(source, inner, j).start())

        text_sum[window_rows] += lax.dot_general(
            weights, image, (((0,), (0,)), ((), ())), preferred_element_type=jnp.float32
        )
        return carry

    lax.fori_loop(0, 4, weigh, 0)

    def relay(target_z, sign, j):
        arrived = sum_in[(1 - sign) // 2, target_z, piece(j)].astype(jnp.float32)
        sum_out[target_z, piece(j)] = (own_sum[target_z, piece(j)] + arrived).astype(jnp.bfloat16)
        sum_copy(target_z, sign, j).start()

    def await_sum(target_z, sign, j):
        sum_copy(target_z, sign, j).wait_recv()

    def part_rows(slot, j):
        return text_sum[text_rows(slot, j)]

    def part_first(j):
        for index in (0, 1):
            part_out[2 * index + 1, piece(j)] = part_rows(2 * index + 1, j).astype(jnp.bfloat16)
            part_to_core(index, j).start()

    def part_second(j):
        for index in (0, 1):
            part_to_core(index, j).wait_recv()
        near = part_core[1 - core, piece(j)].astype(jnp.float32)
        part_out[2, piece(j)] = (part_rows(2, j) + near).astype(jnp.bfloat16)
        part_across(j).start()

        @pl.when(odd == 0)
        def _():
            part_third(j, 0.0)

    def part_third(j, relayed):
        far = part_core[1, piece(j)].astype(jnp.float32)
        far = jnp.where(core == 1, far, 0.0) + relayed
        part_out[4, piece(j)] = (part_rows(4, j) + far).astype(jnp.bfloat16)
        part_over(j).start()

    def part_fourth(j):
        part_across(j).wait_recv()

        @pl.when(odd == 1)
        def _():
            part_third(j, part_x[piece(j)].astype(jnp.float32))

    loop(pieces, part_first)

    @pl.when(is_mid)
    def _():
        def near(j):
            await_sum(z + inner, inner, j)
            relay(z + inner, inner, j)

        loop(pieces, near)

    loop(pieces, part_second)

    def middle(j):
        part_fourth(j)

        @pl.when(is_mid)
        def _():
            await_sum(z + 2 * inner, inner, j)
            relay(z + 2 * inner, inner, j)

    loop(pieces, middle)

    @pl.when(is_mid)
    def _():
        def outer(j):
            await_sum(z - inner, -inner, j)
            relay(z - inner, -inner, j)

        loop(pieces, outer)

    def finish(kind, out, total, j):
        wide = raw[kind, piece(j)].astype(jnp.float32)
        scale = inverse_length(wide)
        unit = wide * scale
        grad = LOGIT_SCALE * total
        radial = jnp.sum(unit * grad, axis=-1, keepdims=True)
        out[piece(j)] = ((grad - unit * radial) * scale).astype(out.dtype)

    def finish_image(j):
        await_sum(z, -inner, j)
        total = own_sum[z, piece(j)] + sum_in[(1 + inner) // 2, z, piece(j)].astype(jnp.float32)

        @pl.when(is_mid)
        def _():
            await_sum(z, inner, j)

        other = sum_in[(1 - inner) // 2, z, piece(j)].astype(jnp.float32)
        finish(0, image_out, total + jnp.where(is_mid, other, 0.0), j)

    def finish_text(j):
        part_over(j).wait_recv()
        total = part_rows(0, j) + part_y[piece(j)].astype(jnp.float32)
        total += jnp.where(core == 0, part_core[0, piece(j)].astype(jnp.float32), 0.0)
        total += jnp.where(odd == 0, part_x[piece(j)].astype(jnp.float32), 0.0)
        finish(1, text_out, total, j)

    loop(pieces, finish_text)
    loop(pieces, finish_image)

    def settle(j):
        text_over(j).wait_send()
        text_across(j).wait_send()
        text_core(2, j).wait_send()
        part_across(j).wait_send()
        part_over(j).wait_send()
        for index in (0, 1):
            part_to_core(index, j).wait_send()

        @pl.when(core == 0)
        def _():
            text_core(0, j).wait_send()

        @pl.when(core == 1)
        def _():
            text_core(4, j).wait_send()

        image_copy(z, inner, j).wait_send()

        @pl.when(is_mid)
        def _():
            image_copy(z, -inner, j).wait_send()
            image_copy(z + inner, -inner, j).wait_send()
            image_copy(z - inner, inner, j).wait_send()
            image_copy(z + 2 * inner, -inner, j).wait_send()
            for step, sign in ((1, 1), (2, 1), (-1, -1)):
                sum_copy(z + step * inner, sign * inner, j).wait_send()

        @pl.when(is_end)
        def _():
            for step in (1, 2, 3):
                sum_copy(z + step * inner, inner, j).wait_send()

    loop(pieces, settle)


def square_call(depth, window, image_embeds, text_embeds, shape):
    rows, width = image_embeds.shape
    slots = window // depth + 1
    pieces = rows // PIECE_ROWS
    early = 3 * pieces // 4
    low, wide = jnp.bfloat16, jnp.float32
    return pl.pallas_call(
        functools.partial(ring_kernel, depth, window, pieces, early),
        out_shape=(pltpu.VMEM(shape.shape, shape.dtype),) * 2,
        in_specs=[pl.BlockSpec(memory_space=pl.ANY)] * 2,
        out_specs=(pl.BlockSpec(memory_space=pltpu.VMEM),) * 2,
        scratch_shapes=[
            pltpu.VMEM((2, rows, width), low),
            pltpu.VMEM((depth, rows, width), low),
            pltpu.VMEM((slots * rows, width), low),
            pltpu.VMEM((depth, rows, width), wide),
            pltpu.VMEM((slots * rows, width), wide),
            pltpu.VMEM((depth, rows, width), low),
            pltpu.VMEM((2, depth, rows, width), low),
            pltpu.VMEM((slots, rows, width), low),
            pltpu.VMEM((2, rows, width), low),
            pltpu.VMEM((rows, width), low),
            pltpu.VMEM((rows, width), low),
            pltpu.SemaphoreType.DMA((2,)),
            pltpu.SemaphoreType.DMA((2, depth, pieces)),
            pltpu.SemaphoreType.DMA((depth, pieces)),
            pltpu.SemaphoreType.DMA((5, pieces)),
            pltpu.SemaphoreType.DMA((slots, pieces)),
            pltpu.SemaphoreType.DMA((depth, pieces)),
            pltpu.SemaphoreType.DMA((2, depth, pieces)),
            pltpu.SemaphoreType.DMA((4, pieces)),
            pltpu.SemaphoreType.DMA((4, pieces)),
        ],
        compiler_params=pltpu.CompilerParams(collective_id=0, has_side_effects=True),
    )(image_embeds, text_embeds)


def solution(mesh):
    cycle, depth = mesh.shape["blk"], mesh.shape["grp"]
    window = min(20, cycle * depth // 2)
    chips = cycle // 2
    reach = 1
    while (2 * reach + 1) * depth - (depth - 1) < window:
        reach += 1
    slots = 2 * (reach + 1)

    def per_device(image_embeds, text_embeds):
        rows, width = image_embeds.shape
        shape = jax.ShapeDtypeStruct((rows, width), jnp.bfloat16)
        if chips == 4 and depth == 4 and window == 4 * depth:
            return square_call(depth, window, image_embeds, text_embeds, shape)
        return pl.pallas_call(
            functools.partial(kernel, chips, depth, reach, window),
            out_shape=(shape, shape),
            in_specs=[pl.BlockSpec(memory_space=pl.ANY)] * 2,
            out_specs=(pl.BlockSpec(memory_space=pltpu.VMEM),) * 2,
            scratch_shapes=[
                pltpu.VMEM((2, slots, depth, rows, width), jnp.bfloat16),
                pltpu.VMEM((2, rows, width), jnp.float32),
                pltpu.VMEM((2, rows, rows), jnp.float32),
                pltpu.SemaphoreType.DMA((2,)),
                pltpu.SemaphoreType.DMA((2, 6 + 2 * reach, depth)),
                pltpu.SemaphoreType.DMA((2, slots, depth)),
            ],
            compiler_params=pltpu.CompilerParams(collective_id=0, has_side_effects=True),
        )(image_embeds, text_embeds)

    placed = P(("blk", "grp"), None)
    return jax.shard_map(
        per_device, mesh=mesh, in_specs=(placed, placed), out_specs=(placed, placed), check_vma=False
    )
```

```python
import functools

import jax
import jax.numpy as jnp
from jax import lax
from jax.experimental import pallas as pl
from jax.experimental.pallas import tpu as pltpu
from jax.sharding import PartitionSpec as P

LOGIT_SCALE = 10.0
BIAS_LOGIT = -2.0
EPSILON = 1e-06
PIECE_ROWS = 32
MESH = pl.DeviceIdType.MESH


def kernel(chips, depth, reach, window, image_ref, text_ref, image_out, text_out,
           held, total, own_scale, local_sem, send_sem, recv_sem):
    blk = lax.axis_index("blk")
    grp = lax.axis_index("grp")
    chip, core = blk // 2, blk % 2
    relayed = chips == 4 and reach == 2 and 4 * depth - 1 < window

    def view(kind):
        return (
            chip + kind * (chips - 1 - 2 * chip),
            core + kind * (1 - 2 * core),
            grp + kind * (depth - 1 - 2 * grp),
        )

    def device(kind, c, k, z):
        c = (c + chips) % chips
        linear = 2 * c + k
        return (
            linear + kind * (2 * chips - 1 - 2 * linear),
            z + kind * (depth - 1 - 2 * z),
        )

    first_kind = 1 - chip % 2 if relayed else 0
    kinds = (first_kind, 1 - first_kind)

    def need(k, z, d, source_k, source_z):
        offset = (2 * d + k - source_k) * depth + z - source_z
        return (offset >= 0) & (offset < window)

    def chip_need(z, d, source_k, source_z):
        return need(0, z, d, source_k, source_z) | need(1, z, d, source_k, source_z)

    def arrives(kind, d, source_z):
        c, k, z = view(kind)
        wanted = chip_need(z, d, k, source_z)
        if relayed:
            wanted = wanted | ((d == 2) & (c % 2 == 1))
        return wanted

    def copy(kind, path, source_slot, target_slot, z, target):
        return pltpu.make_async_remote_copy(
            src_ref=held.at[kind, source_slot, z],
            dst_ref=held.at[kind, target_slot, z],
            send_sem=send_sem.at[kind, path, z],
            recv_sem=recv_sem.at[kind, target_slot, z],
            device_id=target,
            device_id_type=MESH,
        )

    def own_sends(kind, z2):
        c, k, z = view(kind)
        sends = [
            ((z2 <= z) & (z + 1 < depth), 0, k, k, (c, k, z + 1)),
            ((z2 >= z) & (z >= 1), 1, k, k, (c, k, z - 1)),
        ]
        for d in range(1, reach + 1):
            wanted = chip_need(z, d, k, z2)
            if relayed and d == 1:
                inside = (z2 > 0) & (z2 < depth - 1)
                wanted = (c % 2 == 0) & (inside | (z2 == z))
            if relayed and d == 2:
                wanted = wanted | (c % 2 == 1)
            sends.append((wanted, 1 + d, k, 2 * d + k, (c + d, k, z)))
        sends.append((need(1 - k, z, 0, k, z2), 2 + reach, k, k, (c, 1 - k, z)))
        return sends

    def arrival_sends(kind, d, z2):
        c, k, z = view(kind)
        sends = []
        slot = 2 * d + k
        if relayed:
            sends.append(((c % 2 == 1) & (d == 2), 3 + reach, slot, 2 + k, (c - 1, k, z)))
            outer = (c % 2 == 1) & (d == 1) & ((z2 == 0) | (z2 == depth - 1))
            sends.append((outer & (z2 <= z) & (z + 1 < depth),
                          4 + 2 * reach, slot, slot, (c, k, z + 1)))
            sends.append((outer & (z2 >= z) & (z >= 1),
                          5 + 2 * reach, slot, slot, (c, k, z - 1)))
        sends.append((need(1 - k, z, d, k, z2), 3 + reach + d, slot, slot, (c, 1 - k, z)))
        return sends

    def each(kind, sends, z2, finish=False):
        for wanted, path, source_slot, target_slot, target in sends:
            @pl.when(wanted)
            def _():
                moved = copy(kind, path, source_slot, target_slot, z2, device(kind, *target))
                if finish:
                    moved.wait_send()
                else:
                    moved.start()

    def await_block(kind, slot, z2):
        c, k, z = view(kind)
        copy(kind, 0, slot, slot, z2, device(kind, c, 1 - k, z)).wait_recv()

    own = []
    for kind, ref in ((0, text_ref), (1, image_ref)):
        _, k, z = view(kind)
        loaded = pltpu.make_async_copy(ref, held.at[kind, k, z], local_sem.at[kind])
        loaded.start()
        own.append(loaded)

    barrier = pltpu.get_barrier_semaphore()

    def greet(target):
        pl.semaphore_signal(barrier, inc=1, device_id=target, device_id_type=MESH)

    greet((2 * chip + 1 - core, grp))
    if relayed:
        partners = [chip + 1 - 2 * (chip % 2), (chip + 2) % 4]
    else:
        partners = [(chip + d + chips) % chips for d in range(-reach, reach + 1) if d]
    for partner in partners:
        greet((2 * partner + core, grp))

    @pl.when(grp > 0)
    def _():
        greet((blk, grp - 1))

    @pl.when(grp < depth - 1)
    def _():
        greet((blk, grp + 1))

    for loaded in own:
        loaded.wait()
    pl.semaphore_wait(
        barrier,
        1 + len(partners) + (grp > 0).astype(jnp.int32) + (grp < depth - 1).astype(jnp.int32),
    )

    def own_block(kind):
        _, k, z = view(kind)
        return held[kind, k, z]

    def inverse_length(block):
        wide = block.astype(jnp.float32)
        return lax.rsqrt(jnp.sum(wide * wide, axis=-1, keepdims=True) + EPSILON)

    rows = held.shape[3]

    def tile(kind, slot, z2):
        _, k, z = view(kind)
        other = held[kind, slot, z2]
        mine = own_block(1 - kind)
        columns = jnp.broadcast_to(inverse_length(other), (rows, rows)).T
        product = lax.dot_general(
            mine, other, (((1,), (1,)), ((), ())), preferred_element_type=jnp.float32
        )
        logits = LOGIT_SCALE * product * own_scale[kind] * columns + BIAS_LOGIT
        inverse = jnp.exp(-logits)
        weights = 1.0 / (1.0 + inverse)
        diagonal = lax.broadcasted_iota(jnp.int32, (rows, rows), 0) == lax.broadcasted_iota(
            jnp.int32, (rows, rows), 1
        )
        first = ((slot == k) & (z2 == z)).astype(jnp.float32)
        positive = jnp.where(diagonal, first, 0.0)
        weights = jnp.where(positive > 0.5, -inverse * weights, weights)
        scaled = (weights * columns).astype(jnp.bfloat16)
        total[kind] += jnp.dot(scaled, other, preferred_element_type=jnp.float32)

    def position(kind, sign, distance):
        _, _, z = view(kind)
        z2 = z + sign * distance
        valid = (z2 >= 0) & (z2 < depth) & (distance >= 0)
        return z2, valid & ((sign > 0) | (distance > 0))

    def prepare(kind, carry):
        total[kind] = jnp.zeros(total.shape[1:], jnp.float32)
        own_scale[kind] = jnp.broadcast_to(inverse_length(own_block(1 - kind)), (rows, rows))
        return carry

    def start_own(kind):
        _, _, z = view(kind)
        each(kind, own_sends(kind, z), z)

    for kind in kinds:
        start_own(kind)
    lax.fori_loop(0, 2, prepare, 0)

    def half_turn(index, carry):
        turn = index // 2
        kind = first_kind + (index % 2) * (1 - 2 * first_kind)
        _, k, z = view(kind)

        for sign in (1, -1):
            z2, valid = position(kind, sign, turn)

            @pl.when(valid & (turn > 0))
            def _():
                await_block(kind, k, z2)
                each(kind, own_sends(kind, z2), z2)

        def stage(step, carry):
            d = jnp.where(step == 0, reach, jnp.where(step == 1, 0, reach - step + 1))
            distance = turn - (d > 0).astype(jnp.int32)
            for sign in (1, -1):
                z2, valid = position(kind, sign, distance)

                @pl.when((d > 0) & valid & arrives(kind, d, z2))
                def _():
                    await_block(kind, 2 * d + k, z2)
                    each(kind, arrival_sends(kind, d, z2), z2)

            def work(item, carry):
                source_k = (k + item // 2) % 2
                z2, valid = position(kind, 1 - 2 * (item % 2), distance)
                slot = 2 * d + source_k

                @pl.when(valid & need(k, z, d, source_k, z2))
                def _():
                    @pl.when(source_k != k)
                    def _():
                        await_block(kind, slot, z2)

                    tile(kind, slot, z2)

                return carry

            return lax.fori_loop(0, 4, work, carry)

        return lax.fori_loop(0, reach + 1, stage, carry)

    lax.fori_loop(0, 2 * (depth + 1), half_turn, 0)

    for kind, out in ((0, image_out), (1, text_out)):
        scale = own_scale[kind][:, :1]
        unit = own_block(1 - kind).astype(jnp.float32) * scale
        grad = LOGIT_SCALE * total[kind]
        inner = jnp.sum(unit * grad, axis=-1, keepdims=True)
        out[...] = ((grad - unit * inner) * scale).astype(out.dtype)

    def settle(z2, carry):
        for kind in (0, 1):
            each(kind, own_sends(kind, z2), z2, finish=True)
            for d in range(1, reach + 1):
                @pl.when(arrives(kind, d, z2))
                def _():
                    each(kind, arrival_sends(kind, d, z2), z2, finish=True)
        return carry

    lax.fori_loop(0, depth, settle, 0)


def ring_kernel(depth, window, pieces, early, relayed, ahead, image_ref, text_ref, image_out, text_out,
                raw, img, txt, own_sum, text_sum, weights, sum_out, sum_in, part_out, part_core,
                part_x, part_y, load_sem, send, image_recv, text_recv, text_core_recv, sum_recv,
                part_recv, part_core_recv):
    blk = lax.axis_index("blk")
    z = lax.axis_index("grp")
    chip, core = blk // 2, blk % 2
    odd = chip % 2
    rows = raw.shape[1]
    span = rows // pieces
    columns = window // depth * rows
    is_end = (z == 0) | (z == depth - 1)
    is_mid = (z > 0) & (z < depth - 1)
    inner = 1 - 2 * (z // 2)
    partner = (2 * chip + 1 - core, z)
    across = (2 * (chip + 1 - 2 * odd) + core, z)
    over = (2 * ((chip + 2) % 4) + core, z)
    corner = (2 * ((chip + 3 - 2 * odd) % 4) + core, z)

    def piece(j):
        return pl.ds(pl.multiple_of(j * span, span), span)

    def slot_rows(slot, j):
        return pl.ds(pl.multiple_of(slot * rows + j * span, span), span)

    def remote(source, target, group, recv, device):
        return pltpu.make_async_remote_copy(
            src_ref=source, dst_ref=target, send_sem=send.at[group], recv_sem=recv,
            device_id=device, device_id_type=MESH,
        )

    def along(sign):
        return blk, jnp.minimum(jnp.maximum(z + sign, 0), depth - 1)

    def image_copy(source_z, sign, j, group=3):
        slot = (source_z - z - sign + 2 * depth - 1) % depth
        return remote(
            img.at[source_z, piece(j)], img.at[source_z, piece(j)], group,
            image_recv.at[slot, j], along(sign),
        )

    def await_image(source_z, j):
        slot = (source_z - z + 2 * depth - 1) % depth
        remote(
            img.at[source_z, piece(j)], img.at[source_z, piece(j)], 3,
            image_recv.at[slot, j], along(inner),
        ).wait_recv()

    def pass_image(source_z, sign, j):
        await_image(source_z, j)
        image_copy(source_z, sign, j).start()

    def sum_slot(target_z, there, sign):
        distance = target_z - there
        distance = jnp.maximum(distance, -distance)
        return jnp.where(sign == 1 - 2 * (there // 2), distance, depth - 1 + distance)

    def sum_copy(target_z, sign, j):
        there = along(sign)
        return remote(
            sum_out.at[target_z, piece(j)], sum_in.at[(1 - sign) // 2, target_z, piece(j)], 2,
            sum_recv.at[sum_slot(target_z, there[1], sign), j], there,
        )

    def await_sum(target_z, sign, j):
        remote(
            sum_out.at[target_z, piece(j)], sum_in.at[(1 - sign) // 2, target_z, piece(j)], 2,
            sum_recv.at[sum_slot(target_z, z, sign), j], along(inner),
        ).wait_recv()

    def text_copy(source_slot, target_slot, recv, j, device):
        return remote(
            txt.at[slot_rows(source_slot, j)], txt.at[slot_rows(target_slot, j)], 0, recv, device
        )

    def text_over(j):
        return text_copy(0, 4, text_recv.at[1, j], j, over)

    def text_across(j):
        return text_copy(4 * odd, 2, text_recv.at[0, j], j, across)

    def text_corner(j):
        return text_copy(0, 2, text_recv.at[0, j], j, corner)

    def text_to_core(slot, j):
        target = slot + 1 - 2 * core
        return text_copy(slot, target, text_core_recv.at[target // 2], j, partner)

    def part_to_core(index, j):
        return remote(
            part_out.at[2 * index + 1, piece(j)], part_core.at[index, piece(j)], 1,
            part_core_recv.at[j], partner,
        )

    def part_across(j):
        return remote(
            part_out.at[2, piece(j)], part_x.at[piece(j)], 1, part_recv.at[0, j], across
        )

    def part_corner(j):
        return remote(
            part_out.at[2, piece(j)], part_x.at[piece(j)], 1, part_recv.at[0, j], corner
        )

    def part_over(j):
        return remote(
            part_out.at[4, piece(j)], part_y.at[piece(j)], 1, part_recv.at[1, j], over
        )

    def span_loop(low, high, body):
        def step(j, carry):
            body(j)
            return carry

        lax.fori_loop(low, high, step, 0)

    def loop(count, body):
        span_loop(0, count, body)

    loads = []
    for kind, ref in ((0, image_ref), (1, text_ref)):
        load = pltpu.make_async_copy(ref, raw.at[kind], load_sem.at[kind])
        load.start()
        loads.append(load)

    barrier = pltpu.get_barrier_semaphore()

    def greet(target):
        pl.semaphore_signal(barrier, inc=1, device_id=target, device_id_type=MESH)

    for target in (partner, across, over, corner):
        greet(target)

    @pl.when(z > 0)
    def _():
        greet((blk, z - 1))

    @pl.when(z < depth - 1)
    def _():
        greet((blk, z + 1))

    def inverse_length(wide):
        return lax.rsqrt(jnp.sum(wide * wide, axis=-1, keepdims=True) + EPSILON)

    def unit_low(kind):
        wide = raw[kind].astype(jnp.float32)
        return (wide * inverse_length(wide)).astype(jnp.bfloat16)

    loads[0].wait()
    img[z] = unit_low(0)
    loads[1].wait()
    txt[pl.ds(0, rows)] = unit_low(1)
    pl.semaphore_wait(
        barrier, 4 + (z > 0).astype(jnp.int32) + (z < depth - 1).astype(jnp.int32)
    )

    def image_start(j):
        image_copy(z, inner, j, 2).start()

        @pl.when(is_mid & (j < early))
        def _():
            image_copy(z, -inner, j).start()

    def text_start(j):
        text_over(j).start()

        @pl.when(odd == 0)
        def _():
            text_across(j).start()

        @pl.when((odd == 1) & (j >= relayed))
        def _():
            text_corner(j).start()

        @pl.when(core == 0)
        def _():
            text_to_core(0, j).start()

    loop(pieces, image_start)
    loop(pieces, text_start)
    text_sum[...] = jnp.zeros(text_sum.shape, jnp.float32)

    def first(j):
        @pl.when(j < pieces)
        def _():
            text_over(j).wait_recv()

            @pl.when((odd == 1) & (j < relayed))
            def _():
                text_across(j).start()

            @pl.when(core == 1)
            def _():
                text_to_core(4, j).start()

        def second(i):
            text_across(i).wait_recv()
            text_to_core(2, i).start()

        @pl.when((odd == 1) & (j < pieces))
        def _():
            second(j)

        @pl.when(is_mid & (j < pieces))
        def _():
            pass_image(z + inner, -inner, j)
            pass_image(z - inner, inner, j)

        @pl.when((odd == 0) & (j >= ahead))
        def _():
            second(j - ahead)

        @pl.when(is_mid & (j >= pieces))
        def _():
            pass_image(z + 2 * inner, -inner, j - pieces)

    loop(pieces + ahead, first)
    for index in (0, 1):
        slot = 2 * index + 1
        block = txt.at[pl.ds(slot * rows, rows)]
        remote(block, block, 0, text_core_recv.at[index], partner).wait_recv()

    def text_window(source):
        start = pl.multiple_of(jnp.where(source < z, rows, 0), rows)
        return pl.ds(start, columns)

    def weigh(source, start, count):
        some = pl.ds(start, count)
        texts = txt[text_window(source)]
        product = lax.dot_general(
            img[source, some], texts, (((1,), (1,)), ((), ())), preferred_element_type=jnp.float32
        )
        inverse = jnp.exp(-BIAS_LOGIT - LOGIT_SCALE * product)
        slope = 1.0 / (1.0 + inverse)
        shape = (count, columns)
        diagonal = lax.broadcasted_iota(jnp.int32, shape, 0) + start == lax.broadcasted_iota(
            jnp.int32, shape, 1
        )
        positive = jnp.where(diagonal, (source == z).astype(jnp.float32), 0.0)
        slope = jnp.where(positive > 0.5, -inverse * slope, slope).astype(jnp.bfloat16)
        weights[source, some] = slope
        own_sum[source, some] = jnp.dot(slope, texts, preferred_element_type=jnp.float32)

    def add_texts(source):
        text_sum[text_window(source)] += lax.dot_general(
            weights[source], img[source], (((0,), (0,)), ((), ())),
            preferred_element_type=jnp.float32,
        )

    def relay(target_z, sign, j):
        await_sum(target_z, sign, j)
        arrived = sum_in[(1 - sign) // 2, target_z, piece(j)].astype(jnp.float32)
        sum_out[target_z, piece(j)] = (own_sum[target_z, piece(j)] + arrived).astype(jnp.bfloat16)
        sum_copy(target_z, sign, j).start()

    def near(j):
        relay(z + inner, inner, j)

    @pl.when(is_end)
    def _():
        group = pieces // 2

        def half_step(index):
            step = (index % 3 == 0) * 2 - (index == 6) + (index == 4) * 3 + (index == 5) * 3
            step += (index == 7)
            source = z + step * inner
            half = (index == 2) + (index % 2) * (index > 2)
            start = half * group

            @pl.when(step > 0)
            def _():
                loop(group, lambda j: await_image(source, start + j))

            weigh(source, pl.multiple_of(start * span, group * span), group * span)

            @pl.when(step > 0)
            def _():
                some = pl.ds(pl.multiple_of(start * span, group * span), group * span)
                sum_out[source, some] = own_sum[source, some].astype(jnp.bfloat16)
                loop(group, lambda j: sum_copy(source, inner, start + j).start())

            @pl.when(half == 1)
            def _():
                add_texts(source)

        loop(8, half_step)

    @pl.when(is_mid)
    def _():
        half = (ahead + pieces) // 2

        def image_step(index):
            def far(j):
                pass_image(z + 2 * inner, -inner, j)

            @pl.when(index == 1)
            def _():
                span_loop(ahead, half, far)

            @pl.when(index == 2)
            def _():
                span_loop(half, pieces, far)
                span_loop(early, pieces, lambda j: image_copy(z, -inner, j).start())
                span_loop(0, pieces // 4, near)

            @pl.when(index == 3)
            def _():
                span_loop(pieces // 4, pieces // 2, near)

            step = (index == 0) * 1 - (index == 1) * 1 + (index == 3) * 2
            source = z + step * inner
            weigh(source, 0, rows)
            add_texts(source)

        loop(4, image_step)

    def part_rows(slot, j):
        return text_sum[slot_rows(slot, j)]

    def part_first(j):
        for index in (0, 1):
            slot = 2 * index + 1
            part_out[slot, piece(j)] = part_rows(slot, j).astype(jnp.bfloat16)
            part_to_core(index, j).start()

    def part_second(j):
        pair = part_core.at[0, pl.ds(0, 2 * span)]
        remote(pair, pair, 1, part_core_recv.at[j], partner).wait_recv()
        side = part_core[1 - core, piece(j)].astype(jnp.float32)
        part_out[2, piece(j)] = (part_rows(2, j) + side).astype(jnp.bfloat16)

        @pl.when((odd == 1) | (j < relayed))
        def _():
            part_across(j).start()

        @pl.when((odd == 0) & (j >= relayed))
        def _():
            part_corner(j).start()

        @pl.when((odd == 0) | (j >= relayed))
        def _():
            part_third(j, 0.0)

    def part_third(j, arrived):
        side = part_core[1, piece(j)].astype(jnp.float32)
        side = jnp.where(core == 1, side, 0.0) + arrived
        part_out[4, piece(j)] = (part_rows(4, j) + side).astype(jnp.bfloat16)
        part_over(j).start()

    loop(pieces, part_first)

    @pl.when(is_mid)
    def _():
        span_loop(pieces // 2, pieces, near)

    loop(pieces, part_second)

    def middle(j):
        @pl.when(is_mid)
        def _():
            relay(z + 2 * inner, inner, j)

        part_across(j).wait_recv()

        @pl.when((odd == 1) & (j < relayed))
        def _():
            part_third(j, part_x[piece(j)].astype(jnp.float32))

    loop(pieces, middle)

    @pl.when(is_mid)
    def _():
        loop(pieces, lambda j: relay(z - inner, -inner, j))

    def finish(kind, out, total, j):
        wide = raw[kind, piece(j)].astype(jnp.float32)
        scale = inverse_length(wide)
        unit = wide * scale
        grad = LOGIT_SCALE * total
        radial = jnp.sum(unit * grad, axis=-1, keepdims=True)
        out[piece(j)] = ((grad - unit * radial) * scale).astype(out.dtype)

    def finish_text(j):
        part_over(j).wait_recv()
        total = part_rows(0, j) + part_y[piece(j)].astype(jnp.float32)
        total += jnp.where(core == 0, part_core[0, piece(j)].astype(jnp.float32), 0.0)
        total += jnp.where(
            (odd == 0) | (j >= relayed), part_x[piece(j)].astype(jnp.float32), 0.0
        )
        finish(1, text_out, total, j)

    def finish_image(j):
        await_sum(z, -inner, j)
        total = own_sum[z, piece(j)] + sum_in[(1 + inner) // 2, z, piece(j)].astype(jnp.float32)

        @pl.when(is_mid)
        def _():
            await_sum(z, inner, j)

        other = sum_in[(1 - inner) // 2, z, piece(j)].astype(jnp.float32)
        finish(0, image_out, total + jnp.where(is_mid, other, 0.0), j)

    loop(pieces, finish_text)
    loop(pieces, finish_image)

    def settle(group):
        remote(img, img, group, image_recv.at[0, 0], partner).wait_send()

    for group in (0, 1, 2):
        settle(group)

    @pl.when(is_mid)
    def _():
        settle(3)


def square_call(depth, window, image_embeds, text_embeds):
    rows, width = image_embeds.shape
    slots = window // depth + 1
    pieces = rows // PIECE_ROWS
    early, relayed, ahead = 3 * pieces // 4, 3 * pieces // 4, pieces // 2
    low, wide = jnp.bfloat16, jnp.float32
    return pl.pallas_call(
        functools.partial(ring_kernel, depth, window, pieces, early, relayed, ahead),
        out_shape=(pltpu.VMEM((rows, width), low),) * 2,
        in_specs=[pl.BlockSpec(memory_space=pl.ANY)] * 2,
        out_specs=(pl.BlockSpec(memory_space=pltpu.VMEM),) * 2,
        scratch_shapes=[
            pltpu.VMEM((2, rows, width), low),
            pltpu.VMEM((depth, rows, width), low),
            pltpu.VMEM((slots * rows, width), low),
            pltpu.VMEM((depth, rows, width), wide),
            pltpu.VMEM((slots * rows, width), wide),
            pltpu.VMEM((depth, rows, (slots - 1) * rows), low),
            pltpu.VMEM((depth, rows, width), low),
            pltpu.VMEM((2, depth, rows, width), low),
            pltpu.VMEM((slots, rows, width), low),
            pltpu.VMEM((2, rows, width), low),
            pltpu.VMEM((rows, width), low),
            pltpu.VMEM((rows, width), low),
            pltpu.SemaphoreType.DMA((2,)),
            pltpu.SemaphoreType.DMA((4,)),
            pltpu.SemaphoreType.DMA((depth - 1, pieces)),
            pltpu.SemaphoreType.DMA((2, pieces)),
            pltpu.SemaphoreType.DMA((2,)),
            pltpu.SemaphoreType.DMA((depth + 1, pieces)),
            pltpu.SemaphoreType.DMA((2, pieces)),
            pltpu.SemaphoreType.DMA((pieces,)),
        ],
        compiler_params=pltpu.CompilerParams(collective_id=0, has_side_effects=True),
    )(image_embeds, text_embeds)


def solution(mesh):
    cycle, depth = mesh.shape["blk"], mesh.shape["grp"]
    window = min(20, cycle * depth // 2)
    chips = cycle // 2
    reach = 1
    while (2 * reach + 1) * depth - (depth - 1) < window:
        reach += 1
    slots = 2 * (reach + 1)

    def per_device(image_embeds, text_embeds):
        rows, width = image_embeds.shape
        shape = jax.ShapeDtypeStruct((rows, width), jnp.bfloat16)
        if chips == 4 and depth == 4 and window == 4 * depth:
            return square_call(depth, window, image_embeds, text_embeds)
        return pl.pallas_call(
            functools.partial(kernel, chips, depth, reach, window),
            out_shape=(shape, shape),
            in_specs=[pl.BlockSpec(memory_space=pl.ANY)] * 2,
            out_specs=(pl.BlockSpec(memory_space=pltpu.VMEM),) * 2,
            scratch_shapes=[
                pltpu.VMEM((2, slots, depth, rows, width), jnp.bfloat16),
                pltpu.VMEM((2, rows, width), jnp.float32),
                pltpu.VMEM((2, rows, rows), jnp.float32),
                pltpu.SemaphoreType.DMA((2,)),
                pltpu.SemaphoreType.DMA((2, 6 + 2 * reach, depth)),
                pltpu.SemaphoreType.DMA((2, slots, depth)),
            ],
            compiler_params=pltpu.CompilerParams(collective_id=0, has_side_effects=True),
        )(image_embeds, text_embeds)

    placed = P(("blk", "grp"), None)
    return jax.shard_map(
        per_device, mesh=mesh, in_specs=(placed, placed), out_specs=(placed, placed), check_vma=False
    )
```

```python
import functools

import jax
import jax.numpy as jnp
from jax import lax
from jax.experimental import pallas as pl
from jax.experimental.pallas import tpu as pltpu
from jax.sharding import PartitionSpec as P

LOGIT_SCALE = 10.0
BIAS_LOGIT = -2.0
EPSILON = 1e-06
PIECE_ROWS = 32
MESH = pl.DeviceIdType.MESH


def kernel(chips, depth, reach, window, image_ref, text_ref, image_out, text_out,
           held, total, own_scale, local_sem, send_sem, recv_sem):
    blk = lax.axis_index("blk")
    grp = lax.axis_index("grp")
    chip, core = blk // 2, blk % 2
    relayed = chips == 4 and reach == 2 and 4 * depth - 1 < window

    def view(kind):
        return (
            chip + kind * (chips - 1 - 2 * chip),
            core + kind * (1 - 2 * core),
            grp + kind * (depth - 1 - 2 * grp),
        )

    def device(kind, c, k, z):
        c = (c + chips) % chips
        linear = 2 * c + k
        return (
            linear + kind * (2 * chips - 1 - 2 * linear),
            z + kind * (depth - 1 - 2 * z),
        )

    first_kind = 1 - chip % 2 if relayed else 0
    kinds = (first_kind, 1 - first_kind)

    def need(k, z, d, source_k, source_z):
        offset = (2 * d + k - source_k) * depth + z - source_z
        return (offset >= 0) & (offset < window)

    def chip_need(z, d, source_k, source_z):
        return need(0, z, d, source_k, source_z) | need(1, z, d, source_k, source_z)

    def arrives(kind, d, source_z):
        c, k, z = view(kind)
        wanted = chip_need(z, d, k, source_z)
        if relayed:
            wanted = wanted | ((d == 2) & (c % 2 == 1))
        return wanted

    def copy(kind, path, source_slot, target_slot, z, target):
        return pltpu.make_async_remote_copy(
            src_ref=held.at[kind, source_slot, z],
            dst_ref=held.at[kind, target_slot, z],
            send_sem=send_sem.at[kind, path, z],
            recv_sem=recv_sem.at[kind, target_slot, z],
            device_id=target,
            device_id_type=MESH,
        )

    def own_sends(kind, z2):
        c, k, z = view(kind)
        sends = [
            ((z2 <= z) & (z + 1 < depth), 0, k, k, (c, k, z + 1)),
            ((z2 >= z) & (z >= 1), 1, k, k, (c, k, z - 1)),
        ]
        for d in range(1, reach + 1):
            wanted = chip_need(z, d, k, z2)
            if relayed and d == 1:
                inside = (z2 > 0) & (z2 < depth - 1)
                wanted = (c % 2 == 0) & (inside | (z2 == z))
            if relayed and d == 2:
                wanted = wanted | (c % 2 == 1)
            sends.append((wanted, 1 + d, k, 2 * d + k, (c + d, k, z)))
        sends.append((need(1 - k, z, 0, k, z2), 2 + reach, k, k, (c, 1 - k, z)))
        return sends

    def arrival_sends(kind, d, z2):
        c, k, z = view(kind)
        sends = []
        slot = 2 * d + k
        if relayed:
            sends.append(((c % 2 == 1) & (d == 2), 3 + reach, slot, 2 + k, (c - 1, k, z)))
            outer = (c % 2 == 1) & (d == 1) & ((z2 == 0) | (z2 == depth - 1))
            sends.append((outer & (z2 <= z) & (z + 1 < depth),
                          4 + 2 * reach, slot, slot, (c, k, z + 1)))
            sends.append((outer & (z2 >= z) & (z >= 1),
                          5 + 2 * reach, slot, slot, (c, k, z - 1)))
        sends.append((need(1 - k, z, d, k, z2), 3 + reach + d, slot, slot, (c, 1 - k, z)))
        return sends

    def each(kind, sends, z2, finish=False):
        for wanted, path, source_slot, target_slot, target in sends:
            @pl.when(wanted)
            def _():
                moved = copy(kind, path, source_slot, target_slot, z2, device(kind, *target))
                if finish:
                    moved.wait_send()
                else:
                    moved.start()

    def await_block(kind, slot, z2):
        c, k, z = view(kind)
        copy(kind, 0, slot, slot, z2, device(kind, c, 1 - k, z)).wait_recv()

    own = []
    for kind, ref in ((0, text_ref), (1, image_ref)):
        _, k, z = view(kind)
        loaded = pltpu.make_async_copy(ref, held.at[kind, k, z], local_sem.at[kind])
        loaded.start()
        own.append(loaded)

    barrier = pltpu.get_barrier_semaphore()

    def greet(target):
        pl.semaphore_signal(barrier, inc=1, device_id=target, device_id_type=MESH)

    greet((2 * chip + 1 - core, grp))
    if relayed:
        partners = [chip + 1 - 2 * (chip % 2), (chip + 2) % 4]
    else:
        partners = [(chip + d + chips) % chips for d in range(-reach, reach + 1) if d]
    for partner in partners:
        greet((2 * partner + core, grp))

    @pl.when(grp > 0)
    def _():
        greet((blk, grp - 1))

    @pl.when(grp < depth - 1)
    def _():
        greet((blk, grp + 1))

    for loaded in own:
        loaded.wait()
    pl.semaphore_wait(
        barrier,
        1 + len(partners) + (grp > 0).astype(jnp.int32) + (grp < depth - 1).astype(jnp.int32),
    )

    def own_block(kind):
        _, k, z = view(kind)
        return held[kind, k, z]

    def inverse_length(block):
        wide = block.astype(jnp.float32)
        return lax.rsqrt(jnp.sum(wide * wide, axis=-1, keepdims=True) + EPSILON)

    rows = held.shape[3]

    def tile(kind, slot, z2):
        _, k, z = view(kind)
        other = held[kind, slot, z2]
        mine = own_block(1 - kind)
        columns = jnp.broadcast_to(inverse_length(other), (rows, rows)).T
        product = lax.dot_general(
            mine, other, (((1,), (1,)), ((), ())), preferred_element_type=jnp.float32
        )
        logits = LOGIT_SCALE * product * own_scale[kind] * columns + BIAS_LOGIT
        inverse = jnp.exp(-logits)
        weights = 1.0 / (1.0 + inverse)
        diagonal = lax.broadcasted_iota(jnp.int32, (rows, rows), 0) == lax.broadcasted_iota(
            jnp.int32, (rows, rows), 1
        )
        first = ((slot == k) & (z2 == z)).astype(jnp.float32)
        positive = jnp.where(diagonal, first, 0.0)
        weights = jnp.where(positive > 0.5, -inverse * weights, weights)
        scaled = (weights * columns).astype(jnp.bfloat16)
        total[kind] += jnp.dot(scaled, other, preferred_element_type=jnp.float32)

    def position(kind, sign, distance):
        _, _, z = view(kind)
        z2 = z + sign * distance
        valid = (z2 >= 0) & (z2 < depth) & (distance >= 0)
        return z2, valid & ((sign > 0) | (distance > 0))

    def prepare(kind, carry):
        total[kind] = jnp.zeros(total.shape[1:], jnp.float32)
        own_scale[kind] = jnp.broadcast_to(inverse_length(own_block(1 - kind)), (rows, rows))
        return carry

    def start_own(kind):
        _, _, z = view(kind)
        each(kind, own_sends(kind, z), z)

    for kind in kinds:
        start_own(kind)
    lax.fori_loop(0, 2, prepare, 0)

    def half_turn(index, carry):
        turn = index // 2
        kind = first_kind + (index % 2) * (1 - 2 * first_kind)
        _, k, z = view(kind)

        for sign in (1, -1):
            z2, valid = position(kind, sign, turn)

            @pl.when(valid & (turn > 0))
            def _():
                await_block(kind, k, z2)
                each(kind, own_sends(kind, z2), z2)

        def stage(step, carry):
            d = jnp.where(step == 0, reach, jnp.where(step == 1, 0, reach - step + 1))
            distance = turn - (d > 0).astype(jnp.int32)
            for sign in (1, -1):
                z2, valid = position(kind, sign, distance)

                @pl.when((d > 0) & valid & arrives(kind, d, z2))
                def _():
                    await_block(kind, 2 * d + k, z2)
                    each(kind, arrival_sends(kind, d, z2), z2)

            def work(item, carry):
                source_k = (k + item // 2) % 2
                z2, valid = position(kind, 1 - 2 * (item % 2), distance)
                slot = 2 * d + source_k

                @pl.when(valid & need(k, z, d, source_k, z2))
                def _():
                    @pl.when(source_k != k)
                    def _():
                        await_block(kind, slot, z2)

                    tile(kind, slot, z2)

                return carry

            return lax.fori_loop(0, 4, work, carry)

        return lax.fori_loop(0, reach + 1, stage, carry)

    lax.fori_loop(0, 2 * (depth + 1), half_turn, 0)

    for kind, out in ((0, image_out), (1, text_out)):
        scale = own_scale[kind][:, :1]
        unit = own_block(1 - kind).astype(jnp.float32) * scale
        grad = LOGIT_SCALE * total[kind]
        inner = jnp.sum(unit * grad, axis=-1, keepdims=True)
        out[...] = ((grad - unit * inner) * scale).astype(out.dtype)

    def settle(z2, carry):
        for kind in (0, 1):
            each(kind, own_sends(kind, z2), z2, finish=True)
            for d in range(1, reach + 1):
                @pl.when(arrives(kind, d, z2))
                def _():
                    each(kind, arrival_sends(kind, d, z2), z2, finish=True)
        return carry

    lax.fori_loop(0, depth, settle, 0)


def ring_kernel(depth, window, pieces, early, relayed, ahead, image_ref, text_ref, image_out, text_out,
                raw, img, txt, own_sum, text_sum, weights, sum_out, sum_in, part_out, part_core,
                part_x, part_y, load_sem, send, image_recv, text_recv, text_core_recv, sum_recv,
                part_recv, part_core_recv):
    blk = lax.axis_index("blk")
    z = lax.axis_index("grp")
    chip, core = blk // 2, blk % 2
    odd = chip % 2
    rows = raw.shape[1]
    span = rows // pieces
    parts, part_span = 2 * pieces, span // 2
    columns = window // depth * rows
    is_end = (z == 0) | (z == depth - 1)
    is_mid = (z > 0) & (z < depth - 1)
    inner = 1 - 2 * (z // 2)
    partner = (2 * chip + 1 - core, z)
    across = (2 * (chip + 1 - 2 * odd) + core, z)
    over = (2 * ((chip + 2) % 4) + core, z)
    corner = (2 * ((chip + 3 - 2 * odd) % 4) + core, z)

    def piece(j):
        return pl.ds(pl.multiple_of(j * span, span), span)

    def part(j):
        return pl.ds(pl.multiple_of(j * part_span, part_span), part_span)

    def slot_rows(slot, j):
        return pl.ds(pl.multiple_of(slot * rows + j * span, span), span)

    def remote(source, target, group, recv, device):
        return pltpu.make_async_remote_copy(
            src_ref=source, dst_ref=target, send_sem=send.at[group], recv_sem=recv,
            device_id=device, device_id_type=MESH,
        )

    def along(sign):
        return blk, jnp.minimum(jnp.maximum(z + sign, 0), depth - 1)

    def image_copy(source_z, sign, j, group=3):
        slot = (source_z - z - sign + 2 * depth - 1) % depth
        return remote(
            img.at[source_z, piece(j)], img.at[source_z, piece(j)], group,
            image_recv.at[slot, j], along(sign),
        )

    def await_image(source_z, j):
        slot = (source_z - z + 2 * depth - 1) % depth
        remote(
            img.at[source_z, piece(j)], img.at[source_z, piece(j)], 3,
            image_recv.at[slot, j], along(inner),
        ).wait_recv()

    def pass_image(source_z, sign, j):
        await_image(source_z, j)
        image_copy(source_z, sign, j).start()

    def sum_slot(target_z, there, sign):
        distance = target_z - there
        distance = jnp.maximum(distance, -distance)
        return jnp.where(sign == 1 - 2 * (there // 2), distance, depth - 1 + distance)

    def sum_copy(target_z, sign, j):
        there = along(sign)
        return remote(
            sum_out.at[target_z, piece(j)], sum_in.at[(1 - sign) // 2, target_z, piece(j)], 2,
            sum_recv.at[sum_slot(target_z, there[1], sign), j], there,
        )

    def await_sum(target_z, sign, j):
        remote(
            sum_out.at[target_z, piece(j)], sum_in.at[(1 - sign) // 2, target_z, piece(j)], 2,
            sum_recv.at[sum_slot(target_z, z, sign), j], along(inner),
        ).wait_recv()

    def text_copy(source_slot, target_slot, recv, j, device):
        return remote(
            txt.at[slot_rows(source_slot, j)], txt.at[slot_rows(target_slot, j)], 0, recv, device
        )

    def text_over(j):
        return text_copy(0, 4, text_recv.at[1, j], j, over)

    def text_across(j):
        return text_copy(4 * odd, 2, text_recv.at[0, j], j, across)

    def text_corner(j):
        return text_copy(0, 2, text_recv.at[0, j], j, corner)

    def text_to_core(slot, j):
        target = slot + 1 - 2 * core
        return text_copy(slot, target, text_core_recv.at[target // 2], j, partner)

    def part_to_core(index, j):
        return remote(
            part_out.at[2 * index + 1, part(j)], part_core.at[index, part(j)], 1,
            part_core_recv.at[j], partner,
        )

    def part_across(j):
        return remote(
            part_out.at[2, part(j)], part_x.at[part(j)], 1, part_recv.at[0, j], across
        )

    def part_corner(j):
        return remote(
            part_out.at[2, part(j)], part_x.at[part(j)], 1, part_recv.at[0, j], corner
        )

    def part_over(j):
        return remote(
            part_out.at[4, part(j)], part_y.at[part(j)], 1, part_recv.at[1, j], over
        )

    def span_loop(low, high, body):
        def step(j, carry):
            body(j)
            return carry

        lax.fori_loop(low, high, step, 0)

    def loop(count, body):
        span_loop(0, count, body)

    loads = []
    for kind, ref in ((0, image_ref), (1, text_ref)):
        load = pltpu.make_async_copy(ref, raw.at[kind], load_sem.at[kind])
        load.start()
        loads.append(load)

    barrier = pltpu.get_barrier_semaphore()

    def greet(target):
        pl.semaphore_signal(barrier, inc=1, device_id=target, device_id_type=MESH)

    for target in (partner, across, over, corner):
        greet(target)

    @pl.when(z > 0)
    def _():
        greet((blk, z - 1))

    @pl.when(z < depth - 1)
    def _():
        greet((blk, z + 1))

    def inverse_length(wide):
        return lax.rsqrt(jnp.sum(wide * wide, axis=-1, keepdims=True) + EPSILON)

    def unit_low(kind):
        wide = raw[kind].astype(jnp.float32)
        return (wide * inverse_length(wide)).astype(jnp.bfloat16)

    loads[0].wait()
    img[z] = unit_low(0)
    loads[1].wait()
    txt[pl.ds(0, rows)] = unit_low(1)
    pl.semaphore_wait(
        barrier, 4 + (z > 0).astype(jnp.int32) + (z < depth - 1).astype(jnp.int32)
    )

    def image_start(j):
        image_copy(z, inner, j, 2).start()

        @pl.when(is_mid & (j < early))
        def _():
            image_copy(z, -inner, j).start()

    def text_start(j):
        text_over(j).start()

        @pl.when(odd == 0)
        def _():
            text_across(j).start()

        @pl.when((odd == 1) & (j >= relayed))
        def _():
            text_corner(j).start()

        @pl.when(core == 0)
        def _():
            text_to_core(0, j).start()

    loop(pieces, image_start)
    loop(pieces, text_start)
    text_sum[...] = jnp.zeros(text_sum.shape, jnp.float32)

    def first(j):
        @pl.when(j < pieces)
        def _():
            text_over(j).wait_recv()

            @pl.when((odd == 1) & (j < relayed))
            def _():
                text_across(j).start()

            @pl.when(core == 1)
            def _():
                text_to_core(4, j).start()

        def second(i):
            text_across(i).wait_recv()
            text_to_core(2, i).start()

        @pl.when((odd == 1) & (j < pieces))
        def _():
            second(j)

        @pl.when(is_mid & (j < pieces))
        def _():
            pass_image(z + inner, -inner, j)
            pass_image(z - inner, inner, j)

        @pl.when((odd == 0) & (j >= ahead))
        def _():
            second(j - ahead)

        @pl.when(is_mid & (j >= pieces))
        def _():
            pass_image(z + 2 * inner, -inner, j - pieces)

    loop(pieces + ahead, first)
    for index in (0, 1):
        slot = 2 * index + 1
        block = txt.at[pl.ds(slot * rows, rows)]
        remote(block, block, 0, text_core_recv.at[index], partner).wait_recv()

    def text_window(source):
        start = pl.multiple_of(jnp.where(source < z, rows, 0), rows)
        return pl.ds(start, columns)

    def weigh(source, start, count):
        some = pl.ds(start, count)
        texts = txt[text_window(source)]
        product = lax.dot_general(
            img[source, some], texts, (((1,), (1,)), ((), ())), preferred_element_type=jnp.float32
        )
        inverse = jnp.exp(-BIAS_LOGIT - LOGIT_SCALE * product)
        slope = 1.0 / (1.0 + inverse)
        shape = (count, columns)
        diagonal = lax.broadcasted_iota(jnp.int32, shape, 0) + start == lax.broadcasted_iota(
            jnp.int32, shape, 1
        )
        positive = jnp.where(diagonal, (source == z).astype(jnp.float32), 0.0)
        slope = jnp.where(positive > 0.5, -inverse * slope, slope).astype(jnp.bfloat16)
        weights[source, some] = slope
        own_sum[source, some] = jnp.dot(slope, texts, preferred_element_type=jnp.float32)

    def add_texts(*sources):
        slopes = jnp.concatenate([weights[source] for source in sources])
        images = jnp.concatenate([img[source] for source in sources])
        text_sum[text_window(sources[0])] += lax.dot_general(
            slopes, images, (((0,), (0,)), ((), ())), preferred_element_type=jnp.float32
        )

    def relay(target_z, sign, j):
        await_sum(target_z, sign, j)
        arrived = sum_in[(1 - sign) // 2, target_z, piece(j)].astype(jnp.float32)
        sum_out[target_z, piece(j)] = (own_sum[target_z, piece(j)] + arrived).astype(jnp.bfloat16)
        sum_copy(target_z, sign, j).start()

    def near(j):
        relay(z + inner, inner, j)

    @pl.when(is_end)
    def _():
        group = pieces // 2
        near_z, far_z, edge_z = z + 2 * inner, z + 3 * inner, z + inner

        def take(source, low, count):
            span_loop(low, low + count, lambda j: await_image(source, j))
            weigh(source, pl.multiple_of(low * span, count * span), count * span)
            some = pl.ds(pl.multiple_of(low * span, count * span), count * span)
            sum_out[source, some] = own_sum[source, some].astype(jnp.bfloat16)

        def give(source, low, high):
            span_loop(low, high, lambda j: sum_copy(source, inner, j).start())

        def far_step(j):
            take(far_z, j, 1)
            give(far_z, j, j + 1)

        take(near_z, 0, group)
        give(near_z, 0, group)
        weigh(z, 0, rows)
        add_texts(z)
        take(near_z, group, group)
        give(near_z, group, pieces - 1)
        add_texts(near_z)
        take(edge_z, 0, group)
        loop(pieces, far_step)
        give(near_z, pieces - 1, pieces)
        take(edge_z, group, group)
        give(edge_z, 0, pieces)
        add_texts(far_z, edge_z)

    @pl.when(is_mid)
    def _():
        half = (ahead + pieces) // 2

        def image_step(index):
            def far(j):
                pass_image(z + 2 * inner, -inner, j)

            @pl.when(index == 1)
            def _():
                span_loop(ahead, half, far)

            @pl.when(index == 2)
            def _():
                span_loop(half, pieces, far)
                span_loop(early, pieces, lambda j: image_copy(z, -inner, j).start())
                span_loop(0, pieces // 4, near)

            @pl.when(index == 3)
            def _():
                span_loop(pieces // 4, pieces // 2, near)

            step = (index == 0) * 1 - (index == 1) * 1 + (index == 3) * 2
            source = z + step * inner
            weigh(source, 0, rows)
            add_texts(source)

        loop(4, image_step)

    def part_rows(slot, j):
        return text_sum[pl.ds(pl.multiple_of(slot * rows + j * part_span, part_span), part_span)]

    def part_first(j):
        for index in (0, 1):
            slot = 2 * index + 1
            part_out[slot, part(j)] = part_rows(slot, j).astype(jnp.bfloat16)
            part_to_core(index, j).start()

    def part_second(j):
        pair = part_core.at[0, pl.ds(0, 2 * part_span)]
        remote(pair, pair, 1, part_core_recv.at[j], partner).wait_recv()
        side = part_core[1 - core, part(j)].astype(jnp.float32)
        part_out[2, part(j)] = (part_rows(2, j) + side).astype(jnp.bfloat16)

        @pl.when((odd == 1) | (j < 2 * relayed))
        def _():
            part_across(j).start()

        @pl.when((odd == 0) & (j >= 2 * relayed))
        def _():
            part_corner(j).start()

        @pl.when((odd == 0) | (j >= 2 * relayed))
        def _():
            part_third(j, 0.0)

    def part_third(j, arrived):
        side = part_core[1, part(j)].astype(jnp.float32)
        side = jnp.where(core == 1, side, 0.0) + arrived
        part_out[4, part(j)] = (part_rows(4, j) + side).astype(jnp.bfloat16)
        part_over(j).start()

    def part_relay(j):
        part_across(j).wait_recv()
        part_third(j, part_x[part(j)].astype(jnp.float32))

    loop(parts, part_first)

    @pl.when(is_mid)
    def _():
        span_loop(pieces // 2, pieces - 1, near)

    loop(parts, part_second)

    @pl.when(is_mid)
    def _():
        loop(pieces, lambda j: relay(z + 2 * inner, inner, j))

    def outer(j):
        @pl.when((odd == 1) & (j < relayed))
        def _():
            part_relay(2 * j)
            part_relay(2 * j + 1)

        @pl.when(is_mid)
        def _():
            relay(z - inner, -inner, j)

            @pl.when(j == 1)
            def _():
                near(pieces - 1)

    loop(pieces, outer)

    def finish(kind, out, total, j):
        wide = raw[kind, piece(j)].astype(jnp.float32)
        scale = inverse_length(wide)
        unit = wide * scale
        grad = LOGIT_SCALE * total
        radial = jnp.sum(unit * grad, axis=-1, keepdims=True)
        out[piece(j)] = ((grad - unit * radial) * scale).astype(out.dtype)

    def finish_text(j):
        direct = (odd == 0) | (j >= relayed)
        for half in (0, 1):
            part_over(2 * j + half).wait_recv()

            @pl.when(direct)
            def _():
                part_across(2 * j + half).wait_recv()

        total = text_sum[slot_rows(0, j)] + part_y[piece(j)].astype(jnp.float32)
        total += jnp.where(core == 0, part_core[0, piece(j)].astype(jnp.float32), 0.0)
        total += jnp.where(direct, part_x[piece(j)].astype(jnp.float32), 0.0)
        finish(1, text_out, total, j)

    def finish_image(j):
        await_sum(z, -inner, j)
        total = own_sum[z, piece(j)] + sum_in[(1 + inner) // 2, z, piece(j)].astype(jnp.float32)

        @pl.when(is_mid)
        def _():
            await_sum(z, inner, j)

        other = sum_in[(1 - inner) // 2, z, piece(j)].astype(jnp.float32)
        finish(0, image_out, total + jnp.where(is_mid, other, 0.0), j)

    def finish_both(j):
        finish_image(j)
        finish_text(j)

    loop(pieces, finish_both)

    def settle(group):
        remote(img, img, group, image_recv.at[0, 0], partner).wait_send()

    for group in (0, 1, 2):
        settle(group)

    @pl.when(is_mid)
    def _():
        settle(3)


def square_call(depth, window, image_embeds, text_embeds):
    rows, width = image_embeds.shape
    slots = window // depth + 1
    pieces = rows // PIECE_ROWS
    early, relayed, ahead = 3 * pieces // 4, 3 * pieces // 4, pieces // 2
    low, wide = jnp.bfloat16, jnp.float32
    return pl.pallas_call(
        functools.partial(ring_kernel, depth, window, pieces, early, relayed, ahead),
        out_shape=(pltpu.VMEM((rows, width), low),) * 2,
        in_specs=[pl.BlockSpec(memory_space=pl.ANY)] * 2,
        out_specs=(pl.BlockSpec(memory_space=pltpu.VMEM),) * 2,
        scratch_shapes=[
            pltpu.VMEM((2, rows, width), low),
            pltpu.VMEM((depth, rows, width), low),
            pltpu.VMEM((slots * rows, width), low),
            pltpu.VMEM((depth, rows, width), wide),
            pltpu.VMEM((slots * rows, width), wide),
            pltpu.VMEM((depth, rows, (slots - 1) * rows), low),
            pltpu.VMEM((depth, rows, width), low),
            pltpu.VMEM((2, depth, rows, width), low),
            pltpu.VMEM((slots, rows, width), low),
            pltpu.VMEM((2, rows, width), low),
            pltpu.VMEM((rows, width), low),
            pltpu.VMEM((rows, width), low),
            pltpu.SemaphoreType.DMA((2,)),
            pltpu.SemaphoreType.DMA((4,)),
            pltpu.SemaphoreType.DMA((depth - 1, pieces)),
            pltpu.SemaphoreType.DMA((2, pieces)),
            pltpu.SemaphoreType.DMA((2,)),
            pltpu.SemaphoreType.DMA((depth + 1, pieces)),
            pltpu.SemaphoreType.DMA((2, 2 * pieces)),
            pltpu.SemaphoreType.DMA((2 * pieces,)),
        ],
        compiler_params=pltpu.CompilerParams(collective_id=0, has_side_effects=True),
    )(image_embeds, text_embeds)


def solution(mesh):
    cycle, depth = mesh.shape["blk"], mesh.shape["grp"]
    window = min(20, cycle * depth // 2)
    chips = cycle // 2
    reach = 1
    while (2 * reach + 1) * depth - (depth - 1) < window:
        reach += 1
    slots = 2 * (reach + 1)

    def per_device(image_embeds, text_embeds):
        rows, width = image_embeds.shape
        shape = jax.ShapeDtypeStruct((rows, width), jnp.bfloat16)
        if chips == 4 and depth == 4 and window == 4 * depth:
            return square_call(depth, window, image_embeds, text_embeds)
        return pl.pallas_call(
            functools.partial(kernel, chips, depth, reach, window),
            out_shape=(shape, shape),
            in_specs=[pl.BlockSpec(memory_space=pl.ANY)] * 2,
            out_specs=(pl.BlockSpec(memory_space=pltpu.VMEM),) * 2,
            scratch_shapes=[
                pltpu.VMEM((2, slots, depth, rows, width), jnp.bfloat16),
                pltpu.VMEM((2, rows, width), jnp.float32),
                pltpu.VMEM((2, rows, rows), jnp.float32),
                pltpu.SemaphoreType.DMA((2,)),
                pltpu.SemaphoreType.DMA((2, 6 + 2 * reach, depth)),
                pltpu.SemaphoreType.DMA((2, slots, depth)),
            ],
            compiler_params=pltpu.CompilerParams(collective_id=0, has_side_effects=True),
        )(image_embeds, text_embeds)

    placed = P(("blk", "grp"), None)
    return jax.shard_map(
        per_device, mesh=mesh, in_specs=(placed, placed), out_specs=(placed, placed), check_vma=False
    )
```

```python
import functools

import jax
import jax.numpy as jnp
from jax import lax
from jax.experimental import pallas as pl
from jax.experimental.pallas import tpu as pltpu
from jax.sharding import PartitionSpec as P

LOGIT_SCALE = 10.0
BIAS_LOGIT = -2.0
EPSILON = 1e-06
PIECE_ROWS = 32
MESH = pl.DeviceIdType.MESH


def kernel(chips, depth, reach, window, image_ref, text_ref, image_out, text_out,
           held, total, own_scale, local_sem, send_sem, recv_sem):
    blk = lax.axis_index("blk")
    grp = lax.axis_index("grp")
    chip, core = blk // 2, blk % 2
    relayed = chips == 4 and reach == 2 and 4 * depth - 1 < window

    def view(kind):
        return (
            chip + kind * (chips - 1 - 2 * chip),
            core + kind * (1 - 2 * core),
            grp + kind * (depth - 1 - 2 * grp),
        )

    def device(kind, c, k, z):
        c = (c + chips) % chips
        linear = 2 * c + k
        return (
            linear + kind * (2 * chips - 1 - 2 * linear),
            z + kind * (depth - 1 - 2 * z),
        )

    first_kind = 1 - chip % 2 if relayed else 0
    kinds = (first_kind, 1 - first_kind)

    def need(k, z, d, source_k, source_z):
        offset = (2 * d + k - source_k) * depth + z - source_z
        return (offset >= 0) & (offset < window)

    def chip_need(z, d, source_k, source_z):
        return need(0, z, d, source_k, source_z) | need(1, z, d, source_k, source_z)

    def arrives(kind, d, source_z):
        c, k, z = view(kind)
        wanted = chip_need(z, d, k, source_z)
        if relayed:
            wanted = wanted | ((d == 2) & (c % 2 == 1))
        return wanted

    def copy(kind, path, source_slot, target_slot, z, target):
        return pltpu.make_async_remote_copy(
            src_ref=held.at[kind, source_slot, z],
            dst_ref=held.at[kind, target_slot, z],
            send_sem=send_sem.at[kind, path, z],
            recv_sem=recv_sem.at[kind, target_slot, z],
            device_id=target,
            device_id_type=MESH,
        )

    def own_sends(kind, z2):
        c, k, z = view(kind)
        sends = [
            ((z2 <= z) & (z + 1 < depth), 0, k, k, (c, k, z + 1)),
            ((z2 >= z) & (z >= 1), 1, k, k, (c, k, z - 1)),
        ]
        for d in range(1, reach + 1):
            wanted = chip_need(z, d, k, z2)
            if relayed and d == 1:
                inside = (z2 > 0) & (z2 < depth - 1)
                wanted = (c % 2 == 0) & (inside | (z2 == z))
            if relayed and d == 2:
                wanted = wanted | (c % 2 == 1)
            sends.append((wanted, 1 + d, k, 2 * d + k, (c + d, k, z)))
        sends.append((need(1 - k, z, 0, k, z2), 2 + reach, k, k, (c, 1 - k, z)))
        return sends

    def arrival_sends(kind, d, z2):
        c, k, z = view(kind)
        sends = []
        slot = 2 * d + k
        if relayed:
            sends.append(((c % 2 == 1) & (d == 2), 3 + reach, slot, 2 + k, (c - 1, k, z)))
            outer = (c % 2 == 1) & (d == 1) & ((z2 == 0) | (z2 == depth - 1))
            sends.append((outer & (z2 <= z) & (z + 1 < depth),
                          4 + 2 * reach, slot, slot, (c, k, z + 1)))
            sends.append((outer & (z2 >= z) & (z >= 1),
                          5 + 2 * reach, slot, slot, (c, k, z - 1)))
        sends.append((need(1 - k, z, d, k, z2), 3 + reach + d, slot, slot, (c, 1 - k, z)))
        return sends

    def each(kind, sends, z2, finish=False):
        for wanted, path, source_slot, target_slot, target in sends:
            @pl.when(wanted)
            def _():
                moved = copy(kind, path, source_slot, target_slot, z2, device(kind, *target))
                if finish:
                    moved.wait_send()
                else:
                    moved.start()

    def await_block(kind, slot, z2):
        c, k, z = view(kind)
        copy(kind, 0, slot, slot, z2, device(kind, c, 1 - k, z)).wait_recv()

    own = []
    for kind, ref in ((0, text_ref), (1, image_ref)):
        _, k, z = view(kind)
        loaded = pltpu.make_async_copy(ref, held.at[kind, k, z], local_sem.at[kind])
        loaded.start()
        own.append(loaded)

    barrier = pltpu.get_barrier_semaphore()

    def greet(target):
        pl.semaphore_signal(barrier, inc=1, device_id=target, device_id_type=MESH)

    greet((2 * chip + 1 - core, grp))
    if relayed:
        partners = [chip + 1 - 2 * (chip % 2), (chip + 2) % 4]
    else:
        partners = [(chip + d + chips) % chips for d in range(-reach, reach + 1) if d]
    for partner in partners:
        greet((2 * partner + core, grp))

    @pl.when(grp > 0)
    def _():
        greet((blk, grp - 1))

    @pl.when(grp < depth - 1)
    def _():
        greet((blk, grp + 1))

    for loaded in own:
        loaded.wait()
    pl.semaphore_wait(
        barrier,
        1 + len(partners) + (grp > 0).astype(jnp.int32) + (grp < depth - 1).astype(jnp.int32),
    )

    def own_block(kind):
        _, k, z = view(kind)
        return held[kind, k, z]

    def inverse_length(block):
        wide = block.astype(jnp.float32)
        return lax.rsqrt(jnp.sum(wide * wide, axis=-1, keepdims=True) + EPSILON)

    rows = held.shape[3]

    def tile(kind, slot, z2):
        _, k, z = view(kind)
        other = held[kind, slot, z2]
        mine = own_block(1 - kind)
        columns = jnp.broadcast_to(inverse_length(other), (rows, rows)).T
        product = lax.dot_general(
            mine, other, (((1,), (1,)), ((), ())), preferred_element_type=jnp.float32
        )
        logits = LOGIT_SCALE * product * own_scale[kind] * columns + BIAS_LOGIT
        inverse = jnp.exp(-logits)
        weights = 1.0 / (1.0 + inverse)
        diagonal = lax.broadcasted_iota(jnp.int32, (rows, rows), 0) == lax.broadcasted_iota(
            jnp.int32, (rows, rows), 1
        )
        first = ((slot == k) & (z2 == z)).astype(jnp.float32)
        positive = jnp.where(diagonal, first, 0.0)
        weights = jnp.where(positive > 0.5, -inverse * weights, weights)
        scaled = (weights * columns).astype(jnp.bfloat16)
        total[kind] += jnp.dot(scaled, other, preferred_element_type=jnp.float32)

    def position(kind, sign, distance):
        _, _, z = view(kind)
        z2 = z + sign * distance
        valid = (z2 >= 0) & (z2 < depth) & (distance >= 0)
        return z2, valid & ((sign > 0) | (distance > 0))

    def prepare(kind, carry):
        total[kind] = jnp.zeros(total.shape[1:], jnp.float32)
        own_scale[kind] = jnp.broadcast_to(inverse_length(own_block(1 - kind)), (rows, rows))
        return carry

    def start_own(kind):
        _, _, z = view(kind)
        each(kind, own_sends(kind, z), z)

    for kind in kinds:
        start_own(kind)
    lax.fori_loop(0, 2, prepare, 0)

    def half_turn(index, carry):
        turn = index // 2
        kind = first_kind + (index % 2) * (1 - 2 * first_kind)
        _, k, z = view(kind)

        for sign in (1, -1):
            z2, valid = position(kind, sign, turn)

            @pl.when(valid & (turn > 0))
            def _():
                await_block(kind, k, z2)
                each(kind, own_sends(kind, z2), z2)

        def stage(step, carry):
            d = jnp.where(step == 0, reach, jnp.where(step == 1, 0, reach - step + 1))
            distance = turn - (d > 0).astype(jnp.int32)
            for sign in (1, -1):
                z2, valid = position(kind, sign, distance)

                @pl.when((d > 0) & valid & arrives(kind, d, z2))
                def _():
                    await_block(kind, 2 * d + k, z2)
                    each(kind, arrival_sends(kind, d, z2), z2)

            def work(item, carry):
                source_k = (k + item // 2) % 2
                z2, valid = position(kind, 1 - 2 * (item % 2), distance)
                slot = 2 * d + source_k

                @pl.when(valid & need(k, z, d, source_k, z2))
                def _():
                    @pl.when(source_k != k)
                    def _():
                        await_block(kind, slot, z2)

                    tile(kind, slot, z2)

                return carry

            return lax.fori_loop(0, 4, work, carry)

        return lax.fori_loop(0, reach + 1, stage, carry)

    lax.fori_loop(0, 2 * (depth + 1), half_turn, 0)

    for kind, out in ((0, image_out), (1, text_out)):
        scale = own_scale[kind][:, :1]
        unit = own_block(1 - kind).astype(jnp.float32) * scale
        grad = LOGIT_SCALE * total[kind]
        inner = jnp.sum(unit * grad, axis=-1, keepdims=True)
        out[...] = ((grad - unit * inner) * scale).astype(out.dtype)

    def settle(z2, carry):
        for kind in (0, 1):
            each(kind, own_sends(kind, z2), z2, finish=True)
            for d in range(1, reach + 1):
                @pl.when(arrives(kind, d, z2))
                def _():
                    each(kind, arrival_sends(kind, d, z2), z2, finish=True)
        return carry

    lax.fori_loop(0, depth, settle, 0)


def ring_kernel(depth, window, pieces, early, relayed, passed, ahead, image_ref, text_ref, image_out, text_out,
                raw, img, txt, own_sum, text_sum, weights, sum_out, sum_in, part_out, part_core,
                part_x, part_y, load_sem, send, image_recv, text_recv, text_core_recv, sum_recv,
                part_recv, part_core_recv):
    blk = lax.axis_index("blk")
    z = lax.axis_index("grp")
    chip, core = blk // 2, blk % 2
    odd = chip % 2
    rows = raw.shape[1]
    span = rows // pieces
    parts, part_span = 2 * pieces, span // 2
    columns = window // depth * rows
    is_end = (z == 0) | (z == depth - 1)
    is_mid = (z > 0) & (z < depth - 1)
    inner = 1 - 2 * (z // 2)
    bare = (z == 0) & (core == 0)
    passed = jnp.where(bare, 0, passed)
    partner = (2 * chip + 1 - core, z)
    across = (2 * (chip + 1 - 2 * odd) + core, z)
    over = (2 * ((chip + 2) % 4) + core, z)
    corner = (2 * ((chip + 3 - 2 * odd) % 4) + core, z)

    def piece(j):
        return pl.ds(pl.multiple_of(j * span, span), span)

    def part(j):
        return pl.ds(pl.multiple_of(j * part_span, part_span), part_span)

    def slot_rows(slot, j):
        return pl.ds(pl.multiple_of(slot * rows + j * span, span), span)

    def remote(source, target, group, recv, device):
        return pltpu.make_async_remote_copy(
            src_ref=source, dst_ref=target, send_sem=send.at[group], recv_sem=recv,
            device_id=device, device_id_type=MESH,
        )

    def along(sign):
        return blk, jnp.minimum(jnp.maximum(z + sign, 0), depth - 1)

    def image_copy(source_z, sign, j, group=3):
        slot = (source_z - z - sign + 2 * depth - 1) % depth
        return remote(
            img.at[source_z, piece(j)], img.at[source_z, piece(j)], group,
            image_recv.at[slot, j], along(sign),
        )

    def await_image(source_z, j):
        slot = (source_z - z + 2 * depth - 1) % depth
        remote(
            img.at[source_z, piece(j)], img.at[source_z, piece(j)], 3,
            image_recv.at[slot, j], along(inner),
        ).wait_recv()

    def pass_image(source_z, sign, j):
        await_image(source_z, j)
        image_copy(source_z, sign, j).start()

    def sum_slot(target_z, there, sign):
        distance = target_z - there
        distance = jnp.maximum(distance, -distance)
        return jnp.where(sign == 1 - 2 * (there // 2), distance, depth - 1 + distance)

    def sum_copy(target_z, sign, j):
        there = along(sign)
        return remote(
            sum_out.at[target_z, part(j)], sum_in.at[(1 - sign) // 2, target_z, part(j)], 2,
            sum_recv.at[sum_slot(target_z, there[1], sign), j], there,
        )

    def await_sum(target_z, sign, j):
        remote(
            sum_out.at[target_z, part(j)], sum_in.at[(1 - sign) // 2, target_z, part(j)], 2,
            sum_recv.at[sum_slot(target_z, z, sign), j], along(inner),
        ).wait_recv()

    def text_copy(source_slot, target_slot, recv, j, device):
        return remote(
            txt.at[slot_rows(source_slot, j)], txt.at[slot_rows(target_slot, j)], 0, recv, device
        )

    def text_over(j):
        return text_copy(0, 4, text_recv.at[1, j], j, over)

    def text_across(j):
        return text_copy(4 * odd, 2, text_recv.at[0, j], j, across)

    def text_corner(j):
        return text_copy(0, 2, text_recv.at[0, j], j, corner)

    def text_to_core(slot, j):
        target = slot + 1 - 2 * core
        return text_copy(slot, target, text_core_recv.at[target // 2], j, partner)

    def part_to_core(index, j):
        return remote(
            part_out.at[2 * index + 1, part(j)], part_core.at[index, part(j)], 1,
            part_core_recv.at[j], partner,
        )

    def part_across(j):
        return remote(
            part_out.at[2, part(j)], part_x.at[part(j)], 1, part_recv.at[0, j], across
        )

    def part_corner(j):
        return remote(
            part_out.at[2, part(j)], part_x.at[part(j)], 1, part_recv.at[0, j], corner
        )

    def part_over(j):
        return remote(
            part_out.at[4, part(j)], part_y.at[part(j)], 1, part_recv.at[1, j], over
        )

    def span_loop(low, high, body):
        def step(j, carry):
            body(j)
            return carry

        lax.fori_loop(low, high, step, 0)

    def loop(count, body):
        span_loop(0, count, body)

    loads = []
    for kind, ref in ((0, image_ref), (1, text_ref)):
        load = pltpu.make_async_copy(ref, raw.at[kind], load_sem.at[kind])
        load.start()
        loads.append(load)

    barrier = pltpu.get_barrier_semaphore()

    def greet(target):
        pl.semaphore_signal(barrier, inc=1, device_id=target, device_id_type=MESH)

    for target in (partner, across, over, corner):
        greet(target)

    @pl.when(z > 0)
    def _():
        greet((blk, z - 1))

    @pl.when(z < depth - 1)
    def _():
        greet((blk, z + 1))

    def inverse_length(wide):
        return lax.rsqrt(jnp.sum(wide * wide, axis=-1, keepdims=True) + EPSILON)

    def unit_low(kind):
        wide = raw[kind].astype(jnp.float32)
        return (wide * inverse_length(wide)).astype(jnp.bfloat16)

    loads[0].wait()
    img[z] = unit_low(0)
    loads[1].wait()
    txt[pl.ds(0, rows)] = unit_low(1)
    pl.semaphore_wait(
        barrier, 4 + (z > 0).astype(jnp.int32) + (z < depth - 1).astype(jnp.int32)
    )

    def image_start(j):
        @pl.when(is_end | (j < early))
        def _():
            image_copy(z, inner, j, 2).start()

        @pl.when(is_mid & (j < early))
        def _():
            image_copy(z, -inner, j).start()

    def text_start(j):
        text_over(j).start()

        @pl.when(odd == 0)
        def _():
            text_across(j).start()

        @pl.when((odd == 1) & (j >= relayed))
        def _():
            text_corner(j).start()

        @pl.when(core == 0)
        def _():
            text_to_core(0, j).start()

    loop(pieces, image_start)
    loop(pieces, text_start)
    text_sum[...] = jnp.zeros(text_sum.shape, jnp.float32)

    def pass_inner(q):
        late = q >= early + pieces
        from_far = (q >= early) & (q < early + pieces)
        j = q - jnp.where(late, pieces, jnp.where(from_far, early, 0))
        pass_image(z + inner * (1 + from_far), -inner, j)

    def first(j):
        @pl.when(j < pieces)
        def _():
            text_over(j).wait_recv()

            @pl.when((odd == 1) & (j < relayed))
            def _():
                text_across(j).start()

            @pl.when(core == 1)
            def _():
                text_to_core(4, j).start()

        def second(i):
            text_across(i).wait_recv()
            text_to_core(2, i).start()

        @pl.when((odd == 1) & (j < pieces))
        def _():
            second(j)

        @pl.when(is_mid)
        def _():
            pass_inner(j)

            @pl.when(j < pieces)
            def _():
                pass_image(z - inner, inner, j)

            @pl.when(j == pieces - 1)
            def _():
                span_loop(early, pieces, lambda i: image_copy(z, inner, i, 2).start())

        @pl.when((odd == 0) & (j >= ahead))
        def _():
            second(j - ahead)

    loop(pieces + ahead, first)
    for index in (0, 1):
        slot = 2 * index + 1
        block = txt.at[pl.ds(slot * rows, rows)]
        remote(block, block, 0, text_core_recv.at[index], partner).wait_recv()

    def text_window(source):
        start = pl.multiple_of(jnp.where(source < z, rows, 0), rows)
        return pl.ds(start, columns)

    def slopes_of(source, start, count):
        some = pl.ds(start, count)
        product = lax.dot_general(
            img[source, some], txt[text_window(source)], (((1,), (1,)), ((), ())),
            preferred_element_type=jnp.float32,
        )
        inverse = jnp.exp(-BIAS_LOGIT - LOGIT_SCALE * product)
        slope = 1.0 / (1.0 + inverse)
        shape = (count, columns)
        diagonal = lax.broadcasted_iota(jnp.int32, shape, 0) + start == lax.broadcasted_iota(
            jnp.int32, shape, 1
        )
        positive = jnp.where(diagonal, (source == z).astype(jnp.float32), 0.0)
        slope = jnp.where(positive > 0.5, -inverse * slope, slope).astype(jnp.bfloat16)
        weights[source, some] = slope
        return slope

    def sums_of(source, start, count, slope):
        own_sum[source, pl.ds(start, count)] = jnp.dot(
            slope, txt[text_window(source)], preferred_element_type=jnp.float32
        )

    def weigh(source, start, count):
        sums_of(source, start, count, slopes_of(source, start, count))

    def add_texts(*sources):
        slopes = jnp.concatenate([weights[source] for source in sources])
        images = jnp.concatenate([img[source] for source in sources])
        text_sum[text_window(sources[0])] += lax.dot_general(
            slopes, images, (((0,), (0,)), ((), ())), preferred_element_type=jnp.float32
        )

    def relay(target_z, sign, j):
        await_sum(target_z, sign, j)
        arrived = sum_in[(1 - sign) // 2, target_z, part(j)].astype(jnp.float32)
        sum_out[target_z, part(j)] = (own_sum[target_z, part(j)] + arrived).astype(jnp.bfloat16)
        sum_copy(target_z, sign, j).start()

    def near(j):
        relay(z + inner, inner, j)

    def part_rows(slot, j):
        return text_sum[pl.ds(pl.multiple_of(slot * rows + j * part_span, part_span), part_span)]

    def part_first(j):
        for index in (0, 1):
            slot = 2 * index + 1
            part_out[slot, part(j)] = part_rows(slot, j).astype(jnp.bfloat16)
            part_to_core(index, j).start()

    @pl.when(is_end)
    def _():
        group = pieces // 2
        near_z, far_z, edge_z = z + 2 * inner, z + 3 * inner, z + inner

        def take(source, low, count):
            span_loop(low, low + count, lambda j: await_image(source, j))
            weigh(source, pl.multiple_of(low * span, count * span), count * span)
            some = pl.ds(pl.multiple_of(low * span, count * span), count * span)
            sum_out[source, some] = own_sum[source, some].astype(jnp.bfloat16)

        def give(source, low, high):
            span_loop(2 * low, 2 * high, lambda j: sum_copy(source, inner, j).start())

        def far_step(j):
            take(far_z, j, 1)
            give(far_z, j, j + 1)

        take(near_z, 0, group)
        give(near_z, 0, group)
        weigh(z, 0, rows)
        add_texts(z)
        span_loop(0, group, far_step)
        take(edge_z, 0, group)
        span_loop(group, pieces, far_step)
        take(near_z, group, group)
        give(near_z, group, pieces)
        add_texts(far_z, near_z)
        span_loop(group, pieces, lambda j: await_image(edge_z, j))
        slopes_of(edge_z, group * span, group * span)
        add_texts(edge_z)
        loop(parts, part_first)
        last = pl.ds(group * span, group * span)
        sums_of(edge_z, group * span, group * span, weights[edge_z, last])
        sum_out[edge_z, last] = own_sum[edge_z, last].astype(jnp.bfloat16)
        give(edge_z, 0, pieces)

    @pl.when(is_mid)
    def _():
        def image_step(index):
            @pl.when(index == 1)
            def _():
                span_loop(pieces + ahead, 2 * pieces - 1, pass_inner)

            @pl.when(index == 2)
            def _():
                pass_inner(2 * pieces - 1)
                span_loop(early, pieces, lambda j: image_copy(z, -inner, j).start())

            @pl.when(index == 3)
            def _():
                span_loop(0, parts // 4, near)

            step = (index == 2) * 1 - (index == 0) * 1 + (index == 3) * 2
            source = z + step * inner
            weigh(source, 0, rows)
            add_texts(source)

        loop(4, image_step)
        loop(parts, part_first)

    def part_second(j):
        pair = part_core.at[0, pl.ds(0, 2 * part_span)]
        remote(pair, pair, 1, part_core_recv.at[j], partner).wait_recv()
        side = part_core[1 - core, part(j)].astype(jnp.float32)
        part_out[2, part(j)] = (part_rows(2, j) + side).astype(jnp.bfloat16)

        @pl.when((odd == 1) | (j < passed))
        def _():
            part_across(j).start()

        @pl.when((odd == 0) & (j >= passed))
        def _():
            part_corner(j).start()

        @pl.when(((odd == 0) | (j >= passed)) & ~bare)
        def _():
            part_third(j, 0.0)

    def part_third(j, arrived):
        side = part_core[1, part(j)].astype(jnp.float32)
        side = jnp.where(core == 1, side, 0.0) + arrived
        part_out[4, part(j)] = (part_rows(4, j) + side).astype(jnp.bfloat16)
        part_over(j).start()

    def part_relay(j):
        part_across(j).wait_recv()
        part_third(j, part_x[part(j)].astype(jnp.float32))

    def stage(i):
        j = i - parts // 2

        @pl.when(is_mid & (i < parts))
        def _():
            relay(z + 2 * inner, inner, i)

        @pl.when(is_mid & (j >= parts // 4) & (j < parts))
        def _():
            near(j)

        @pl.when(is_mid & (j > 0) & (j <= parts))
        def _():
            relay(z - inner, -inner, j - 1)

        @pl.when((odd == 1) & (i >= parts - 1) & (i - parts + 1 < passed))
        def _():
            part_relay(i - parts + 1)

    head = parts // 4 + 1
    span_loop(0, head, stage)
    loop(parts, part_second)
    span_loop(head, 2 * parts - 1, stage)

    def finish(kind, out, total, j):
        wide = raw[kind, piece(j)].astype(jnp.float32)
        scale = inverse_length(wide)
        unit = wide * scale
        grad = LOGIT_SCALE * total
        radial = jnp.sum(unit * grad, axis=-1, keepdims=True)
        out[piece(j)] = ((grad - unit * radial) * scale).astype(out.dtype)

    def finish_text(j):
        direct = (odd == 0) | (2 * j >= passed)
        for half in (0, 1):
            @pl.when(~bare)
            def _():
                part_over(2 * j + half).wait_recv()

            @pl.when(direct)
            def _():
                part_across(2 * j + half).wait_recv()

        total = text_sum[slot_rows(0, j)]
        total += jnp.where(bare, 0.0, part_y[piece(j)].astype(jnp.float32))
        total += jnp.where(core == 0, part_core[0, piece(j)].astype(jnp.float32), 0.0)
        total += jnp.where(direct, part_x[piece(j)].astype(jnp.float32), 0.0)
        finish(1, text_out, total, j)

    def finish_image(j):
        for half in (0, 1):
            await_sum(z, -inner, 2 * j + half)

        @pl.when(is_mid)
        def _():
            for half in (0, 1):
                await_sum(z, inner, 2 * j + half)

        total = own_sum[z, piece(j)] + sum_in[(1 + inner) // 2, z, piece(j)].astype(jnp.float32)
        other = sum_in[(1 - inner) // 2, z, piece(j)].astype(jnp.float32)
        finish(0, image_out, total + jnp.where(is_mid, other, 0.0), j)

    def finish_both(j):
        finish_image(j)
        finish_text(j)

    loop(pieces, finish_both)

    def settle(group, count=depth):
        some = img.at[pl.ds(0, count)]
        remote(some, some, group, image_recv.at[0, 0], partner).wait_send()

    settle(0)
    settle(2)

    @pl.when(bare)
    def _():
        settle(1, 3)

    @pl.when(~bare)
    def _():
        settle(1)

    @pl.when(is_mid)
    def _():
        settle(3)


def square_call(depth, window, image_embeds, text_embeds):
    rows, width = image_embeds.shape
    slots = window // depth + 1
    pieces = rows // PIECE_ROWS
    early, relayed, passed, ahead = 3 * pieces // 4, 3 * pieces // 4, 2 * pieces, pieces // 2
    low, wide = jnp.bfloat16, jnp.float32
    return pl.pallas_call(
        functools.partial(ring_kernel, depth, window, pieces, early, relayed, passed, ahead),
        out_shape=(pltpu.VMEM((rows, width), low),) * 2,
        in_specs=[pl.BlockSpec(memory_space=pl.ANY)] * 2,
        out_specs=(pl.BlockSpec(memory_space=pltpu.VMEM),) * 2,
        scratch_shapes=[
            pltpu.VMEM((2, rows, width), low),
            pltpu.VMEM((depth, rows, width), low),
            pltpu.VMEM((slots * rows, width), low),
            pltpu.VMEM((depth, rows, width), wide),
            pltpu.VMEM((slots * rows, width), wide),
            pltpu.VMEM((depth, rows, (slots - 1) * rows), low),
            pltpu.VMEM((depth, rows, width), low),
            pltpu.VMEM((2, depth, rows, width), low),
            pltpu.VMEM((slots, rows, width), low),
            pltpu.VMEM((2, rows, width), low),
            pltpu.VMEM((rows, width), low),
            pltpu.VMEM((rows, width), low),
            pltpu.SemaphoreType.DMA((2,)),
            pltpu.SemaphoreType.DMA((4,)),
            pltpu.SemaphoreType.DMA((depth - 1, pieces)),
            pltpu.SemaphoreType.DMA((2, pieces)),
            pltpu.SemaphoreType.DMA((2,)),
            pltpu.SemaphoreType.DMA((depth + 1, 2 * pieces)),
            pltpu.SemaphoreType.DMA((2, 2 * pieces)),
            pltpu.SemaphoreType.DMA((2 * pieces,)),
        ],
        compiler_params=pltpu.CompilerParams(collective_id=0, has_side_effects=True),
    )(image_embeds, text_embeds)


def solution(mesh):
    cycle, depth = mesh.shape["blk"], mesh.shape["grp"]
    window = min(20, cycle * depth // 2)
    chips = cycle // 2
    reach = 1
    while (2 * reach + 1) * depth - (depth - 1) < window:
        reach += 1
    slots = 2 * (reach + 1)

    def per_device(image_embeds, text_embeds):
        rows, width = image_embeds.shape
        shape = jax.ShapeDtypeStruct((rows, width), jnp.bfloat16)
        if chips == 4 and depth == 4 and window == 4 * depth:
            return square_call(depth, window, image_embeds, text_embeds)
        return pl.pallas_call(
            functools.partial(kernel, chips, depth, reach, window),
            out_shape=(shape, shape),
            in_specs=[pl.BlockSpec(memory_space=pl.ANY)] * 2,
            out_specs=(pl.BlockSpec(memory_space=pltpu.VMEM),) * 2,
            scratch_shapes=[
                pltpu.VMEM((2, slots, depth, rows, width), jnp.bfloat16),
                pltpu.VMEM((2, rows, width), jnp.float32),
                pltpu.VMEM((2, rows, rows), jnp.float32),
                pltpu.SemaphoreType.DMA((2,)),
                pltpu.SemaphoreType.DMA((2, 6 + 2 * reach, depth)),
                pltpu.SemaphoreType.DMA((2, slots, depth)),
            ],
            compiler_params=pltpu.CompilerParams(collective_id=0, has_side_effects=True),
        )(image_embeds, text_embeds)

    placed = P(("blk", "grp"), None)
    return jax.shard_map(
        per_device, mesh=mesh, in_specs=(placed, placed), out_specs=(placed, placed), check_vma=False
    )
```

```python
import functools

import jax
import jax.numpy as jnp
from jax import lax
from jax.experimental import pallas as pl
from jax.experimental.pallas import tpu as pltpu
from jax.sharding import PartitionSpec as P

LOGIT_SCALE = 10.0
BIAS_LOGIT = -2.0
EPSILON = 1e-06
PIECE_ROWS = 32
MESH = pl.DeviceIdType.MESH


def kernel(chips, depth, reach, window, image_ref, text_ref, image_out, text_out,
           held, total, own_scale, local_sem, send_sem, recv_sem):
    blk = lax.axis_index("blk")
    grp = lax.axis_index("grp")
    chip, core = blk // 2, blk % 2
    relayed = chips == 4 and reach == 2 and 4 * depth - 1 < window

    def view(kind):
        return (
            chip + kind * (chips - 1 - 2 * chip),
            core + kind * (1 - 2 * core),
            grp + kind * (depth - 1 - 2 * grp),
        )

    def device(kind, c, k, z):
        c = (c + chips) % chips
        linear = 2 * c + k
        return (
            linear + kind * (2 * chips - 1 - 2 * linear),
            z + kind * (depth - 1 - 2 * z),
        )

    first_kind = 1 - chip % 2 if relayed else 0
    kinds = (first_kind, 1 - first_kind)

    def need(k, z, d, source_k, source_z):
        offset = (2 * d + k - source_k) * depth + z - source_z
        return (offset >= 0) & (offset < window)

    def chip_need(z, d, source_k, source_z):
        return need(0, z, d, source_k, source_z) | need(1, z, d, source_k, source_z)

    def arrives(kind, d, source_z):
        c, k, z = view(kind)
        wanted = chip_need(z, d, k, source_z)
        if relayed:
            wanted = wanted | ((d == 2) & (c % 2 == 1))
        return wanted

    def copy(kind, path, source_slot, target_slot, z, target):
        return pltpu.make_async_remote_copy(
            src_ref=held.at[kind, source_slot, z],
            dst_ref=held.at[kind, target_slot, z],
            send_sem=send_sem.at[kind, path, z],
            recv_sem=recv_sem.at[kind, target_slot, z],
            device_id=target,
            device_id_type=MESH,
        )

    def own_sends(kind, z2):
        c, k, z = view(kind)
        sends = [
            ((z2 <= z) & (z + 1 < depth), 0, k, k, (c, k, z + 1)),
            ((z2 >= z) & (z >= 1), 1, k, k, (c, k, z - 1)),
        ]
        for d in range(1, reach + 1):
            wanted = chip_need(z, d, k, z2)
            if relayed and d == 1:
                inside = (z2 > 0) & (z2 < depth - 1)
                wanted = (c % 2 == 0) & (inside | (z2 == z))
            if relayed and d == 2:
                wanted = wanted | (c % 2 == 1)
            sends.append((wanted, 1 + d, k, 2 * d + k, (c + d, k, z)))
        sends.append((need(1 - k, z, 0, k, z2), 2 + reach, k, k, (c, 1 - k, z)))
        return sends

    def arrival_sends(kind, d, z2):
        c, k, z = view(kind)
        sends = []
        slot = 2 * d + k
        if relayed:
            sends.append(((c % 2 == 1) & (d == 2), 3 + reach, slot, 2 + k, (c - 1, k, z)))
            outer = (c % 2 == 1) & (d == 1) & ((z2 == 0) | (z2 == depth - 1))
            sends.append((outer & (z2 <= z) & (z + 1 < depth),
                          4 + 2 * reach, slot, slot, (c, k, z + 1)))
            sends.append((outer & (z2 >= z) & (z >= 1),
                          5 + 2 * reach, slot, slot, (c, k, z - 1)))
        sends.append((need(1 - k, z, d, k, z2), 3 + reach + d, slot, slot, (c, 1 - k, z)))
        return sends

    def each(kind, sends, z2, finish=False):
        for wanted, path, source_slot, target_slot, target in sends:
            @pl.when(wanted)
            def _():
                moved = copy(kind, path, source_slot, target_slot, z2, device(kind, *target))
                if finish:
                    moved.wait_send()
                else:
                    moved.start()

    def await_block(kind, slot, z2):
        c, k, z = view(kind)
        copy(kind, 0, slot, slot, z2, device(kind, c, 1 - k, z)).wait_recv()

    own = []
    for kind, ref in ((0, text_ref), (1, image_ref)):
        _, k, z = view(kind)
        loaded = pltpu.make_async_copy(ref, held.at[kind, k, z], local_sem.at[kind])
        loaded.start()
        own.append(loaded)

    barrier = pltpu.get_barrier_semaphore()

    def greet(target):
        pl.semaphore_signal(barrier, inc=1, device_id=target, device_id_type=MESH)

    greet((2 * chip + 1 - core, grp))
    if relayed:
        partners = [chip + 1 - 2 * (chip % 2), (chip + 2) % 4]
    else:
        partners = [(chip + d + chips) % chips for d in range(-reach, reach + 1) if d]
    for partner in partners:
        greet((2 * partner + core, grp))

    @pl.when(grp > 0)
    def _():
        greet((blk, grp - 1))

    @pl.when(grp < depth - 1)
    def _():
        greet((blk, grp + 1))

    for loaded in own:
        loaded.wait()
    pl.semaphore_wait(
        barrier,
        1 + len(partners) + (grp > 0).astype(jnp.int32) + (grp < depth - 1).astype(jnp.int32),
    )

    def own_block(kind):
        _, k, z = view(kind)
        return held[kind, k, z]

    def inverse_length(block):
        wide = block.astype(jnp.float32)
        return lax.rsqrt(jnp.sum(wide * wide, axis=-1, keepdims=True) + EPSILON)

    rows = held.shape[3]

    def tile(kind, slot, z2):
        _, k, z = view(kind)
        other = held[kind, slot, z2]
        mine = own_block(1 - kind)
        columns = jnp.broadcast_to(inverse_length(other), (rows, rows)).T
        product = lax.dot_general(
            mine, other, (((1,), (1,)), ((), ())), preferred_element_type=jnp.float32
        )
        logits = LOGIT_SCALE * product * own_scale[kind] * columns + BIAS_LOGIT
        inverse = jnp.exp(-logits)
        weights = 1.0 / (1.0 + inverse)
        diagonal = lax.broadcasted_iota(jnp.int32, (rows, rows), 0) == lax.broadcasted_iota(
            jnp.int32, (rows, rows), 1
        )
        first = ((slot == k) & (z2 == z)).astype(jnp.float32)
        positive = jnp.where(diagonal, first, 0.0)
        weights = jnp.where(positive > 0.5, -inverse * weights, weights)
        scaled = (weights * columns).astype(jnp.bfloat16)
        total[kind] += jnp.dot(scaled, other, preferred_element_type=jnp.float32)

    def position(kind, sign, distance):
        _, _, z = view(kind)
        z2 = z + sign * distance
        valid = (z2 >= 0) & (z2 < depth) & (distance >= 0)
        return z2, valid & ((sign > 0) | (distance > 0))

    def prepare(kind, carry):
        total[kind] = jnp.zeros(total.shape[1:], jnp.float32)
        own_scale[kind] = jnp.broadcast_to(inverse_length(own_block(1 - kind)), (rows, rows))
        return carry

    def start_own(kind):
        _, _, z = view(kind)
        each(kind, own_sends(kind, z), z)

    for kind in kinds:
        start_own(kind)
    lax.fori_loop(0, 2, prepare, 0)

    def half_turn(index, carry):
        turn = index // 2
        kind = first_kind + (index % 2) * (1 - 2 * first_kind)
        _, k, z = view(kind)

        for sign in (1, -1):
            z2, valid = position(kind, sign, turn)

            @pl.when(valid & (turn > 0))
            def _():
                await_block(kind, k, z2)
                each(kind, own_sends(kind, z2), z2)

        def stage(step, carry):
            d = jnp.where(step == 0, reach, jnp.where(step == 1, 0, reach - step + 1))
            distance = turn - (d > 0).astype(jnp.int32)
            for sign in (1, -1):
                z2, valid = position(kind, sign, distance)

                @pl.when((d > 0) & valid & arrives(kind, d, z2))
                def _():
                    await_block(kind, 2 * d + k, z2)
                    each(kind, arrival_sends(kind, d, z2), z2)

            def work(item, carry):
                source_k = (k + item // 2) % 2
                z2, valid = position(kind, 1 - 2 * (item % 2), distance)
                slot = 2 * d + source_k

                @pl.when(valid & need(k, z, d, source_k, z2))
                def _():
                    @pl.when(source_k != k)
                    def _():
                        await_block(kind, slot, z2)

                    tile(kind, slot, z2)

                return carry

            return lax.fori_loop(0, 4, work, carry)

        return lax.fori_loop(0, reach + 1, stage, carry)

    lax.fori_loop(0, 2 * (depth + 1), half_turn, 0)

    for kind, out in ((0, image_out), (1, text_out)):
        scale = own_scale[kind][:, :1]
        unit = own_block(1 - kind).astype(jnp.float32) * scale
        grad = LOGIT_SCALE * total[kind]
        inner = jnp.sum(unit * grad, axis=-1, keepdims=True)
        out[...] = ((grad - unit * inner) * scale).astype(out.dtype)

    def settle(z2, carry):
        for kind in (0, 1):
            each(kind, own_sends(kind, z2), z2, finish=True)
            for d in range(1, reach + 1):
                @pl.when(arrives(kind, d, z2))
                def _():
                    each(kind, arrival_sends(kind, d, z2), z2, finish=True)
        return carry

    lax.fori_loop(0, depth, settle, 0)


def ring_kernel(depth, window, pieces, early, relayed, passed, ahead, image_ref, text_ref, both_out,
                raw, img, txt, own_sum, text_sum, weights, sum_out, sum_in, part_out, part_core,
                part_x, part_y, load_sem, send, image_recv, text_recv, text_core_recv, sum_recv,
                part_recv, part_core_recv):
    blk = lax.axis_index("blk")
    z = lax.axis_index("grp")
    chip, core = blk // 2, blk % 2
    odd = chip % 2
    rows = raw.shape[1]
    span = rows // pieces
    parts, part_span = 2 * pieces, span // 2
    columns = window // depth * rows
    is_end = (z == 0) | (z == depth - 1)
    is_mid = (z > 0) & (z < depth - 1)
    inner = 1 - 2 * (z // 2)
    bare = (z == 0) & (core == 0)
    passed = jnp.where(bare, 0, passed)
    partner = (2 * chip + 1 - core, z)
    across = (2 * (chip + 1 - 2 * odd) + core, z)
    over = (2 * ((chip + 2) % 4) + core, z)
    corner = (2 * ((chip + 3 - 2 * odd) % 4) + core, z)

    def piece(j):
        return pl.ds(pl.multiple_of(j * span, span), span)

    def part(j):
        return pl.ds(pl.multiple_of(j * part_span, part_span), part_span)

    def slot_rows(slot, j):
        return pl.ds(pl.multiple_of(slot * rows + j * span, span), span)

    def remote(source, target, group, recv, device):
        return pltpu.make_async_remote_copy(
            src_ref=source, dst_ref=target, send_sem=send.at[group], recv_sem=recv,
            device_id=device, device_id_type=MESH,
        )

    def along(sign):
        return blk, jnp.minimum(jnp.maximum(z + sign, 0), depth - 1)

    def image_copy(source_z, sign, j, group=3):
        slot = (source_z - z - sign + 2 * depth - 1) % depth
        return remote(
            img.at[source_z, piece(j)], img.at[source_z, piece(j)], group,
            image_recv.at[slot, j], along(sign),
        )

    def await_image(source_z, j):
        slot = (source_z - z + 2 * depth - 1) % depth
        remote(
            img.at[source_z, piece(j)], img.at[source_z, piece(j)], 3,
            image_recv.at[slot, j], along(inner),
        ).wait_recv()

    def pass_image(source_z, sign, j):
        await_image(source_z, j)
        image_copy(source_z, sign, j).start()

    def sum_slot(target_z, there, sign):
        distance = target_z - there
        distance = jnp.maximum(distance, -distance)
        return jnp.where(sign == 1 - 2 * (there // 2), distance, depth - 1 + distance)

    def sum_copy(target_z, sign, j):
        there = along(sign)
        return remote(
            sum_out.at[target_z, part(j)], sum_in.at[(1 - sign) // 2, target_z, part(j)], 2,
            sum_recv.at[sum_slot(target_z, there[1], sign), j], there,
        )

    def await_sum(target_z, sign, j):
        remote(
            sum_out.at[target_z, part(j)], sum_in.at[(1 - sign) // 2, target_z, part(j)], 2,
            sum_recv.at[sum_slot(target_z, z, sign), j], along(inner),
        ).wait_recv()

    def text_copy(source_slot, target_slot, recv, j, device):
        return remote(
            txt.at[slot_rows(source_slot, j)], txt.at[slot_rows(target_slot, j)], 0, recv, device
        )

    def text_over(j):
        return text_copy(0, 4, text_recv.at[1, j], j, over)

    def text_across(j):
        return text_copy(4 * odd, 2, text_recv.at[0, j], j, across)

    def text_corner(j):
        return text_copy(0, 2, text_recv.at[0, j], j, corner)

    def text_to_core(slot, j):
        target = slot + 1 - 2 * core
        return text_copy(slot, target, text_core_recv.at[target // 2], j, partner)

    def part_to_core(index, j):
        return remote(
            part_out.at[2 * index + 1, part(j)], part_core.at[index, part(j)], 1,
            part_core_recv.at[j], partner,
        )

    def part_across(j):
        return remote(
            part_out.at[2, part(j)], part_x.at[part(j)], 1, part_recv.at[0, j], across
        )

    def part_corner(j):
        return remote(
            part_out.at[2, part(j)], part_x.at[part(j)], 1, part_recv.at[0, j], corner
        )

    def part_over(j):
        return remote(
            part_out.at[4, part(j)], part_y.at[part(j)], 1, part_recv.at[1, j], over
        )

    def span_loop(low, high, body):
        def step(j, carry):
            body(j)
            return carry

        lax.fori_loop(low, high, step, 0)

    def loop(count, body):
        span_loop(0, count, body)

    loads = []
    for kind, ref in ((0, image_ref), (1, text_ref)):
        load = pltpu.make_async_copy(ref, raw.at[kind], load_sem.at[kind])
        load.start()
        loads.append(load)

    barrier = pltpu.get_barrier_semaphore()

    def greet(target):
        pl.semaphore_signal(barrier, inc=1, device_id=target, device_id_type=MESH)

    for target in (partner, across, over, corner):
        greet(target)

    @pl.when(z > 0)
    def _():
        greet((blk, z - 1))

    @pl.when(z < depth - 1)
    def _():
        greet((blk, z + 1))

    def inverse_length(wide):
        return lax.rsqrt(jnp.sum(wide * wide, axis=-1, keepdims=True) + EPSILON)

    def unit_low(kind):
        wide = raw[kind].astype(jnp.float32)
        return (wide * inverse_length(wide)).astype(jnp.bfloat16)

    loads[0].wait()
    img[z] = unit_low(0)
    loads[1].wait()
    txt[pl.ds(0, rows)] = unit_low(1)
    pl.semaphore_wait(
        barrier, 4 + (z > 0).astype(jnp.int32) + (z < depth - 1).astype(jnp.int32)
    )

    def image_start(j):
        @pl.when(is_end | (j < early))
        def _():
            image_copy(z, inner, j, 2).start()

        @pl.when(is_mid & (j < early))
        def _():
            image_copy(z, -inner, j).start()

    def text_start(j):
        text_over(j).start()

        @pl.when(odd == 0)
        def _():
            text_across(j).start()

        @pl.when((odd == 1) & (j >= relayed))
        def _():
            text_corner(j).start()

        @pl.when(core == 0)
        def _():
            text_to_core(0, j).start()

    loop(pieces, image_start)
    loop(pieces, text_start)
    text_sum[...] = jnp.zeros(text_sum.shape, jnp.float32)

    def pass_inner(q):
        late = q >= early + pieces
        from_far = (q >= early) & (q < early + pieces)
        j = q - jnp.where(late, pieces, jnp.where(from_far, early, 0))
        pass_image(z + inner * (1 + from_far), -inner, j)

    def first(j):
        @pl.when(j < pieces)
        def _():
            text_over(j).wait_recv()

            @pl.when((odd == 1) & (j < relayed))
            def _():
                text_across(j).start()

            @pl.when(core == 1)
            def _():
                text_to_core(4, j).start()

        def second(i):
            text_across(i).wait_recv()
            text_to_core(2, i).start()

        @pl.when((odd == 1) & (j < pieces))
        def _():
            second(j)

        @pl.when(is_mid)
        def _():
            pass_inner(j)

            @pl.when(j < pieces)
            def _():
                pass_image(z - inner, inner, j)

            @pl.when(j == pieces - 1)
            def _():
                span_loop(early, pieces, lambda i: image_copy(z, inner, i, 2).start())

        @pl.when((odd == 0) & (j >= ahead))
        def _():
            second(j - ahead)

    loop(pieces + ahead, first)
    for index in (0, 1):
        slot = 2 * index + 1
        block = txt.at[pl.ds(slot * rows, rows)]
        remote(block, block, 0, text_core_recv.at[index], partner).wait_recv()

    def text_window(source):
        start = pl.multiple_of(jnp.where(source < z, rows, 0), rows)
        return pl.ds(start, columns)

    def slopes_of(source, start, count):
        some = pl.ds(start, count)
        product = lax.dot_general(
            img[source, some], txt[text_window(source)], (((1,), (1,)), ((), ())),
            preferred_element_type=jnp.float32,
        )
        inverse = jnp.exp(-BIAS_LOGIT - LOGIT_SCALE * product)
        slope = 1.0 / (1.0 + inverse)
        shape = (count, columns)
        diagonal = lax.broadcasted_iota(jnp.int32, shape, 0) + start == lax.broadcasted_iota(
            jnp.int32, shape, 1
        )
        positive = jnp.where(diagonal, (source == z).astype(jnp.float32), 0.0)
        slope = jnp.where(positive > 0.5, -inverse * slope, slope).astype(jnp.bfloat16)
        weights[source, some] = slope
        return slope

    def sums_of(source, start, count, slope):
        own_sum[source, pl.ds(start, count)] = jnp.dot(
            slope, txt[text_window(source)], preferred_element_type=jnp.float32
        )

    def weigh(source, start, count):
        sums_of(source, start, count, slopes_of(source, start, count))

    def add_texts(*sources):
        slopes = jnp.concatenate([weights[source] for source in sources])
        images = jnp.concatenate([img[source] for source in sources])
        text_sum[text_window(sources[0])] += lax.dot_general(
            slopes, images, (((0,), (0,)), ((), ())), preferred_element_type=jnp.float32
        )

    def relay(target_z, sign, j):
        await_sum(target_z, sign, j)
        arrived = sum_in[(1 - sign) // 2, target_z, part(j)].astype(jnp.float32)
        sum_out[target_z, part(j)] = (own_sum[target_z, part(j)] + arrived).astype(jnp.bfloat16)
        sum_copy(target_z, sign, j).start()

    def near(j):
        relay(z + inner, inner, j)

    def part_rows(slot, j):
        return text_sum[pl.ds(pl.multiple_of(slot * rows + j * part_span, part_span), part_span)]

    def part_first(j):
        for index in (0, 1):
            slot = 2 * index + 1
            part_out[slot, part(j)] = part_rows(slot, j).astype(jnp.bfloat16)
            part_to_core(index, j).start()

    @pl.when(is_end)
    def _():
        group = pieces // 2
        near_z, far_z, edge_z = z + 2 * inner, z + 3 * inner, z + inner

        def take(source, low, count):
            span_loop(low, low + count, lambda j: await_image(source, j))
            weigh(source, pl.multiple_of(low * span, count * span), count * span)
            some = pl.ds(pl.multiple_of(low * span, count * span), count * span)
            sum_out[source, some] = own_sum[source, some].astype(jnp.bfloat16)

        def give(source, low, high):
            span_loop(2 * low, 2 * high, lambda j: sum_copy(source, inner, j).start())

        def far_step(j):
            take(far_z, j, 1)
            give(far_z, j, j + 1)

        take(near_z, 0, group)
        give(near_z, 0, group)
        weigh(z, 0, rows)
        add_texts(z)
        span_loop(0, group, far_step)
        take(edge_z, 0, group)
        span_loop(group, pieces, far_step)
        take(near_z, group, group)
        give(near_z, group, pieces)
        add_texts(far_z, near_z)
        span_loop(group, pieces, lambda j: await_image(edge_z, j))
        slopes_of(edge_z, group * span, group * span)
        add_texts(edge_z)
        loop(parts, part_first)
        last = pl.ds(group * span, group * span)
        sums_of(edge_z, group * span, group * span, weights[edge_z, last])
        sum_out[edge_z, last] = own_sum[edge_z, last].astype(jnp.bfloat16)
        give(edge_z, 0, pieces)

    @pl.when(is_mid)
    def _():
        def rest(j):
            image_copy(z, -inner, j).start()

        def image_step(index):
            @pl.when(index == 1)
            def _():
                span_loop(pieces + ahead, 2 * pieces - 1, pass_inner)

            @pl.when(index == 2)
            def _():
                pass_inner(2 * pieces - 1)

                @pl.when(core == 0)
                def _():
                    span_loop(early, pieces, rest)

            @pl.when(index == 3)
            def _():
                span_loop(0, parts // 4, near)

            step = (index == 2) * 1 - (index == 0) * 1 + (index == 3) * 2
            source = z + step * inner
            weigh(source, 0, rows)
            add_texts(source)

        loop(4, image_step)

        @pl.when(core == 1)
        def _():
            span_loop(early, pieces, rest)

        loop(parts, part_first)

    def part_second(j):
        pair = part_core.at[0, pl.ds(0, 2 * part_span)]
        remote(pair, pair, 1, part_core_recv.at[j], partner).wait_recv()
        side = part_core[1 - core, part(j)].astype(jnp.float32)
        part_out[2, part(j)] = (part_rows(2, j) + side).astype(jnp.bfloat16)

        @pl.when((odd == 1) | (j < passed))
        def _():
            part_across(j).start()

        @pl.when((odd == 0) & (j >= passed))
        def _():
            part_corner(j).start()

        @pl.when(((odd == 0) | (j >= passed)) & ~bare)
        def _():
            part_third(j, 0.0)

    def part_third(j, arrived):
        side = part_core[1, part(j)].astype(jnp.float32)
        side = jnp.where(core == 1, side, 0.0) + arrived
        part_out[4, part(j)] = (part_rows(4, j) + side).astype(jnp.bfloat16)
        part_over(j).start()

    def part_relay(j):
        part_across(j).wait_recv()
        part_third(j, part_x[part(j)].astype(jnp.float32))

    def stage(i):
        j = i - parts // 2

        @pl.when(is_mid & (i < parts))
        def _():
            relay(z + 2 * inner, inner, i)

        @pl.when(is_mid & (j >= parts // 4) & (j < parts))
        def _():
            near(j)

        @pl.when(is_mid & (j > 0) & (j <= parts))
        def _():
            relay(z - inner, -inner, j - 1)

        @pl.when((odd == 1) & (i >= parts - 1) & (i - parts + 1 < passed))
        def _():
            part_relay(i - parts + 1)

    head = parts // 4 + 1
    span_loop(0, head, stage)
    loop(parts, part_second)
    span_loop(head, 2 * parts - 1, stage)

    def finish(kind, out, total, j):
        wide = raw[kind, piece(j)].astype(jnp.float32)
        scale = inverse_length(wide)
        unit = wide * scale
        grad = LOGIT_SCALE * total
        radial = jnp.sum(unit * grad, axis=-1, keepdims=True)
        out[piece(j)] = ((grad - unit * radial) * scale).astype(out.dtype)

    def finish_text(j):
        direct = (odd == 0) | (2 * j >= passed)
        for half in (0, 1):
            @pl.when(~bare)
            def _():
                part_over(2 * j + half).wait_recv()

            @pl.when(direct)
            def _():
                part_across(2 * j + half).wait_recv()

        total = text_sum[slot_rows(0, j)]
        total += jnp.where(bare, 0.0, part_y[piece(j)].astype(jnp.float32))
        total += jnp.where(core == 0, part_core[0, piece(j)].astype(jnp.float32), 0.0)
        total += jnp.where(direct, part_x[piece(j)].astype(jnp.float32), 0.0)
        finish(1, both_out.at[pl.ds(rows, rows)], total, j)

    def finish_image(j):
        for half in (0, 1):
            await_sum(z, -inner, 2 * j + half)

        @pl.when(is_mid)
        def _():
            for half in (0, 1):
                await_sum(z, inner, 2 * j + half)

        total = own_sum[z, piece(j)] + sum_in[(1 + inner) // 2, z, piece(j)].astype(jnp.float32)
        other = sum_in[(1 - inner) // 2, z, piece(j)].astype(jnp.float32)
        finish(0, both_out.at[pl.ds(0, rows)], total + jnp.where(is_mid, other, 0.0), j)

    def finish_both(j):
        finish_image(j)
        finish_text(j)

    loop(pieces, finish_both)

    def settle(group, count=depth):
        some = img.at[pl.ds(0, count)]
        remote(some, some, group, image_recv.at[0, 0], partner).wait_send()

    settle(0)
    settle(2)

    @pl.when(bare)
    def _():
        settle(1, 3)

    @pl.when(~bare)
    def _():
        settle(1)

    @pl.when(is_mid)
    def _():
        settle(3)


def square_call(depth, window, image_embeds, text_embeds):
    rows, width = image_embeds.shape
    slots = window // depth + 1
    pieces = rows // PIECE_ROWS
    early, relayed, passed, ahead = 3 * pieces // 4, 3 * pieces // 4, 2 * pieces, pieces // 2
    low, wide = jnp.bfloat16, jnp.float32
    both = pl.pallas_call(
        functools.partial(ring_kernel, depth, window, pieces, early, relayed, passed, ahead),
        out_shape=pltpu.VMEM((2 * rows, width), low),
        in_specs=[pl.BlockSpec(memory_space=pl.ANY)] * 2,
        out_specs=pl.BlockSpec(memory_space=pltpu.VMEM),
        scratch_shapes=[
            pltpu.VMEM((2, rows, width), low),
            pltpu.VMEM((depth, rows, width), low),
            pltpu.VMEM((slots * rows, width), low),
            pltpu.VMEM((depth, rows, width), wide),
            pltpu.VMEM((slots * rows, width), wide),
            pltpu.VMEM((depth, rows, (slots - 1) * rows), low),
            pltpu.VMEM((depth, rows, width), low),
            pltpu.VMEM((2, depth, rows, width), low),
            pltpu.VMEM((slots, rows, width), low),
            pltpu.VMEM((2, rows, width), low),
            pltpu.VMEM((rows, width), low),
            pltpu.VMEM((rows, width), low),
            pltpu.SemaphoreType.DMA((2,)),
            pltpu.SemaphoreType.DMA((4,)),
            pltpu.SemaphoreType.DMA((depth - 1, pieces)),
            pltpu.SemaphoreType.DMA((2, pieces)),
            pltpu.SemaphoreType.DMA((2,)),
            pltpu.SemaphoreType.DMA((depth + 1, 2 * pieces)),
            pltpu.SemaphoreType.DMA((2, 2 * pieces)),
            pltpu.SemaphoreType.DMA((2 * pieces,)),
        ],
        compiler_params=pltpu.CompilerParams(collective_id=0, has_side_effects=True),
    )(image_embeds, text_embeds)
    return both[:rows], both[rows:]


def solution(mesh):
    cycle, depth = mesh.shape["blk"], mesh.shape["grp"]
    window = min(20, cycle * depth // 2)
    chips = cycle // 2
    reach = 1
    while (2 * reach + 1) * depth - (depth - 1) < window:
        reach += 1
    slots = 2 * (reach + 1)

    def per_device(image_embeds, text_embeds):
        rows, width = image_embeds.shape
        shape = jax.ShapeDtypeStruct((rows, width), jnp.bfloat16)
        if chips == 4 and depth == 4 and window == 4 * depth:
            return square_call(depth, window, image_embeds, text_embeds)
        return pl.pallas_call(
            functools.partial(kernel, chips, depth, reach, window),
            out_shape=(shape, shape),
            in_specs=[pl.BlockSpec(memory_space=pl.ANY)] * 2,
            out_specs=(pl.BlockSpec(memory_space=pltpu.VMEM),) * 2,
            scratch_shapes=[
                pltpu.VMEM((2, slots, depth, rows, width), jnp.bfloat16),
                pltpu.VMEM((2, rows, width), jnp.float32),
                pltpu.VMEM((2, rows, rows), jnp.float32),
                pltpu.SemaphoreType.DMA((2,)),
                pltpu.SemaphoreType.DMA((2, 6 + 2 * reach, depth)),
                pltpu.SemaphoreType.DMA((2, slots, depth)),
            ],
            compiler_params=pltpu.CompilerParams(collective_id=0, has_side_effects=True),
        )(image_embeds, text_embeds)

    placed = P(("blk", "grp"), None)
    return jax.shard_map(
        per_device, mesh=mesh, in_specs=(placed, placed), out_specs=(placed, placed), check_vma=False
    )
```

```python
import functools

import jax
import jax.numpy as jnp
from jax import lax
from jax.experimental import pallas as pl
from jax.experimental.pallas import tpu as pltpu
from jax.sharding import PartitionSpec as P

LOGIT_SCALE = 10.0
BIAS_LOGIT = -2.0
EPSILON = 1e-06
PIECE_ROWS = 32
MESH = pl.DeviceIdType.MESH


def kernel(chips, depth, reach, window, image_ref, text_ref, image_out, text_out,
           held, total, own_scale, local_sem, send_sem, recv_sem):
    blk = lax.axis_index("blk")
    grp = lax.axis_index("grp")
    chip, core = blk // 2, blk % 2
    relayed = chips == 4 and reach == 2 and 4 * depth - 1 < window

    def view(kind):
        return (
            chip + kind * (chips - 1 - 2 * chip),
            core + kind * (1 - 2 * core),
            grp + kind * (depth - 1 - 2 * grp),
        )

    def device(kind, c, k, z):
        c = (c + chips) % chips
        linear = 2 * c + k
        return (
            linear + kind * (2 * chips - 1 - 2 * linear),
            z + kind * (depth - 1 - 2 * z),
        )

    first_kind = 1 - chip % 2 if relayed else 0
    kinds = (first_kind, 1 - first_kind)

    def need(k, z, d, source_k, source_z):
        offset = (2 * d + k - source_k) * depth + z - source_z
        return (offset >= 0) & (offset < window)

    def chip_need(z, d, source_k, source_z):
        return need(0, z, d, source_k, source_z) | need(1, z, d, source_k, source_z)

    def arrives(kind, d, source_z):
        c, k, z = view(kind)
        wanted = chip_need(z, d, k, source_z)
        if relayed:
            wanted = wanted | ((d == 2) & (c % 2 == 1))
        return wanted

    def copy(kind, path, source_slot, target_slot, z, target):
        return pltpu.make_async_remote_copy(
            src_ref=held.at[kind, source_slot, z],
            dst_ref=held.at[kind, target_slot, z],
            send_sem=send_sem.at[kind, path, z],
            recv_sem=recv_sem.at[kind, target_slot, z],
            device_id=target,
            device_id_type=MESH,
        )

    def own_sends(kind, z2):
        c, k, z = view(kind)
        sends = [
            ((z2 <= z) & (z + 1 < depth), 0, k, k, (c, k, z + 1)),
            ((z2 >= z) & (z >= 1), 1, k, k, (c, k, z - 1)),
        ]
        for d in range(1, reach + 1):
            wanted = chip_need(z, d, k, z2)
            if relayed and d == 1:
                inside = (z2 > 0) & (z2 < depth - 1)
                wanted = (c % 2 == 0) & (inside | (z2 == z))
            if relayed and d == 2:
                wanted = wanted | (c % 2 == 1)
            sends.append((wanted, 1 + d, k, 2 * d + k, (c + d, k, z)))
        sends.append((need(1 - k, z, 0, k, z2), 2 + reach, k, k, (c, 1 - k, z)))
        return sends

    def arrival_sends(kind, d, z2):
        c, k, z = view(kind)
        sends = []
        slot = 2 * d + k
        if relayed:
            sends.append(((c % 2 == 1) & (d == 2), 3 + reach, slot, 2 + k, (c - 1, k, z)))
            outer = (c % 2 == 1) & (d == 1) & ((z2 == 0) | (z2 == depth - 1))
            sends.append((outer & (z2 <= z) & (z + 1 < depth),
                          4 + 2 * reach, slot, slot, (c, k, z + 1)))
            sends.append((outer & (z2 >= z) & (z >= 1),
                          5 + 2 * reach, slot, slot, (c, k, z - 1)))
        sends.append((need(1 - k, z, d, k, z2), 3 + reach + d, slot, slot, (c, 1 - k, z)))
        return sends

    def each(kind, sends, z2, finish=False):
        for wanted, path, source_slot, target_slot, target in sends:
            @pl.when(wanted)
            def _():
                moved = copy(kind, path, source_slot, target_slot, z2, device(kind, *target))
                if finish:
                    moved.wait_send()
                else:
                    moved.start()

    def await_block(kind, slot, z2):
        c, k, z = view(kind)
        copy(kind, 0, slot, slot, z2, device(kind, c, 1 - k, z)).wait_recv()

    own = []
    for kind, ref in ((0, text_ref), (1, image_ref)):
        _, k, z = view(kind)
        loaded = pltpu.make_async_copy(ref, held.at[kind, k, z], local_sem.at[kind])
        loaded.start()
        own.append(loaded)

    barrier = pltpu.get_barrier_semaphore()

    def greet(target):
        pl.semaphore_signal(barrier, inc=1, device_id=target, device_id_type=MESH)

    greet((2 * chip + 1 - core, grp))
    if relayed:
        partners = [chip + 1 - 2 * (chip % 2), (chip + 2) % 4]
    else:
        partners = [(chip + d + chips) % chips for d in range(-reach, reach + 1) if d]
    for partner in partners:
        greet((2 * partner + core, grp))

    @pl.when(grp > 0)
    def _():
        greet((blk, grp - 1))

    @pl.when(grp < depth - 1)
    def _():
        greet((blk, grp + 1))

    for loaded in own:
        loaded.wait()
    pl.semaphore_wait(
        barrier,
        1 + len(partners) + (grp > 0).astype(jnp.int32) + (grp < depth - 1).astype(jnp.int32),
    )

    def own_block(kind):
        _, k, z = view(kind)
        return held[kind, k, z]

    def inverse_length(block):
        wide = block.astype(jnp.float32)
        return lax.rsqrt(jnp.sum(wide * wide, axis=-1, keepdims=True) + EPSILON)

    rows = held.shape[3]

    def tile(kind, slot, z2):
        _, k, z = view(kind)
        other = held[kind, slot, z2]
        mine = own_block(1 - kind)
        columns = jnp.broadcast_to(inverse_length(other), (rows, rows)).T
        product = lax.dot_general(
            mine, other, (((1,), (1,)), ((), ())), preferred_element_type=jnp.float32
        )
        logits = LOGIT_SCALE * product * own_scale[kind] * columns + BIAS_LOGIT
        inverse = jnp.exp(-logits)
        weights = 1.0 / (1.0 + inverse)
        diagonal = lax.broadcasted_iota(jnp.int32, (rows, rows), 0) == lax.broadcasted_iota(
            jnp.int32, (rows, rows), 1
        )
        first = ((slot == k) & (z2 == z)).astype(jnp.float32)
        positive = jnp.where(diagonal, first, 0.0)
        weights = jnp.where(positive > 0.5, -inverse * weights, weights)
        scaled = (weights * columns).astype(jnp.bfloat16)
        total[kind] += jnp.dot(scaled, other, preferred_element_type=jnp.float32)

    def position(kind, sign, distance):
        _, _, z = view(kind)
        z2 = z + sign * distance
        valid = (z2 >= 0) & (z2 < depth) & (distance >= 0)
        return z2, valid & ((sign > 0) | (distance > 0))

    def prepare(kind, carry):
        total[kind] = jnp.zeros(total.shape[1:], jnp.float32)
        own_scale[kind] = jnp.broadcast_to(inverse_length(own_block(1 - kind)), (rows, rows))
        return carry

    def start_own(kind):
        _, _, z = view(kind)
        each(kind, own_sends(kind, z), z)

    for kind in kinds:
        start_own(kind)
    lax.fori_loop(0, 2, prepare, 0)

    def half_turn(index, carry):
        turn = index // 2
        kind = first_kind + (index % 2) * (1 - 2 * first_kind)
        _, k, z = view(kind)

        for sign in (1, -1):
            z2, valid = position(kind, sign, turn)

            @pl.when(valid & (turn > 0))
            def _():
                await_block(kind, k, z2)
                each(kind, own_sends(kind, z2), z2)

        def stage(step, carry):
            d = jnp.where(step == 0, reach, jnp.where(step == 1, 0, reach - step + 1))
            distance = turn - (d > 0).astype(jnp.int32)
            for sign in (1, -1):
                z2, valid = position(kind, sign, distance)

                @pl.when((d > 0) & valid & arrives(kind, d, z2))
                def _():
                    await_block(kind, 2 * d + k, z2)
                    each(kind, arrival_sends(kind, d, z2), z2)

            def work(item, carry):
                source_k = (k + item // 2) % 2
                z2, valid = position(kind, 1 - 2 * (item % 2), distance)
                slot = 2 * d + source_k

                @pl.when(valid & need(k, z, d, source_k, z2))
                def _():
                    @pl.when(source_k != k)
                    def _():
                        await_block(kind, slot, z2)

                    tile(kind, slot, z2)

                return carry

            return lax.fori_loop(0, 4, work, carry)

        return lax.fori_loop(0, reach + 1, stage, carry)

    lax.fori_loop(0, 2 * (depth + 1), half_turn, 0)

    for kind, out in ((0, image_out), (1, text_out)):
        scale = own_scale[kind][:, :1]
        unit = own_block(1 - kind).astype(jnp.float32) * scale
        grad = LOGIT_SCALE * total[kind]
        inner = jnp.sum(unit * grad, axis=-1, keepdims=True)
        out[...] = ((grad - unit * inner) * scale).astype(out.dtype)

    def settle(z2, carry):
        for kind in (0, 1):
            each(kind, own_sends(kind, z2), z2, finish=True)
            for d in range(1, reach + 1):
                @pl.when(arrives(kind, d, z2))
                def _():
                    each(kind, arrival_sends(kind, d, z2), z2, finish=True)
        return carry

    lax.fori_loop(0, depth, settle, 0)


def ring_kernel(depth, window, pieces, early, relayed, passed, ahead, image_ref, text_ref, both_out,
                raw, img, txt, own_sum, text_sum, weights, sum_out, sum_in, part_out, part_core,
                part_x, part_y, load_sem, send, image_recv, text_recv, text_core_recv, sum_recv,
                part_recv, part_core_recv):
    blk = lax.axis_index("blk")
    z = lax.axis_index("grp")
    chip, core = blk // 2, blk % 2
    odd = chip % 2
    rows = raw.shape[1]
    span = rows // pieces
    parts, part_span = 2 * pieces, span // 2
    columns = window // depth * rows
    is_end = (z == 0) | (z == depth - 1)
    is_mid = (z > 0) & (z < depth - 1)
    inner = 1 - 2 * (z // 2)
    bare = (z == 0) & (core == 0)
    passed = jnp.where(bare, 0, passed)
    partner = (2 * chip + 1 - core, z)
    across = (2 * (chip + 1 - 2 * odd) + core, z)
    over = (2 * ((chip + 2) % 4) + core, z)
    corner = (2 * ((chip + 3 - 2 * odd) % 4) + core, z)

    def piece(j):
        return pl.ds(pl.multiple_of(j * span, span), span)

    def part(j):
        return pl.ds(pl.multiple_of(j * part_span, part_span), part_span)

    def slot_rows(slot, j):
        return pl.ds(pl.multiple_of(slot * rows + j * span, span), span)

    def remote(source, target, group, recv, device):
        return pltpu.make_async_remote_copy(
            src_ref=source, dst_ref=target, send_sem=send.at[group], recv_sem=recv,
            device_id=device, device_id_type=MESH,
        )

    def along(sign):
        return blk, jnp.minimum(jnp.maximum(z + sign, 0), depth - 1)

    def image_copy(source_z, sign, j, group=3):
        slot = (source_z - z - sign + 2 * depth - 1) % depth
        return remote(
            img.at[source_z, piece(j)], img.at[source_z, piece(j)], group,
            image_recv.at[slot, j], along(sign),
        )

    def await_image(source_z, j):
        slot = (source_z - z + 2 * depth - 1) % depth
        remote(
            img.at[source_z, piece(j)], img.at[source_z, piece(j)], 3,
            image_recv.at[slot, j], along(inner),
        ).wait_recv()

    def pass_image(source_z, sign, j):
        await_image(source_z, j)
        image_copy(source_z, sign, j).start()

    def sum_slot(target_z, there, sign):
        distance = target_z - there
        distance = jnp.maximum(distance, -distance)
        return jnp.where(sign == 1 - 2 * (there // 2), distance, depth - 1 + distance)

    def sum_copy(target_z, sign, j):
        there = along(sign)
        return remote(
            sum_out.at[target_z, part(j)], sum_in.at[(1 - sign) // 2, target_z, part(j)], 2,
            sum_recv.at[sum_slot(target_z, there[1], sign), j], there,
        )

    def await_sum(target_z, sign, j):
        remote(
            sum_out.at[target_z, part(j)], sum_in.at[(1 - sign) // 2, target_z, part(j)], 2,
            sum_recv.at[sum_slot(target_z, z, sign), j], along(inner),
        ).wait_recv()

    def text_copy(source_slot, target_slot, recv, j, device):
        return remote(
            txt.at[slot_rows(source_slot, j)], txt.at[slot_rows(target_slot, j)], 0, recv, device
        )

    def text_over(j):
        return text_copy(0, 4, text_recv.at[1, j], j, over)

    def text_across(j):
        return text_copy(4 * odd, 2, text_recv.at[0, j], j, across)

    def text_corner(j):
        return text_copy(0, 2, text_recv.at[0, j], j, corner)

    def text_to_core(slot, j):
        target = slot + 1 - 2 * core
        return text_copy(slot, target, text_core_recv.at[target // 2], j, partner)

    def part_to_core(index, j):
        return remote(
            part_out.at[2 * index + 1, part(j)], part_core.at[index, part(j)], 1,
            part_core_recv.at[j], partner,
        )

    def part_across(j):
        return remote(
            part_out.at[2, part(j)], part_x.at[part(j)], 1, part_recv.at[0, j], across
        )

    def part_corner(j):
        return remote(
            part_out.at[2, part(j)], part_x.at[part(j)], 1, part_recv.at[0, j], corner
        )

    def part_over(j):
        return remote(
            part_out.at[4, part(j)], part_y.at[part(j)], 1, part_recv.at[1, j], over
        )

    def span_loop(low, high, body):
        def step(j, carry):
            body(j)
            return carry

        lax.fori_loop(low, high, step, 0)

    def loop(count, body):
        span_loop(0, count, body)

    loads = []
    for kind, ref in ((0, image_ref), (1, text_ref)):
        load = pltpu.make_async_copy(ref, raw.at[kind], load_sem.at[kind])
        load.start()
        loads.append(load)

    barrier = pltpu.get_barrier_semaphore()

    def greet(target):
        pl.semaphore_signal(barrier, inc=1, device_id=target, device_id_type=MESH)

    for target in (partner, across, over, corner):
        greet(target)

    @pl.when(z > 0)
    def _():
        greet((blk, z - 1))

    @pl.when(z < depth - 1)
    def _():
        greet((blk, z + 1))

    def inverse_length(wide):
        return lax.rsqrt(jnp.sum(wide * wide, axis=-1, keepdims=True) + EPSILON)

    def unit_low(kind):
        wide = raw[kind].astype(jnp.float32)
        return (wide * inverse_length(wide)).astype(jnp.bfloat16)

    loads[0].wait()
    img[z] = unit_low(0)
    loads[1].wait()
    txt[pl.ds(0, rows)] = unit_low(1)
    pl.semaphore_wait(
        barrier, 4 + (z > 0).astype(jnp.int32) + (z < depth - 1).astype(jnp.int32)
    )

    def image_start(j):
        @pl.when(is_end | (j < early))
        def _():
            image_copy(z, inner, j, 2).start()

        @pl.when(is_mid & (j < early))
        def _():
            image_copy(z, -inner, j).start()

    def text_start(j):
        text_over(j).start()

        @pl.when(odd == 0)
        def _():
            text_across(j).start()

        @pl.when((odd == 1) & (j >= relayed))
        def _():
            text_corner(j).start()

        @pl.when(core == 0)
        def _():
            text_to_core(0, j).start()

    loop(pieces, image_start)
    loop(pieces, text_start)
    text_sum[...] = jnp.zeros(text_sum.shape, jnp.float32)

    def pass_inner(q):
        late = q >= early + pieces
        from_far = (q >= early) & (q < early + pieces)
        j = q - jnp.where(late, pieces, jnp.where(from_far, early, 0))
        pass_image(z + inner * (1 + from_far), -inner, j)

    def first(j):
        @pl.when(j < pieces)
        def _():
            text_over(j).wait_recv()

            @pl.when((odd == 1) & (j < relayed))
            def _():
                text_across(j).start()

            @pl.when(core == 1)
            def _():
                text_to_core(4, j).start()

        def second(i):
            text_across(i).wait_recv()
            text_to_core(2, i).start()

        @pl.when((odd == 1) & (j < pieces))
        def _():
            second(j)

        @pl.when(is_mid)
        def _():
            pass_inner(j)

            @pl.when(j < pieces)
            def _():
                pass_image(z - inner, inner, j)

            @pl.when(j == pieces - 1)
            def _():
                span_loop(early, pieces, lambda i: image_copy(z, inner, i, 2).start())

        @pl.when((odd == 0) & (j >= ahead))
        def _():
            second(j - ahead)

    loop(pieces + ahead, first)
    waiting = (odd == 0) & (core == 1)

    @pl.when(is_mid & waiting)
    def _():
        span_loop(pieces + ahead, 2 * pieces - 1, pass_inner)

    for index in (0, 1):
        slot = 2 * index + 1
        block = txt.at[pl.ds(slot * rows, rows)]
        remote(block, block, 0, text_core_recv.at[index], partner).wait_recv()

    def text_window(source):
        start = pl.multiple_of(jnp.where(source < z, rows, 0), rows)
        return pl.ds(start, columns)

    def slopes_of(source, start, count):
        some = pl.ds(start, count)
        product = lax.dot_general(
            img[source, some], txt[text_window(source)], (((1,), (1,)), ((), ())),
            preferred_element_type=jnp.float32,
        )
        inverse = jnp.exp(-BIAS_LOGIT - LOGIT_SCALE * product)
        slope = 1.0 / (1.0 + inverse)
        shape = (count, columns)
        diagonal = lax.broadcasted_iota(jnp.int32, shape, 0) + start == lax.broadcasted_iota(
            jnp.int32, shape, 1
        )
        positive = jnp.where(diagonal, (source == z).astype(jnp.float32), 0.0)
        slope = jnp.where(positive > 0.5, -inverse * slope, slope).astype(jnp.bfloat16)
        weights[source, some] = slope
        return slope

    def sums_of(source, start, count, slope):
        own_sum[source, pl.ds(start, count)] = jnp.dot(
            slope, txt[text_window(source)], preferred_element_type=jnp.float32
        )

    def weigh(source, start, count):
        sums_of(source, start, count, slopes_of(source, start, count))

    def add_texts(*sources):
        slopes = jnp.concatenate([weights[source] for source in sources])
        images = jnp.concatenate([img[source] for source in sources])
        text_sum[text_window(sources[0])] += lax.dot_general(
            slopes, images, (((0,), (0,)), ((), ())), preferred_element_type=jnp.float32
        )

    def relay(target_z, sign, j):
        await_sum(target_z, sign, j)
        arrived = sum_in[(1 - sign) // 2, target_z, part(j)].astype(jnp.float32)
        sum_out[target_z, part(j)] = (own_sum[target_z, part(j)] + arrived).astype(jnp.bfloat16)
        sum_copy(target_z, sign, j).start()

    def near(j):
        relay(z + inner, inner, j)

    def part_rows(slot, j):
        return text_sum[pl.ds(pl.multiple_of(slot * rows + j * part_span, part_span), part_span)]

    def part_first(j):
        for index in (0, 1):
            slot = 2 * index + 1
            part_out[slot, part(j)] = part_rows(slot, j).astype(jnp.bfloat16)
            part_to_core(index, j).start()

    @pl.when(is_end)
    def _():
        group = pieces // 2
        near_z, far_z, edge_z = z + 2 * inner, z + 3 * inner, z + inner

        def take(source, low, count):
            span_loop(low, low + count, lambda j: await_image(source, j))
            weigh(source, pl.multiple_of(low * span, count * span), count * span)
            some = pl.ds(pl.multiple_of(low * span, count * span), count * span)
            sum_out[source, some] = own_sum[source, some].astype(jnp.bfloat16)

        def give(source, low, high):
            span_loop(2 * low, 2 * high, lambda j: sum_copy(source, inner, j).start())

        def far_step(j):
            take(far_z, j, 1)
            give(far_z, j, j + 1)

        take(near_z, 0, group)
        give(near_z, 0, group)
        weigh(z, 0, rows)
        add_texts(z)
        span_loop(0, group, far_step)
        take(edge_z, 0, group)
        span_loop(group, pieces, far_step)
        take(near_z, group, group)
        give(near_z, group, pieces)
        add_texts(far_z, near_z)
        span_loop(group, pieces, lambda j: await_image(edge_z, j))
        slopes_of(edge_z, group * span, group * span)
        add_texts(edge_z)
        loop(parts, part_first)
        last = pl.ds(group * span, group * span)
        sums_of(edge_z, group * span, group * span, weights[edge_z, last])
        sum_out[edge_z, last] = own_sum[edge_z, last].astype(jnp.bfloat16)
        give(edge_z, 0, pieces)

    @pl.when(is_mid)
    def _():
        def rest(j):
            image_copy(z, -inner, j).start()

        def image_step(index):
            @pl.when((index == 1) & ~waiting)
            def _():
                span_loop(pieces + ahead, 2 * pieces - 1, pass_inner)

            @pl.when(index == 2)
            def _():
                pass_inner(2 * pieces - 1)

                @pl.when(core == 0)
                def _():
                    span_loop(early, pieces, rest)

            @pl.when(index == 3)
            def _():
                span_loop(0, parts // 4, near)

            step = (index == 2) * 1 - (index == 0) * 1 + (index == 3) * 2
            source = z + step * inner
            weigh(source, 0, rows)
            add_texts(source)

        loop(4, image_step)

        @pl.when(core == 1)
        def _():
            span_loop(early, pieces, rest)

        loop(parts, part_first)

    def part_second(j):
        pair = part_core.at[0, pl.ds(0, 2 * part_span)]
        remote(pair, pair, 1, part_core_recv.at[j], partner).wait_recv()
        side = part_core[1 - core, part(j)].astype(jnp.float32)
        part_out[2, part(j)] = (part_rows(2, j) + side).astype(jnp.bfloat16)

        @pl.when((odd == 1) | (j < passed))
        def _():
            part_across(j).start()

        @pl.when((odd == 0) & (j >= passed) & (~bare | (j < parts // 2)))
        def _():
            part_corner(j).start()

        @pl.when(((odd == 0) | (j >= passed)) & ~bare)
        def _():
            part_third(j, 0.0)

    def part_third(j, arrived):
        side = part_core[1, part(j)].astype(jnp.float32)
        side = jnp.where(core == 1, side, 0.0) + arrived
        part_out[4, part(j)] = (part_rows(4, j) + side).astype(jnp.bfloat16)
        part_over(j).start()

    def part_relay(j):
        part_across(j).wait_recv()
        part_third(j, part_x[part(j)].astype(jnp.float32))

    def stage(i):
        j = i - parts // 2 - 1

        @pl.when(is_mid & (i < parts))
        def _():
            relay(z + 2 * inner, inner, i)

        @pl.when(is_mid & (j >= parts // 4) & (j < parts))
        def _():
            near(j)

        @pl.when(is_mid & (j > 0) & (j <= parts))
        def _():
            relay(z - inner, -inner, j - 1)

        @pl.when((odd == 1) & (i >= parts - 1) & (i - parts + 1 < passed))
        def _():
            part_relay(i - parts + 1)

    head = parts // 2
    span_loop(0, head, stage)
    loop(parts, part_second)
    span_loop(head, 2 * parts - 1, stage)

    def finish(kind, out, total, j):
        wide = raw[kind, piece(j)].astype(jnp.float32)
        scale = inverse_length(wide)
        unit = wide * scale
        grad = LOGIT_SCALE * total
        radial = jnp.sum(unit * grad, axis=-1, keepdims=True)
        out[piece(j)] = ((grad - unit * radial) * scale).astype(out.dtype)

    def finish_text(j):
        direct = (odd == 0) | (2 * j >= passed)
        for half in (0, 1):
            @pl.when(~bare)
            def _():
                part_over(2 * j + half).wait_recv()

            @pl.when(direct)
            def _():
                part_across(2 * j + half).wait_recv()

        total = text_sum[slot_rows(0, j)]
        total += jnp.where(bare, 0.0, part_y[piece(j)].astype(jnp.float32))
        total += jnp.where(core == 0, part_core[0, piece(j)].astype(jnp.float32), 0.0)
        total += jnp.where(direct, part_x[piece(j)].astype(jnp.float32), 0.0)
        finish(1, both_out.at[pl.ds(rows, rows)], total, j)

    def finish_image(j):
        for half in (0, 1):
            await_sum(z, -inner, 2 * j + half)

        @pl.when(is_mid)
        def _():
            for half in (0, 1):
                await_sum(z, inner, 2 * j + half)

        total = own_sum[z, piece(j)] + sum_in[(1 + inner) // 2, z, piece(j)].astype(jnp.float32)
        other = sum_in[(1 - inner) // 2, z, piece(j)].astype(jnp.float32)
        finish(0, both_out.at[pl.ds(0, rows)], total + jnp.where(is_mid, other, 0.0), j)

    def finish_both(j):
        finish_image(j)

        @pl.when(bare & (odd == 0) & (j == 0))
        def _():
            span_loop(parts // 2, parts, lambda i: part_corner(i).start())

        finish_text(j)

    loop(pieces, finish_both)

    def settle(group, count=depth):
        some = img.at[pl.ds(0, count)]
        remote(some, some, group, image_recv.at[0, 0], partner).wait_send()

    settle(0)
    settle(2)

    @pl.when(bare)
    def _():
        settle(1, 3)

    @pl.when(~bare)
    def _():
        settle(1)

    @pl.when(is_mid)
    def _():
        settle(3)


def square_call(depth, window, image_embeds, text_embeds):
    rows, width = image_embeds.shape
    slots = window // depth + 1
    pieces = rows // PIECE_ROWS
    early, relayed, passed, ahead = 3 * pieces // 4, 3 * pieces // 4, 2 * pieces, pieces // 2
    low, wide = jnp.bfloat16, jnp.float32
    both = pl.pallas_call(
        functools.partial(ring_kernel, depth, window, pieces, early, relayed, passed, ahead),
        out_shape=pltpu.VMEM((2 * rows, width), low),
        in_specs=[pl.BlockSpec(memory_space=pl.ANY)] * 2,
        out_specs=pl.BlockSpec(memory_space=pltpu.VMEM),
        scratch_shapes=[
            pltpu.VMEM((2, rows, width), low),
            pltpu.VMEM((depth, rows, width), low),
            pltpu.VMEM((slots * rows, width), low),
            pltpu.VMEM((depth, rows, width), wide),
            pltpu.VMEM((slots * rows, width), wide),
            pltpu.VMEM((depth, rows, (slots - 1) * rows), low),
            pltpu.VMEM((depth, rows, width), low),
            pltpu.VMEM((2, depth, rows, width), low),
            pltpu.VMEM((slots, rows, width), low),
            pltpu.VMEM((2, rows, width), low),
            pltpu.VMEM((rows, width), low),
            pltpu.VMEM((rows, width), low),
            pltpu.SemaphoreType.DMA((2,)),
            pltpu.SemaphoreType.DMA((4,)),
            pltpu.SemaphoreType.DMA((depth - 1, pieces)),
            pltpu.SemaphoreType.DMA((2, pieces)),
            pltpu.SemaphoreType.DMA((2,)),
            pltpu.SemaphoreType.DMA((depth + 1, 2 * pieces)),
            pltpu.SemaphoreType.DMA((2, 2 * pieces)),
            pltpu.SemaphoreType.DMA((2 * pieces,)),
        ],
        compiler_params=pltpu.CompilerParams(collective_id=0, has_side_effects=True),
    )(image_embeds, text_embeds)
    return both[:rows], both[rows:]


def solution(mesh):
    cycle, depth = mesh.shape["blk"], mesh.shape["grp"]
    window = min(20, cycle * depth // 2)
    chips = cycle // 2
    reach = 1
    while (2 * reach + 1) * depth - (depth - 1) < window:
        reach += 1
    slots = 2 * (reach + 1)

    def per_device(image_embeds, text_embeds):
        rows, width = image_embeds.shape
        shape = jax.ShapeDtypeStruct((rows, width), jnp.bfloat16)
        if chips == 4 and depth == 4 and window == 4 * depth:
            return square_call(depth, window, image_embeds, text_embeds)
        return pl.pallas_call(
            functools.partial(kernel, chips, depth, reach, window),
            out_shape=(shape, shape),
            in_specs=[pl.BlockSpec(memory_space=pl.ANY)] * 2,
            out_specs=(pl.BlockSpec(memory_space=pltpu.VMEM),) * 2,
            scratch_shapes=[
                pltpu.VMEM((2, slots, depth, rows, width), jnp.bfloat16),
                pltpu.VMEM((2, rows, width), jnp.float32),
                pltpu.VMEM((2, rows, rows), jnp.float32),
                pltpu.SemaphoreType.DMA((2,)),
                pltpu.SemaphoreType.DMA((2, 6 + 2 * reach, depth)),
                pltpu.SemaphoreType.DMA((2, slots, depth)),
            ],
            compiler_params=pltpu.CompilerParams(collective_id=0, has_side_effects=True),
        )(image_embeds, text_embeds)

    placed = P(("blk", "grp"), None)
    return jax.shard_map(
        per_device, mesh=mesh, in_specs=(placed, placed), out_specs=(placed, placed), check_vma=False
    )
```

```python
import functools

import jax
import jax.numpy as jnp
from jax import lax
from jax.experimental import pallas as pl
from jax.experimental.pallas import tpu as pltpu
from jax.sharding import PartitionSpec as P

LOGIT_SCALE = 10.0
BIAS_LOGIT = -2.0
EPSILON = 1e-06
PIECE_ROWS = 32
MESH = pl.DeviceIdType.MESH


def kernel(chips, depth, reach, window, image_ref, text_ref, image_out, text_out,
           held, total, own_scale, local_sem, send_sem, recv_sem):
    blk = lax.axis_index("blk")
    grp = lax.axis_index("grp")
    chip, core = blk // 2, blk % 2
    relayed = chips == 4 and reach == 2 and 4 * depth - 1 < window

    def view(kind):
        return (
            chip + kind * (chips - 1 - 2 * chip),
            core + kind * (1 - 2 * core),
            grp + kind * (depth - 1 - 2 * grp),
        )

    def device(kind, c, k, z):
        c = (c + chips) % chips
        linear = 2 * c + k
        return (
            linear + kind * (2 * chips - 1 - 2 * linear),
            z + kind * (depth - 1 - 2 * z),
        )

    first_kind = 1 - chip % 2 if relayed else 0
    kinds = (first_kind, 1 - first_kind)

    def need(k, z, d, source_k, source_z):
        offset = (2 * d + k - source_k) * depth + z - source_z
        return (offset >= 0) & (offset < window)

    def chip_need(z, d, source_k, source_z):
        return need(0, z, d, source_k, source_z) | need(1, z, d, source_k, source_z)

    def arrives(kind, d, source_z):
        c, k, z = view(kind)
        wanted = chip_need(z, d, k, source_z)
        if relayed:
            wanted = wanted | ((d == 2) & (c % 2 == 1))
        return wanted

    def copy(kind, path, source_slot, target_slot, z, target):
        return pltpu.make_async_remote_copy(
            src_ref=held.at[kind, source_slot, z],
            dst_ref=held.at[kind, target_slot, z],
            send_sem=send_sem.at[kind, path, z],
            recv_sem=recv_sem.at[kind, target_slot, z],
            device_id=target,
            device_id_type=MESH,
        )

    def own_sends(kind, z2):
        c, k, z = view(kind)
        sends = [
            ((z2 <= z) & (z + 1 < depth), 0, k, k, (c, k, z + 1)),
            ((z2 >= z) & (z >= 1), 1, k, k, (c, k, z - 1)),
        ]
        for d in range(1, reach + 1):
            wanted = chip_need(z, d, k, z2)
            if relayed and d == 1:
                inside = (z2 > 0) & (z2 < depth - 1)
                wanted = (c % 2 == 0) & (inside | (z2 == z))
            if relayed and d == 2:
                wanted = wanted | (c % 2 == 1)
            sends.append((wanted, 1 + d, k, 2 * d + k, (c + d, k, z)))
        sends.append((need(1 - k, z, 0, k, z2), 2 + reach, k, k, (c, 1 - k, z)))
        return sends

    def arrival_sends(kind, d, z2):
        c, k, z = view(kind)
        sends = []
        slot = 2 * d + k
        if relayed:
            sends.append(((c % 2 == 1) & (d == 2), 3 + reach, slot, 2 + k, (c - 1, k, z)))
            outer = (c % 2 == 1) & (d == 1) & ((z2 == 0) | (z2 == depth - 1))
            sends.append((outer & (z2 <= z) & (z + 1 < depth),
                          4 + 2 * reach, slot, slot, (c, k, z + 1)))
            sends.append((outer & (z2 >= z) & (z >= 1),
                          5 + 2 * reach, slot, slot, (c, k, z - 1)))
        sends.append((need(1 - k, z, d, k, z2), 3 + reach + d, slot, slot, (c, 1 - k, z)))
        return sends

    def each(kind, sends, z2, finish=False):
        for wanted, path, source_slot, target_slot, target in sends:
            @pl.when(wanted)
            def _():
                moved = copy(kind, path, source_slot, target_slot, z2, device(kind, *target))
                if finish:
                    moved.wait_send()
                else:
                    moved.start()

    def await_block(kind, slot, z2):
        c, k, z = view(kind)
        copy(kind, 0, slot, slot, z2, device(kind, c, 1 - k, z)).wait_recv()

    own = []
    for kind, ref in ((0, text_ref), (1, image_ref)):
        _, k, z = view(kind)
        loaded = pltpu.make_async_copy(ref, held.at[kind, k, z], local_sem.at[kind])
        loaded.start()
        own.append(loaded)

    barrier = pltpu.get_barrier_semaphore()

    def greet(target):
        pl.semaphore_signal(barrier, inc=1, device_id=target, device_id_type=MESH)

    greet((2 * chip + 1 - core, grp))
    if relayed:
        partners = [chip + 1 - 2 * (chip % 2), (chip + 2) % 4]
    else:
        partners = [(chip + d + chips) % chips for d in range(-reach, reach + 1) if d]
    for partner in partners:
        greet((2 * partner + core, grp))

    @pl.when(grp > 0)
    def _():
        greet((blk, grp - 1))

    @pl.when(grp < depth - 1)
    def _():
        greet((blk, grp + 1))

    for loaded in own:
        loaded.wait()
    pl.semaphore_wait(
        barrier,
        1 + len(partners) + (grp > 0).astype(jnp.int32) + (grp < depth - 1).astype(jnp.int32),
    )

    def own_block(kind):
        _, k, z = view(kind)
        return held[kind, k, z]

    def inverse_length(block):
        wide = block.astype(jnp.float32)
        return lax.rsqrt(jnp.sum(wide * wide, axis=-1, keepdims=True) + EPSILON)

    rows = held.shape[3]

    def tile(kind, slot, z2):
        _, k, z = view(kind)
        other = held[kind, slot, z2]
        mine = own_block(1 - kind)
        columns = jnp.broadcast_to(inverse_length(other), (rows, rows)).T
        product = lax.dot_general(
            mine, other, (((1,), (1,)), ((), ())), preferred_element_type=jnp.float32
        )
        logits = LOGIT_SCALE * product * own_scale[kind] * columns + BIAS_LOGIT
        inverse = jnp.exp(-logits)
        weights = 1.0 / (1.0 + inverse)
        diagonal = lax.broadcasted_iota(jnp.int32, (rows, rows), 0) == lax.broadcasted_iota(
            jnp.int32, (rows, rows), 1
        )
        first = ((slot == k) & (z2 == z)).astype(jnp.float32)
        positive = jnp.where(diagonal, first, 0.0)
        weights = jnp.where(positive > 0.5, -inverse * weights, weights)
        scaled = (weights * columns).astype(jnp.bfloat16)
        total[kind] += jnp.dot(scaled, other, preferred_element_type=jnp.float32)

    def position(kind, sign, distance):
        _, _, z = view(kind)
        z2 = z + sign * distance
        valid = (z2 >= 0) & (z2 < depth) & (distance >= 0)
        return z2, valid & ((sign > 0) | (distance > 0))

    def prepare(kind, carry):
        total[kind] = jnp.zeros(total.shape[1:], jnp.float32)
        own_scale[kind] = jnp.broadcast_to(inverse_length(own_block(1 - kind)), (rows, rows))
        return carry

    def start_own(kind):
        _, _, z = view(kind)
        each(kind, own_sends(kind, z), z)

    for kind in kinds:
        start_own(kind)
    lax.fori_loop(0, 2, prepare, 0)

    def half_turn(index, carry):
        turn = index // 2
        kind = first_kind + (index % 2) * (1 - 2 * first_kind)
        _, k, z = view(kind)

        for sign in (1, -1):
            z2, valid = position(kind, sign, turn)

            @pl.when(valid & (turn > 0))
            def _():
                await_block(kind, k, z2)
                each(kind, own_sends(kind, z2), z2)

        def stage(step, carry):
            d = jnp.where(step == 0, reach, jnp.where(step == 1, 0, reach - step + 1))
            distance = turn - (d > 0).astype(jnp.int32)
            for sign in (1, -1):
                z2, valid = position(kind, sign, distance)

                @pl.when((d > 0) & valid & arrives(kind, d, z2))
                def _():
                    await_block(kind, 2 * d + k, z2)
                    each(kind, arrival_sends(kind, d, z2), z2)

            def work(item, carry):
                source_k = (k + item // 2) % 2
                z2, valid = position(kind, 1 - 2 * (item % 2), distance)
                slot = 2 * d + source_k

                @pl.when(valid & need(k, z, d, source_k, z2))
                def _():
                    @pl.when(source_k != k)
                    def _():
                        await_block(kind, slot, z2)

                    tile(kind, slot, z2)

                return carry

            return lax.fori_loop(0, 4, work, carry)

        return lax.fori_loop(0, reach + 1, stage, carry)

    lax.fori_loop(0, 2 * (depth + 1), half_turn, 0)

    for kind, out in ((0, image_out), (1, text_out)):
        scale = own_scale[kind][:, :1]
        unit = own_block(1 - kind).astype(jnp.float32) * scale
        grad = LOGIT_SCALE * total[kind]
        inner = jnp.sum(unit * grad, axis=-1, keepdims=True)
        out[...] = ((grad - unit * inner) * scale).astype(out.dtype)

    def settle(z2, carry):
        for kind in (0, 1):
            each(kind, own_sends(kind, z2), z2, finish=True)
            for d in range(1, reach + 1):
                @pl.when(arrives(kind, d, z2))
                def _():
                    each(kind, arrival_sends(kind, d, z2), z2, finish=True)
        return carry

    lax.fori_loop(0, depth, settle, 0)


def ring_kernel(depth, window, pieces, early, relayed, passed, ahead, image_ref, text_ref, both_out,
                raw, img, txt, own_sum, text_sum, weights, sum_out, sum_in, part_out, part_core,
                part_x, part_y, load_sem, send, image_recv, text_recv, text_core_recv, sum_recv,
                part_recv, part_core_recv):
    blk = lax.axis_index("blk")
    z = lax.axis_index("grp")
    chip, core = blk // 2, blk % 2
    odd = chip % 2
    rows = raw.shape[1]
    span = rows // pieces
    parts, part_span = 2 * pieces, span // 2
    columns = window // depth * rows
    is_end = (z == 0) | (z == depth - 1)
    is_mid = (z > 0) & (z < depth - 1)
    inner = 1 - 2 * (z // 2)
    bare = (z == 0) & (core == 0)
    passed = jnp.where(bare, 0, passed)
    partner = (2 * chip + 1 - core, z)
    across = (2 * (chip + 1 - 2 * odd) + core, z)
    over = (2 * ((chip + 2) % 4) + core, z)
    corner = (2 * ((chip + 3 - 2 * odd) % 4) + core, z)

    def piece(j):
        return pl.ds(pl.multiple_of(j * span, span), span)

    def part(j):
        return pl.ds(pl.multiple_of(j * part_span, part_span), part_span)

    def slot_rows(slot, j):
        return pl.ds(pl.multiple_of(slot * rows + j * span, span), span)

    def remote(source, target, group, recv, device):
        return pltpu.make_async_remote_copy(
            src_ref=source, dst_ref=target, send_sem=send.at[group], recv_sem=recv,
            device_id=device, device_id_type=MESH,
        )

    def along(sign):
        return blk, jnp.minimum(jnp.maximum(z + sign, 0), depth - 1)

    def image_copy(source_z, sign, j, group=3):
        slot = (source_z - z - sign + 2 * depth - 1) % depth
        return remote(
            img.at[source_z, piece(j)], img.at[source_z, piece(j)], group,
            image_recv.at[slot, j], along(sign),
        )

    def await_image(source_z, j):
        slot = (source_z - z + 2 * depth - 1) % depth
        remote(
            img.at[source_z, piece(j)], img.at[source_z, piece(j)], 3,
            image_recv.at[slot, j], along(inner),
        ).wait_recv()

    def pass_image(source_z, sign, j):
        await_image(source_z, j)
        image_copy(source_z, sign, j).start()

    def sum_slot(target_z, there, sign, j):
        distance = target_z - there
        distance = jnp.maximum(distance, -distance)
        inward = sign == 1 - 2 * (there // 2)
        own = distance == 0
        row = jnp.where(own, 0, jnp.where(inward, distance, depth - 1))
        column = jnp.where(own, j // 2 + jnp.where(inward, 0, pieces), j)
        return sum_recv.at[row, column]

    def sum_copy(target_z, sign, j):
        there = along(sign)
        return remote(
            sum_out.at[target_z, part(j)], sum_in.at[(1 - sign) // 2, target_z, part(j)], 2,
            sum_slot(target_z, there[1], sign, j), there,
        )

    def await_sum(target_z, sign, j):
        remote(
            sum_out.at[target_z, part(j)], sum_in.at[(1 - sign) // 2, target_z, part(j)], 2,
            sum_slot(target_z, z, sign, j), along(inner),
        ).wait_recv()

    def text_copy(source_slot, target_slot, recv, j, device):
        return remote(
            txt.at[slot_rows(source_slot, j)], txt.at[slot_rows(target_slot, j)], 0, recv, device
        )

    def text_over(j):
        return text_copy(0, 4, text_recv.at[1, j], j, over)

    def text_across(j):
        return text_copy(4 * odd, 2, text_recv.at[0, j], j, across)

    def text_corner(j):
        return text_copy(0, 2, text_recv.at[0, j], j, corner)

    def text_to_core(slot, j):
        target = slot + 1 - 2 * core
        return text_copy(slot, target, text_core_recv.at[target // 2], j, partner)

    def part_to_core(index, j):
        return remote(
            part_out.at[2 * index + 1, part(j)], part_core.at[index, part(j)], 1,
            part_core_recv.at[j], partner,
        )

    def part_across(j):
        return remote(
            part_out.at[2, part(j)], part_x.at[part(j)], 1, part_recv.at[j // pieces, j % pieces], across
        )

    def part_corner(j):
        return remote(
            part_out.at[2, part(j)], part_x.at[part(j)], 1, part_recv.at[j // pieces, j % pieces], corner
        )

    def part_over(j):
        return remote(
            part_out.at[4, part(j)], part_y.at[part(j)], 1, part_recv.at[2, j // 2], over
        )

    def span_loop(low, high, body):
        def step(j, carry):
            body(j)
            return carry

        lax.fori_loop(low, high, step, 0)

    def loop(count, body):
        span_loop(0, count, body)

    loads = []
    for kind, ref in ((0, image_ref), (1, text_ref)):
        load = pltpu.make_async_copy(ref, raw.at[kind], load_sem.at[kind])
        load.start()
        loads.append(load)

    barrier = pltpu.get_barrier_semaphore()

    def greet(target):
        pl.semaphore_signal(barrier, inc=1, device_id=target, device_id_type=MESH)

    for target in (partner, across, over, corner):
        greet(target)

    @pl.when(z > 0)
    def _():
        greet((blk, z - 1))

    @pl.when(z < depth - 1)
    def _():
        greet((blk, z + 1))

    def inverse_length(wide):
        return lax.rsqrt(jnp.sum(wide * wide, axis=-1, keepdims=True) + EPSILON)

    def unit_low(kind):
        wide = raw[kind].astype(jnp.float32)
        return (wide * inverse_length(wide)).astype(jnp.bfloat16)

    loads[0].wait()
    img[z] = unit_low(0)
    loads[1].wait()
    txt[pl.ds(0, rows)] = unit_low(1)
    pl.semaphore_wait(
        barrier, 4 + (z > 0).astype(jnp.int32) + (z < depth - 1).astype(jnp.int32)
    )

    def image_start(j):
        @pl.when(is_end | (j < early))
        def _():
            image_copy(z, inner, j, 2).start()

        @pl.when(is_mid & (j < early))
        def _():
            image_copy(z, -inner, j).start()

    def text_start(j):
        text_over(j).start()

        @pl.when(odd == 0)
        def _():
            text_across(j).start()

        @pl.when((odd == 1) & (j >= relayed))
        def _():
            text_corner(j).start()

        @pl.when(core == 0)
        def _():
            text_to_core(0, j).start()

    loop(pieces, image_start)
    loop(pieces, text_start)
    text_sum[...] = jnp.zeros(text_sum.shape, jnp.float32)

    def pass_inner(q):
        late = q >= early + pieces
        from_far = (q >= early) & (q < early + pieces)
        j = q - jnp.where(late, pieces, jnp.where(from_far, early, 0))
        pass_image(z + inner * (1 + from_far), -inner, j)

    def first(j):
        @pl.when(j < pieces)
        def _():
            text_over(j).wait_recv()

            @pl.when((odd == 1) & (j < relayed))
            def _():
                text_across(j).start()

            @pl.when(core == 1)
            def _():
                text_to_core(4, j).start()

        def second(i):
            text_across(i).wait_recv()
            text_to_core(2, i).start()

        @pl.when((odd == 1) & (j < pieces))
        def _():
            second(j)

        @pl.when(is_mid)
        def _():
            pass_inner(j)

            @pl.when(j < pieces)
            def _():
                pass_image(z - inner, inner, j)

            @pl.when(j == pieces - 1)
            def _():
                span_loop(early, pieces, lambda i: image_copy(z, inner, i, 2).start())

        @pl.when((odd == 0) & (j >= ahead))
        def _():
            second(j - ahead)

    loop(pieces + ahead, first)
    waiting = (odd == 0) & (core == 1)

    @pl.when(is_mid & waiting)
    def _():
        span_loop(pieces + ahead, 2 * pieces - 1, pass_inner)

    for index in (0, 1):
        slot = 2 * index + 1
        block = txt.at[pl.ds(slot * rows, rows)]
        remote(block, block, 0, text_core_recv.at[index], partner).wait_recv()

    def text_window(source):
        start = pl.multiple_of(jnp.where(source < z, rows, 0), rows)
        return pl.ds(start, columns)

    def slopes_of(source, start, count):
        some = pl.ds(start, count)
        product = lax.dot_general(
            img[source, some], txt[text_window(source)], (((1,), (1,)), ((), ())),
            preferred_element_type=jnp.float32,
        )
        inverse = jnp.exp(-BIAS_LOGIT - LOGIT_SCALE * product)
        slope = 1.0 / (1.0 + inverse)
        shape = (count, columns)
        diagonal = lax.broadcasted_iota(jnp.int32, shape, 0) + start == lax.broadcasted_iota(
            jnp.int32, shape, 1
        )
        positive = jnp.where(diagonal, (source == z).astype(jnp.float32), 0.0)
        slope = jnp.where(positive > 0.5, -inverse * slope, slope).astype(jnp.bfloat16)
        weights[source, some] = slope
        return slope

    def sums_of(source, start, count, slope):
        own_sum[source, pl.ds(start, count)] = jnp.dot(
            slope, txt[text_window(source)], preferred_element_type=jnp.float32
        )

    def weigh(source, start, count):
        sums_of(source, start, count, slopes_of(source, start, count))

    def add_texts(*sources):
        slopes = jnp.concatenate([weights[source] for source in sources])
        images = jnp.concatenate([img[source] for source in sources])
        text_sum[text_window(sources[0])] += lax.dot_general(
            slopes, images, (((0,), (0,)), ((), ())), preferred_element_type=jnp.float32
        )

    def relay(target_z, sign, j):
        await_sum(target_z, sign, j)
        arrived = sum_in[(1 - sign) // 2, target_z, part(j)].astype(jnp.float32)
        sum_out[target_z, part(j)] = (own_sum[target_z, part(j)] + arrived).astype(jnp.bfloat16)
        sum_copy(target_z, sign, j).start()

    def near(j):
        relay(z + inner, inner, j)

    def part_rows(slot, j):
        return text_sum[pl.ds(pl.multiple_of(slot * rows + j * part_span, part_span), part_span)]

    def part_first(j):
        for index in (0, 1):
            slot = 2 * index + 1
            part_out[slot, part(j)] = part_rows(slot, j).astype(jnp.bfloat16)
            part_to_core(index, j).start()

    @pl.when(is_end)
    def _():
        group = pieces // 2
        near_z, far_z, edge_z = z + 2 * inner, z + 3 * inner, z + inner

        def take(source, low, count):
            span_loop(low, low + count, lambda j: await_image(source, j))
            weigh(source, pl.multiple_of(low * span, count * span), count * span)
            some = pl.ds(pl.multiple_of(low * span, count * span), count * span)
            sum_out[source, some] = own_sum[source, some].astype(jnp.bfloat16)

        def give(source, low, high):
            span_loop(2 * low, 2 * high, lambda j: sum_copy(source, inner, j).start())

        def far_step(j):
            take(far_z, j, 1)
            give(far_z, j, j + 1)

        take(near_z, 0, group)
        give(near_z, 0, group)
        weigh(z, 0, rows)
        add_texts(z)
        span_loop(0, group, far_step)
        take(edge_z, 0, group)
        span_loop(group, pieces, far_step)
        take(near_z, group, group)
        give(near_z, group, pieces)
        add_texts(far_z, near_z)
        span_loop(group, pieces, lambda j: await_image(edge_z, j))
        slopes_of(edge_z, group * span, group * span)
        add_texts(edge_z)
        loop(parts, part_first)
        last = pl.ds(group * span, group * span)
        sums_of(edge_z, group * span, group * span, weights[edge_z, last])
        sum_out[edge_z, last] = own_sum[edge_z, last].astype(jnp.bfloat16)
        give(edge_z, 0, pieces)

    @pl.when(is_mid)
    def _():
        def rest(j):
            image_copy(z, -inner, j).start()

        def image_step(index):
            @pl.when((index == 1) & ~waiting)
            def _():
                span_loop(pieces + ahead, 2 * pieces - 1, pass_inner)

            @pl.when(index == 2)
            def _():
                pass_inner(2 * pieces - 1)

                @pl.when(core == 0)
                def _():
                    span_loop(early, pieces, rest)

            @pl.when(index == 3)
            def _():
                span_loop(0, parts // 4, near)

            step = (index == 2) * 1 - (index == 0) * 1 + (index == 3) * 2
            source = z + step * inner
            weigh(source, 0, rows)
            add_texts(source)

        loop(4, image_step)

        @pl.when(core == 1)
        def _():
            span_loop(early, pieces, rest)

        loop(parts, part_first)

    def part_second(j):
        pair = part_core.at[0, pl.ds(0, 2 * part_span)]
        remote(pair, pair, 1, part_core_recv.at[j], partner).wait_recv()
        side = part_core[1 - core, part(j)].astype(jnp.float32)
        part_out[2, part(j)] = (part_rows(2, j) + side).astype(jnp.bfloat16)

        @pl.when((odd == 1) | (j < passed))
        def _():
            part_across(j).start()

        @pl.when((odd == 0) & (j >= passed) & (~bare | (j < parts // 2)))
        def _():
            part_corner(j).start()

        @pl.when(((odd == 0) | (j >= passed)) & ~bare)
        def _():
            part_third(j, 0.0)

    def part_third(j, arrived):
        side = part_core[1, part(j)].astype(jnp.float32)
        side = jnp.where(core == 1, side, 0.0) + arrived
        part_out[4, part(j)] = (part_rows(4, j) + side).astype(jnp.bfloat16)
        part_over(j).start()

    def part_relay(j):
        part_across(j).wait_recv()
        part_third(j, part_x[part(j)].astype(jnp.float32))

    def stage(i):
        j = i - parts // 2 - 1

        @pl.when(is_mid & (i < parts))
        def _():
            relay(z + 2 * inner, inner, i)

        @pl.when(is_mid & (j >= parts // 4) & (j < parts))
        def _():
            near(j)

        @pl.when(is_mid & (j > 0) & (j <= parts))
        def _():
            relay(z - inner, -inner, j - 1)

        @pl.when((odd == 1) & (i >= parts - 1) & (i - parts + 1 < passed))
        def _():
            part_relay(i - parts + 1)

    head = parts // 2
    span_loop(0, head, stage)
    loop(parts, part_second)
    span_loop(head, 2 * parts - 1, stage)

    def finish(kind, out, total, j):
        wide = raw[kind, piece(j)].astype(jnp.float32)
        scale = inverse_length(wide)
        unit = wide * scale
        grad = LOGIT_SCALE * total
        radial = jnp.sum(unit * grad, axis=-1, keepdims=True)
        out[piece(j)] = ((grad - unit * radial) * scale).astype(out.dtype)

    def finish_text(j):
        direct = (odd == 0) | (2 * j >= passed)
        @pl.when(~bare)
        def _():
            remote(
                part_out.at[4, piece(j)], part_y.at[piece(j)], 1, part_recv.at[2, j], over
            ).wait_recv()

        @pl.when(direct)
        def _():
            for half in (0, 1):
                part_across(2 * j + half).wait_recv()

        total = text_sum[slot_rows(0, j)]
        total += jnp.where(bare, 0.0, part_y[piece(j)].astype(jnp.float32))
        total += jnp.where(core == 0, part_core[0, piece(j)].astype(jnp.float32), 0.0)
        total += jnp.where(direct, part_x[piece(j)].astype(jnp.float32), 0.0)
        finish(1, both_out.at[pl.ds(rows, rows)], total, j)

    def await_own(sign, j):
        remote(
            sum_out.at[z, piece(j)], sum_in.at[(1 - sign) // 2, z, piece(j)], 2,
            sum_slot(z, z, sign, 2 * j), along(inner),
        ).wait_recv()

    def finish_image(j):
        await_own(-inner, j)

        @pl.when(is_mid)
        def _():
            await_own(inner, j)

        total = own_sum[z, piece(j)] + sum_in[(1 + inner) // 2, z, piece(j)].astype(jnp.float32)
        other = sum_in[(1 - inner) // 2, z, piece(j)].astype(jnp.float32)
        finish(0, both_out.at[pl.ds(0, rows)], total + jnp.where(is_mid, other, 0.0), j)

    def finish_both(j):
        finish_image(j)

        @pl.when(bare & (odd == 0) & (j == 0))
        def _():
            span_loop(parts // 2, parts, lambda i: part_corner(i).start())

        finish_text(j)

    loop(pieces, finish_both)

    def settle(group, count=depth):
        some = img.at[pl.ds(0, count)]
        remote(some, some, group, image_recv.at[0, 0], partner).wait_send()

    settle(0)
    settle(2)

    @pl.when(bare)
    def _():
        settle(1, 3)

    @pl.when(~bare)
    def _():
        settle(1)

    @pl.when(is_mid)
    def _():
        settle(3)


def square_call(depth, window, image_embeds, text_embeds):
    rows, width = image_embeds.shape
    slots = window // depth + 1
    pieces = rows // PIECE_ROWS
    early, relayed, passed, ahead = 3 * pieces // 4, 3 * pieces // 4, 2 * pieces, pieces // 2
    low, wide = jnp.bfloat16, jnp.float32
    both = pl.pallas_call(
        functools.partial(ring_kernel, depth, window, pieces, early, relayed, passed, ahead),
        out_shape=pltpu.VMEM((2 * rows, width), low),
        in_specs=[pl.BlockSpec(memory_space=pl.ANY)] * 2,
        out_specs=pl.BlockSpec(memory_space=pltpu.VMEM),
        scratch_shapes=[
            pltpu.VMEM((2, rows, width), low),
            pltpu.VMEM((depth, rows, width), low),
            pltpu.VMEM((slots * rows, width), low),
            pltpu.VMEM((depth, rows, width), wide),
            pltpu.VMEM((slots * rows, width), wide),
            pltpu.VMEM((depth, rows, (slots - 1) * rows), low),
            pltpu.VMEM((depth, rows, width), low),
            pltpu.VMEM((2, depth, rows, width), low),
            pltpu.VMEM((slots, rows, width), low),
            pltpu.VMEM((2, rows, width), low),
            pltpu.VMEM((rows, width), low),
            pltpu.VMEM((rows, width), low),
            pltpu.SemaphoreType.DMA((2,)),
            pltpu.SemaphoreType.DMA((4,)),
            pltpu.SemaphoreType.DMA((depth - 1, pieces)),
            pltpu.SemaphoreType.DMA((2, pieces)),
            pltpu.SemaphoreType.DMA((2,)),
            pltpu.SemaphoreType.DMA((depth, 2 * pieces)),
            pltpu.SemaphoreType.DMA((3, pieces)),
            pltpu.SemaphoreType.DMA((2 * pieces,)),
        ],
        compiler_params=pltpu.CompilerParams(collective_id=0, has_side_effects=True),
    )(image_embeds, text_embeds)
    return both[:rows], both[rows:]


def solution(mesh):
    cycle, depth = mesh.shape["blk"], mesh.shape["grp"]
    window = min(20, cycle * depth // 2)
    chips = cycle // 2
    reach = 1
    while (2 * reach + 1) * depth - (depth - 1) < window:
        reach += 1
    slots = 2 * (reach + 1)

    def per_device(image_embeds, text_embeds):
        rows, width = image_embeds.shape
        shape = jax.ShapeDtypeStruct((rows, width), jnp.bfloat16)
        if chips == 4 and depth == 4 and window == 4 * depth:
            return square_call(depth, window, image_embeds, text_embeds)
        return pl.pallas_call(
            functools.partial(kernel, chips, depth, reach, window),
            out_shape=(shape, shape),
            in_specs=[pl.BlockSpec(memory_space=pl.ANY)] * 2,
            out_specs=(pl.BlockSpec(memory_space=pltpu.VMEM),) * 2,
            scratch_shapes=[
                pltpu.VMEM((2, slots, depth, rows, width), jnp.bfloat16),
                pltpu.VMEM((2, rows, width), jnp.float32),
                pltpu.VMEM((2, rows, rows), jnp.float32),
                pltpu.SemaphoreType.DMA((2,)),
                pltpu.SemaphoreType.DMA((2, 6 + 2 * reach, depth)),
                pltpu.SemaphoreType.DMA((2, slots, depth)),
            ],
            compiler_params=pltpu.CompilerParams(collective_id=0, has_side_effects=True),
        )(image_embeds, text_embeds)

    placed = P(("blk", "grp"), None)
    return jax.shard_map(
        per_device, mesh=mesh, in_specs=(placed, placed), out_specs=(placed, placed), check_vma=False
    )
```
